32 devices in a mesh: grp: 2 (over y), tile: 4 (over z), coil: 2 (over x), spk: 2 (over core).
Axes of the slice: x: 2, y: 2, z: 4, core: 2. Of those that a mesh axis runs over, the one named last changes fastest.
Arguments:
- coil_maps: float32 [2, 512, 2, 256], P('coil', ('grp', 'tile', 'spk')), parts along dimension 1, may hold values from -6 to 6
- kspace_data: bfloat16 [2, 128, 2, 256], P('coil', ('grp', 'tile', 'spk')), parts along dimension 1, may hold values from -24 to 24
- interp_weights: bfloat16 [128, 6, 256], P(('grp', 'tile', 'spk')), parts along dimension 0, may hold values from 0.099609375 to 1
- sample_bins: int32 [128, 256], P(('grp', 'tile', 'spk')), parts along dimension 0, may hold values from 0 to 65535, as said below
- spoke_count: int32 [16], P(('grp', 'tile', 'spk')), parts along dimension 0, may hold values from 1 to 8, 32 in all
- thresholds: float32 [3], replicated, may hold values from 0.05 to 0.3
Outputs:
- image: float32 [512, 2, 256], P(('grp', 'tile', 'spk')), parts along dimension 0
The draws below stay inside these ranges and needn't reach their ends.
There are 2 independent parts, one for each index of `grp`. The reference program is written for one: setup_inputs(seed, part) draws one part's arguments, and reference() takes and returns one part's arrays. A program takes and returns all parts, laid end to end along the dimension named above; an argument that names none is the same for every part. Nothing has to cross between parts.
Inputs may be any that keep to these rules, and one draw needn't show every extreme that they name: `sample_bins`: sample k of each spoke lies on a straight line through cell (128, 128), at offset k - 128 along the spoke's direction, coordinates taken modulo 256. `spoke_count`: each independent slice has its own 8 counts, and the whole array holds one such block of counts per slice. The 8 counts of each slice sum to 32. In every draw, at least one device of each slice holds 8 live spokes. A device's live spokes are its first ones.
All inputs are finite; a program needn't handle non-finite values.
Results may differ from the reference program's by a relative error of at most 0.0016.
Values may be sent and summed in bfloat16 or wider, within the bound.
No kernel may reach another device: no remote copies, remote signals or barrier semaphores. Data moves between devices by JAX's collectives and lax.ppermute only.
A program may use at most 64 MiB of HBM per device.

```python
import math
import jax
import jax.numpy as jnp
import numpy as np
from jax import lax

N = 256
RO = 256
SPK_DEV = 8
LEVELS = 3
ITERS = 4
COILS = 2
BLOCKS = 8
SPOKES = 64


def draw_sample_bins(key, part):
    key_side, key_sign, key_slope = jax.random.split(key, 3)
    middle = N // 2
    side_pick = jax.random.randint(key_side, (SPOKES,), 0, 2)
    sign_pick = jax.random.randint(key_sign, (SPOKES,), 0, 2) * 2 - 1
    slope_val = jax.random.randint(key_slope, (SPOKES,), -middle, middle + 1)
    row_dir = jnp.where(side_pick == 1, sign_pick * middle, slope_val)
    col_dir = jnp.where(side_pick == 1, slope_val, sign_pick * middle)
    offsets = jnp.arange(RO, dtype=jnp.int32) - RO // 2
    row_bins = (middle + offsets[None, :] * row_dir[:, None] * 2 // RO) % N
    col_bins = (middle + offsets[None, :] * col_dir[:, None] * 2 // RO) % N
    return (row_bins * N + col_bins).astype(jnp.int32)


def steps_of(stream_key, dims, cuts, least, high):
    factor_of, own = 1.0, jax.random.fold_in(stream_key, 6)
    for position, parts in cuts:
        steps = jnp.exp(jax.random.uniform(jax.random.fold_in(own, position), (parts,), jnp.float32, least / len(cuts), high / len(cuts)))
        factor_of = factor_of * jnp.repeat(steps, dims[position] // parts).reshape([-1 if axis == position else 1 for axis in range(len(dims))])
    return factor_of


def profile(number_of, total, most, lean):
    portions = [(1 << 20) // math.isqrt(grade ** lean) + 1 for grade in range(2, number_of + 1)]
    surplus, holding = total - most - (number_of - 1), [1] * (number_of - 1)
    while surplus > 0:
        movable = [i for i in range(number_of - 1) if holding[i] < most]
        whole, left = sum([portions[i] for i in movable]), surplus
        for i in movable:
            addition = min(most - holding[i], max(1, left * portions[i] // whole), surplus)
            holding[i] = holding[i] + addition
            surplus = surplus - addition
    return np.array([most] + holding)


def uneven(rng, number_of, total, reach, skew):
    if number_of == 2:
        one = jax.random.randint(rng, (), max(1, total - reach), min(reach, total - 1) + 1)
        return jnp.stack([one, total - one])
    sizes = jnp.asarray(profile(number_of, total, reach, skew), jnp.int32)
    twos = (number_of - 1) // 2
    giver, sink = sizes[1:1 + 2 * twos:2], sizes[2:2 + 2 * twos:2]
    margin = jnp.minimum(giver - 1, reach - sink)
    passed = jax.random.randint(jax.random.fold_in(rng, 1), (twos,), 0, 1 << 20) % (margin + 1)
    sizes = sizes.at[1:1 + 2 * twos:2].set(giver - passed).at[2:2 + 2 * twos:2].set(sink + passed)
    return sizes[jax.random.permutation(jax.random.fold_in(rng, 2), number_of)]


def gaussian(rng, dims, spread, limit, pieces=(), kind=jnp.bfloat16):
    entries = jax.random.normal(rng, dims, jnp.float32) * spread
    if len(pieces) > 0:
        entries = steps_of(rng, dims, pieces, -0.22, 0.18) * entries
    return jnp.clip(entries, min=-limit, max=limit).astype(kind)


def setup_inputs(seed: int = 0, part: int = 0) -> dict:
    splits = jax.random.split(jax.random.key(seed), 7)
    own_keys = jax.random.split(jax.random.fold_in(splits[6], part), 7)
    return {
        "coil_maps": gaussian(own_keys[0], (COILS, N, 2, N), (1.0 / (2.0 * COILS) ** 0.5), 6.0, ((0, 2), (1, 8)), jnp.float32),
        "kspace_data": gaussian(own_keys[1], (COILS, SPOKES, 2, RO), 4.0, 24.0, ((0, 2), (1, 8))),
        "interp_weights": jnp.clip(0.099609375 + 0.9003906 * jax.random.uniform(own_keys[2], (SPOKES, 6, RO), jnp.float32) ** steps_of(own_keys[2], (SPOKES, 6, RO), ((0, 8),), -0.2, 0.2), 0.099609375, 1.0).astype(jnp.bfloat16),
        "sample_bins": draw_sample_bins(jax.random.fold_in(jax.random.fold_in(splits[6], part), 71), part),
        "spoke_count": uneven(own_keys[4], BLOCKS, BLOCKS * SPK_DEV // 2, SPK_DEV, 2).astype(jnp.int32),
        "thresholds": jnp.clip(jax.random.uniform(splits[5], (LEVELS,), jnp.float32, 0.05, 0.3), 0.05, 0.3),
    }


HIGH = lax.Precision.HIGHEST
STEP_SIZE = 0.5
RSQRT2 = 0.7071067811865476

def dft_table(length, direction):
    positions = jnp.arange(length, dtype=jnp.int32)
    phases = positions[:, None] * positions[None, :] % length
    angles = phases.astype(jnp.float32) * jnp.float32(2.0 * math.pi / length)
    norm_scale = 1.0 / math.sqrt(length)
    cosine = jnp.cos(angles) * norm_scale
    sine_tab = jnp.sin(angles) * norm_scale
    top_rows = jnp.stack([cosine, -direction * sine_tab], axis=1)
    bottom = jnp.stack([direction * sine_tab, cosine], axis=1)
    return jnp.stack([top_rows, bottom], axis=0)

def haar_matrix(length, levels):
    haar_mat = jnp.eye(length, dtype=jnp.float32)
    positions = jnp.arange(length, dtype=jnp.int32)
    out_i = positions[:, None]
    in_j = positions[None, :]
    for level_num in range(levels):
        span_len = length >> level_num
        half_len = span_len // 2
        low_hit = (out_i < half_len) & ((in_j == 2 * out_i) | (in_j == 2 * out_i + 1))
        high_pos = out_i - half_len
        high_hit = (out_i >= half_len) & (out_i < span_len) & ((in_j == 2 * high_pos) | (in_j == 2 * high_pos + 1))
        sign_val = jnp.where(in_j == 2 * high_pos + 1, -1.0, 1.0)
        step_mat = jnp.where(low_hit, RSQRT2, jnp.where(high_hit, sign_val * RSQRT2, 0.0))
        step_mat = step_mat + jnp.where((out_i >= span_len) & (in_j == out_i), 1.0, 0.0)
        haar_mat = jnp.dot(step_mat.astype(jnp.float32), haar_mat, precision=HIGH)
    return haar_mat

def haar_labels(length, levels):
    positions = jnp.arange(length, dtype=jnp.int32)
    band_label = jnp.ones((length,), jnp.int32)
    for level_num in range(1, levels + 1):
        band_label = band_label + (positions < length >> level_num).astype(jnp.int32)
    return band_label

def wavelet_shrink(target, thresholds, levels):
    row_count, pair_dim, col_count = target.shape
    block_len = 2 ** levels
    row_haar = haar_matrix(block_len, levels)
    col_haar = haar_matrix(col_count, levels)
    grouped = target.reshape(row_count // block_len, block_len, pair_dim, col_count)
    coeffs = jnp.einsum('ij,gjpc->gipc', row_haar, grouped, precision=HIGH)
    coeffs = jnp.einsum('gipc,kc->gipk', coeffs, col_haar, precision=HIGH)
    band_min = jnp.minimum(haar_labels(block_len, levels)[:, None], haar_labels(col_count, levels)[None, :])
    active = band_min <= levels
    limits = jnp.ones(band_min.shape, jnp.float32)
    for level_num in range(levels):
        limits = jnp.where(band_min == level_num + 1, thresholds[level_num], limits)
    magnitude = jnp.sqrt(coeffs[:, :, 0] ** 2 + coeffs[:, :, 1] ** 2)
    factor = jnp.maximum(magnitude - limits, 0.0) / jnp.maximum(magnitude, limits)
    factor = jnp.where(active, factor, 1.0)
    shrunk = coeffs * factor[:, :, None, :]
    restored = jnp.einsum('gipk,kc->gipc', shrunk, col_haar, precision=HIGH)
    restored = jnp.einsum('ij,gipc->gjpc', row_haar, restored, precision=HIGH)
    return restored.reshape(row_count, pair_dim, col_count)

def complex_mul(left, right):
    real_part = left[:, 0] * right[:, 0] - left[:, 1] * right[:, 1]
    imag_part = left[:, 0] * right[:, 1] + left[:, 1] * right[:, 0]
    return jnp.stack([real_part, imag_part], axis=1)

def conj_mul(left, right):
    real_part = left[:, 0] * right[:, 0] + left[:, 1] * right[:, 1]
    imag_part = left[:, 0] * right[:, 1] - left[:, 1] * right[:, 0]
    return jnp.stack([real_part, imag_part], axis=1)

def reference(coil_maps, kspace_data, interp_weights, sample_bins, spoke_count, thresholds):
    spokes_all = sample_bins.shape[0]
    blocks_all = spoke_count.shape[0]
    per_block = spokes_all // blocks_all
    live_total = spokes_all // 2
    spoke_ids = jnp.arange(spokes_all, dtype=jnp.int32)
    owners = (spoke_ids // per_block).astype(jnp.int32)
    live_mask = (spoke_ids % per_block < spoke_count[owners]).astype(jnp.float32)
    offset = jnp.abs(jnp.arange(RO, dtype=jnp.int32) - RO // 2).astype(jnp.float32)
    density = (offset + 0.5) * (N / (3.0 * RO * live_total))
    row_bins = sample_bins // N
    col_bins = sample_bins % N
    row_taps = [((row_bins + tap_index - 1) % N).astype(jnp.int32) for tap_index in range(3)]
    col_taps = [((col_bins + tap_index - 1) % N).astype(jnp.int32) for tap_index in range(3)]
    weights_f = interp_weights.astype(jnp.float32)
    fwd_table = dft_table(N, 1.0)
    inv_table = dft_table(N, -1.0)

    def coil_gradient(estimate, maps_one, data_one):
        coil_image = complex_mul(maps_one, estimate)
        half_done = jnp.einsum('rpc,pcqv->rqv', coil_image, fwd_table, precision=HIGH)
        kspace = jnp.einsum('rpv,prqu->vqu', half_done, fwd_table, precision=HIGH).astype(jnp.bfloat16)
        kspace = lax.optimization_barrier(kspace).astype(jnp.float32)
        sample_model = jnp.zeros((spokes_all, RO, 2), jnp.float32)
        for col_index in range(3):
            inner_sum = jnp.zeros((spokes_all, RO, 2), jnp.float32)
            for row_index in range(3):
                picked = kspace[col_taps[col_index], :, row_taps[row_index]]
                inner_sum = inner_sum + weights_f[:, row_index, :, None] * picked
            sample_model = sample_model + weights_f[:, 3 + col_index, :, None] * inner_sum
        sample_model = jnp.transpose(sample_model, (0, 2, 1))
        weighted = live_mask[:, None, None] * density[None, None, :] * (sample_model - data_one.astype(jnp.float32))
        gridded = jnp.zeros((N, 2, N), jnp.float32)
        for col_index in range(3):
            smeared = (weights_f[:, 3 + col_index, None, :] * weighted).astype(jnp.bfloat16)
            smeared = lax.optimization_barrier(smeared).astype(jnp.float32)
            smeared_t = jnp.transpose(smeared, (0, 2, 1))
            for row_index in range(3):
                gridded = gridded.at[col_taps[col_index], :, row_taps[row_index]].add(weights_f[:, row_index, :, None] * smeared_t)
        partial_back = jnp.einsum('vpu,puqr->vqr', gridded, inv_table, precision=HIGH)
        coil_back = jnp.einsum('vpr,pvqc->rqc', partial_back, inv_table, precision=HIGH)
        return conj_mul(maps_one, coil_back)
    estimate = jnp.zeros((N, 2, N), jnp.float32)
    for iteration in range(ITERS):
        terms = lax.map(lambda coil_pack: coil_gradient(estimate, coil_pack[0], coil_pack[1]), (coil_maps, kspace_data))
        gradient = lax.optimization_barrier(jnp.sum(terms, axis=0))
        estimate = wavelet_shrink(estimate - STEP_SIZE * gradient, thresholds, LEVELS)
    return estimate
```

```python
import functools
import math

import jax
import jax.numpy as jnp
import numpy as np
from jax import lax
from jax.experimental import pallas as pl
from jax.experimental.pallas import tpu as pltpu
from jax.sharding import PartitionSpec as P

LEVELS = 3
ITERS = 4
STEP_SIZE = 0.5
GROUP = 4
F32 = jnp.float32
BF16 = jnp.bfloat16


def split_host(table):
    high = table.astype(BF16)
    low = (table - high.astype(np.float64)).astype(BF16)
    return high, low


def dft_tables(n):
    idx = np.arange(n)
    angles = 2.0 * math.pi / n * (np.outer(idx, idx) % n)
    scale = 1.0 / math.sqrt(n)
    parts = [np.cos(angles) * scale, np.sin(angles) * scale, -np.sin(angles) * scale]
    pairs = [split_host(part) for part in parts]
    return np.stack([pair[0] for pair in pairs] + [pair[1] for pair in pairs])


def haar_signs(n):
    mat = np.eye(n)
    for level in range(LEVELS):
        span, half = n >> level, n >> (level + 1)
        step = np.eye(n)
        step[:span] = 0.0
        for i in range(half):
            step[i, 2 * i] = step[i, 2 * i + 1] = 1.0
            step[half + i, 2 * i], step[half + i, 2 * i + 1] = 1.0, -1.0
        mat = step @ mat
    return mat


def haar_tables(n):
    col = haar_signs(n)
    row = np.kron(np.eye(n // 2**LEVELS), haar_signs(2**LEVELS))
    return np.stack([col, col.T, row.T, row]).astype(BF16)


def split2(x):
    high = x.astype(BF16)
    return high, (x - high.astype(F32)).astype(BF16)


def split3(x):
    high = x.astype(BF16)
    rest = x - high.astype(F32)
    mid = rest.astype(BF16)
    return high, mid, (rest - mid.astype(F32)).astype(BF16)


def mm(a, b):
    return jnp.dot(a, b, preferred_element_type=F32)


def right_dft(re, im, dft, sign):
    top = jnp.concatenate([re, sign * im], axis=1)
    bottom = jnp.concatenate([im, -sign * re], axis=1)
    high, low = split2(jnp.concatenate([top, bottom], axis=0))
    t_high = jnp.concatenate([dft[0], dft[1]], axis=0)
    t_low = jnp.concatenate([dft[3], dft[4]], axis=0)
    return mm(high, t_high) + mm(low, t_high) + mm(high, t_low)


def left_dft(stacked, dft, sign):
    plus, minus = (1, 2) if sign > 0 else (2, 1)
    high, low = split2(stacked)

    def table(base):
        top = jnp.concatenate([dft[base], dft[base + plus]], axis=1)
        bottom = jnp.concatenate([dft[base + minus], dft[base]], axis=1)
        return jnp.concatenate([top, bottom], axis=0)

    t_high, t_low = table(0), table(3)
    return mm(t_high, high) + mm(t_high, low) + mm(t_low, high)


def labels(positions, length):
    out = jnp.ones(positions.shape, F32)
    for level in range(1, LEVELS + 1):
        out = out + jnp.where(positions < length >> level, 1.0, 0.0)
    return out


def exact_left(signs, parts):
    return sum(mm(signs, part) for part in parts)


def exact_right(parts, signs):
    return sum(mm(part, signs) for part in parts)


def shrink(re, im, thr_ref, haar, last_rows=None):
    n = re.shape[0]
    block = 2**LEVELS
    col_pos = lax.broadcasted_iota(jnp.int32, (n, 1), 0)
    row_pos = lax.broadcasted_iota(jnp.int32, (1, n), 1) % block
    col_label, row_label = labels(col_pos, n), labels(row_pos, block)
    col_scale = jnp.exp2(-0.5 * jnp.minimum(col_label, LEVELS))
    row_scale = jnp.exp2(-0.5 * jnp.minimum(row_label, LEVELS))
    band = jnp.minimum(col_label, row_label)
    limits = jnp.full((n, n), 1.0, F32)
    for level in range(LEVELS):
        limits = jnp.where(band == level + 1, thr_ref[level], limits)
    scale = col_scale * row_scale
    coeffs = []
    for part in (re, im):
        half = exact_left(haar[0], split3(part))
        coeffs.append(exact_right(split3(half), haar[2]) * scale)
    magnitude = jnp.sqrt(coeffs[0] * coeffs[0] + coeffs[1] * coeffs[1])
    factor = jnp.maximum(magnitude - limits, 0.0) / jnp.maximum(magnitude, limits)
    factor = jnp.where(band <= LEVELS, factor, 1.0) * scale
    out = []
    for part in coeffs:
        half = exact_left(haar[1], split3(part * factor))
        if last_rows is None:
            out.append(exact_right(split3(half), haar[3]))
        else:
            out.append(
                sum(
                    lax.dot_general(last_rows, p, (((1,), (1,)), ((), ())), preferred_element_type=F32)
                    for p in split3(half)
                )
            )
    return out


def density_of(ro, n, live_total):
    lane = lax.broadcasted_iota(jnp.int32, (1, ro), 1)
    offset = jnp.abs(lane - ro // 2).astype(F32)
    return (offset + 0.5) * (n / (3.0 * ro * live_total))


def smear(col_table, weighted):
    col = col_table.astype(F32)
    both = [(col * weighted[p : p + 1]).astype(BF16) for p in range(2)]
    return jnp.concatenate(both, axis=0)


def grid_dot(smeared, row_table):
    return lax.dot_general(smeared, row_table, (((1,), (1,)), ((), ())), preferred_element_type=F32)


def adjoint(gridded, dft):
    half = left_dft(gridded, dft, -1)
    n = gridded.shape[0] // 2
    return right_dft(half[:n], half[n:], dft, -1)


def first_kernel(share, first_of, places_of, live_total, pieces, n, *refs):
    piece_refs, refs = refs[:pieces], refs[pieces:]
    dft_ref, row_out, col_out, data_out, back_out = refs[:5]
    slots, rows_s, cols_s, grid_s, list_s, row_sem, col_sem = refs[5:]
    spk_dev, fields, ro = piece_refs[0].shape
    groups = share // GROUP
    for piece, place in zip(piece_refs, places_of(), strict=True):
        slots[pl.ds(place * spk_dev, spk_dev), 0:fields, :] = piece[...].astype(F32)
    taken = jnp.int32(0)
    for block in range(pieces):
        count = jnp.max(slots[block * spk_dev, fields - 1 : fields, :]).astype(jnp.int32)
        for depth in range(spk_dev):
            list_s[taken] = block * spk_dev + depth
            taken = taken + (depth < count).astype(jnp.int32)
    start = first_of()
    density = density_of(ro, n, live_total)
    cells = lax.broadcasted_iota(jnp.int32, (n, ro), 0).astype(F32)
    grid_s[...] = jnp.zeros_like(grid_s)

    def table(at, weights):
        before = jnp.where(at == 0, n - 1.0, at - 1)
        after = jnp.where(at == n - 1, 0.0, at + 1)
        out = jnp.where(cells == after, weights[2:3], 0.0)
        out = jnp.where(cells == at, weights[1:2], out)
        return jnp.where(cells == before, weights[0:1], out).astype(BF16)

    def group_step(group, carry):
        smeared = []
        for j in range(GROUP):
            slot = slots[list_s[start + group * GROUP + j]]
            rows_s[group, :, j * ro : (j + 1) * ro] = table(slot[6:7], slot[0:3])
            col_table = table(slot[7:8], slot[3:6])
            cols_s[group, :, j * ro : (j + 1) * ro] = col_table
            data = slot[8:10]
            data_out[group * GROUP + j] = data
            smeared.append(smear(col_table, -density * data))
        grid_s[...] += grid_dot(jnp.concatenate(smeared, axis=1), rows_s[group])
        pltpu.make_async_copy(rows_s.at[group], row_out.at[group], row_sem.at[group]).start()
        pltpu.make_async_copy(cols_s.at[group], col_out.at[group], col_sem.at[group]).start()
        return carry

    lax.fori_loop(0, groups, group_step, 0)
    back_out[...] = adjoint(grid_s[...], dft_ref)

    def drain(group, carry):
        pltpu.make_async_copy(rows_s.at[group], row_out.at[group], row_sem.at[group]).wait()
        pltpu.make_async_copy(cols_s.at[group], col_out.at[group], col_sem.at[group]).wait()
        return carry

    lax.fori_loop(0, groups, drain, 0)


def step_kernel(share, live_total, n_parts, *refs):
    thr_ref, est_ref, part_refs, refs = refs[0], refs[1], refs[2 : 2 + n_parts], refs[2 + n_parts :]
    map_ref, data_ref, dft_ref, haar_ref, row_hbm, col_hbm, est_out, part_out = refs[:8]
    rows_s, cols_s, weighted_s, grid_s, row_sem, col_sem = refs[8:]
    groups = share // GROUP
    n = map_ref.shape[1]
    ro = data_ref.shape[-1]

    def copies(group):
        return (
            pltpu.make_async_copy(row_hbm.at[group], rows_s.at[group], row_sem.at[group]),
            pltpu.make_async_copy(col_hbm.at[group], cols_s.at[group], col_sem.at[group]),
        )

    for group in range(groups):
        for copy in copies(group):
            copy.start()
    target = []
    for p in range(2):
        gradient = sum(part[p] for part in part_refs)
        target.append(est_ref[p] - STEP_SIZE * gradient)
    re, im = shrink(target[0], target[1], thr_ref, haar_ref)
    est_out[0] = re
    est_out[1] = im
    mre, mim = map_ref[0], map_ref[1]
    half = right_dft(mre * re - mim * im, mre * im + mim * re, dft_ref, 1)
    kspace = left_dft(half, dft_ref, 1).astype(BF16)
    density = density_of(ro, n, live_total)
    grid_s[...] = jnp.zeros_like(grid_s)

    def sample_group(group, carry):
        for copy in copies(group):
            copy.wait()
        for j in range(GROUP):
            inner = mm(kspace, rows_s[group, :, j * ro : (j + 1) * ro])
            col = cols_s[group, :, j * ro : (j + 1) * ro].astype(F32)
            data = data_ref[group * GROUP + j]
            model = [jnp.sum(inner[p * n : (p + 1) * n] * col, axis=0, keepdims=True) for p in range(2)]
            weighted_s[group * GROUP + j] = density * (jnp.concatenate(model, axis=0) - data)
        return carry

    lax.fori_loop(0, groups, sample_group, 0)

    def grid_group(group, carry):
        smeared = [
            smear(cols_s[group, :, j * ro : (j + 1) * ro], weighted_s[group * GROUP + j]) for j in range(GROUP)
        ]
        grid_s[...] += grid_dot(jnp.concatenate(smeared, axis=1), rows_s[group])
        return carry

    lax.fori_loop(0, groups, grid_group, 0)
    back = adjoint(grid_s[...], dft_ref)
    conj_map(map_ref[0], map_ref[1], back, part_out)


def conj_map(mre, mim, back, part_out):
    n = mre.shape[0]
    bre, bim = back[:n], back[n:]
    part_out[0] = mre * bre + mim * bim
    part_out[1] = mre * bim - mim * bre


def map_kernel(places_of, pieces, *refs):
    piece_refs, (back_ref, map_out, part_out, full) = refs[:pieces], refs[pieces:]
    rows = piece_refs[0].shape[0]
    for piece, place in zip(piece_refs, places_of(), strict=True):
        for p in range(2):
            full[p, pl.ds(place * rows, rows), :] = piece[:, p, :]
    for p in range(2):
        map_out[p] = full[p].T
    conj_map(map_out[0], map_out[1], back_ref[...], part_out)


def last_kernel(n_parts, rows, mine_of, thr_ref, est_ref, *refs):
    part_refs, (haar_ref, out_ref) = refs[:n_parts], refs[n_parts:]
    n = est_ref.shape[1]
    target = []
    for p in range(2):
        gradient = sum(part[p] for part in part_refs)
        target.append(est_ref[p] - STEP_SIZE * gradient)
    mine = mine_of()
    pick = lax.broadcasted_iota(jnp.int32, (rows, n), 1) == (
        lax.broadcasted_iota(jnp.int32, (rows, n), 0) + mine * rows
    )
    own = mm(jnp.where(pick, 1.0, 0.0).astype(BF16), haar_ref[2]).astype(BF16)
    re, im = shrink(target[0], target[1], thr_ref, haar_ref, own)
    out_ref[:, 0, :] = re
    out_ref[:, 1, :] = im


def local(coil_maps, kspace_data, interp_weights, sample_bins, spoke_count, thresholds):
    n_tile, n_coil, n_spk = (lax.axis_size(name) for name in ("tile", "coil", "spk"))
    blocks = n_tile * n_spk
    rows, _, n = coil_maps.shape[1:]
    spk_dev, ro = sample_bins.shape
    live_total = blocks * spk_dev // 2
    own_map = coil_maps[0]
    by_core = n_coil == n_spk == 2
    cells = jnp.stack([sample_bins // n, sample_bins % n], axis=1).astype(BF16)
    count = jnp.broadcast_to(spoke_count.astype(BF16)[:, None, None], (spk_dev, 1, ro))
    bundle = jnp.concatenate([interp_weights, cells, kspace_data[0], count], axis=1)

    if by_core:
        onto = [(0, 2), (3, 1), (1, 0), (2, 3)]
        across = [(1, 2), (2, 1)]
        is_own = lax.axis_index("coil") == lax.axis_index("spk")

        def collect(value):
            near = lax.ppermute(value, ("coil", "spk"), onto)
            far = lax.ppermute(value, ("coil", "spk"), across)
            return [jnp.where(is_own, value, far), near]

        def spread(values):
            out = list(values)
            for shift in range(1, n_tile):
                out += [lax.ppermute(v, "tile", [(i, (i + shift) % n_tile) for i in range(n_tile)]) for v in values]
            return out

        def places_of():
            tile, coil = lax.axis_index("tile"), lax.axis_index("coil")
            sent = [(tile - shift + n_tile) % n_tile for shift in range(n_tile)]
            return [at * 2 + block for at in sent for block in (coil, 1 - coil)]

        spokes = spread(collect(bundle))
        maps = spread(collect(own_map))
        share, first_of = live_total, lambda: jnp.int32(0)

        def parts_of(part):
            return [part, lax.ppermute(part, "spk", [(0, 1), (1, 0)])]
    else:
        spokes = list(lax.all_gather(bundle, ("tile", "spk"), axis=0, tiled=False))
        maps = list(lax.all_gather(own_map, ("tile", "spk"), axis=0, tiled=False))
        places_of = lambda: list(range(blocks))
        share = live_total // blocks
        first_of = lambda: (lax.axis_index("tile") * n_spk + lax.axis_index("spk")) * share

        def parts_of(part):
            return [lax.psum(part, ("tile", "coil", "spk"))]

    groups = share // GROUP
    dft = jnp.asarray(dft_tables(n))
    haar = jnp.asarray(haar_tables(n))
    tables = jax.ShapeDtypeStruct((groups, n, GROUP * ro), BF16)
    image = jax.ShapeDtypeStruct((2, n, n), F32)
    vmem = pl.BlockSpec(memory_space=pltpu.VMEM)
    smem = pl.BlockSpec(memory_space=pltpu.SMEM)
    hbm = pl.BlockSpec(memory_space=pl.ANY)
    table_scratch = [pltpu.VMEM(tables.shape, BF16)] * 2
    sems = [pltpu.SemaphoreType.DMA((groups,))] * 2
    row_tab, col_tab, data, back = pl.pallas_call(
        functools.partial(first_kernel, share, first_of, places_of, live_total, blocks, n),
        out_shape=[tables, tables, jax.ShapeDtypeStruct((share, 2, ro), F32), jax.ShapeDtypeStruct((2 * n, n), F32)],
        in_specs=[vmem] * (blocks + 1),
        out_specs=[hbm, hbm, vmem, vmem],
        scratch_shapes=[
            pltpu.VMEM((blocks * spk_dev, 16, ro), F32),
            *table_scratch,
            pltpu.VMEM((2 * n, n), F32),
            pltpu.SMEM((blocks * spk_dev + 1,), jnp.int32),
            *sems,
        ],
    )(*spokes, dft)
    map_t, part = pl.pallas_call(
        functools.partial(map_kernel, places_of, blocks),
        out_shape=[image, image],
        in_specs=[vmem] * (blocks + 1),
        out_specs=[vmem, vmem],
        scratch_shapes=[pltpu.VMEM((2, n, n), F32)],
    )(*maps, back)
    estimate = jnp.zeros((2, n, n), F32)
    parts = parts_of(part)
    for _ in range(1, ITERS):
        estimate, part = pl.pallas_call(
            functools.partial(step_kernel, share, live_total, len(parts)),
            out_shape=[image, image],
            in_specs=[smem] + [vmem] * (len(parts) + 5) + [hbm, hbm],
            out_specs=[vmem, vmem],
            scratch_shapes=[
                *table_scratch,
                pltpu.VMEM((share, 2, ro), F32),
                pltpu.VMEM((2 * n, n), F32),
                *sems,
            ],
        )(thresholds, estimate, *parts, map_t, data, dft, haar, row_tab, col_tab)
        parts = parts_of(part)
    mine_of = lambda: lax.axis_index("tile") * n_spk + lax.axis_index("spk")
    return pl.pallas_call(
        functools.partial(last_kernel, len(parts), rows, mine_of),
        out_shape=jax.ShapeDtypeStruct((rows, 2, n), F32),
        in_specs=[smem] + [vmem] * (len(parts) + 2),
        out_specs=vmem,
    )(thresholds, estimate, *parts, haar)


def solution(mesh):
    placed = (
        P("coil", ("grp", "tile", "spk"), None, None),
        P("coil", ("grp", "tile", "spk"), None, None),
        P(("grp", "tile", "spk"), None, None),
        P(("grp", "tile", "spk"), None),
        P(("grp", "tile", "spk")),
        P(),
    )
    return jax.shard_map(
        local,
        mesh=mesh,
        in_specs=placed,
        out_specs=P(("grp", "tile", "spk"), None, None),
        check_vma=False,
    )
```

```python
import functools
import math

import jax
import jax.numpy as jnp
import numpy as np
from jax import lax
from jax.experimental import pallas as pl
from jax.experimental.pallas import tpu as pltpu
from jax.sharding import PartitionSpec as P

LEVELS = 3
ITERS = 4
STEP_SIZE = 0.5
GROUP = 4
PARAMS = pltpu.CompilerParams(vmem_limit_bytes=26 * 2**20)
F32 = jnp.float32
BF16 = jnp.bfloat16


def split_host(table):
    high = table.astype(BF16)
    low = (table - high.astype(np.float64)).astype(BF16)
    return high, low


def dft_tables(n):
    idx = np.arange(n)
    angles = 2.0 * math.pi / n * (np.outer(idx, idx) % n)
    scale = 1.0 / math.sqrt(n)
    parts = [np.cos(angles) * scale, np.sin(angles) * scale, -np.sin(angles) * scale]
    pairs = [split_host(part) for part in parts]
    return np.stack([pair[0] for pair in pairs] + [pair[1] for pair in pairs])


def haar_signs(n):
    mat = np.eye(n)
    for level in range(LEVELS):
        span, half = n >> level, n >> (level + 1)
        step = np.eye(n)
        step[:span] = 0.0
        for i in range(half):
            step[i, 2 * i] = step[i, 2 * i + 1] = 1.0
            step[half + i, 2 * i], step[half + i, 2 * i + 1] = 1.0, -1.0
        mat = step @ mat
    return mat


def haar_tables(n):
    col = haar_signs(n)
    row = np.kron(np.eye(n // 2**LEVELS), haar_signs(2**LEVELS))
    return np.stack([col, col.T, row.T, row]).astype(BF16)


def split2(x):
    high = x.astype(BF16)
    return high, (x - high.astype(F32)).astype(BF16)


def split3(x):
    high = x.astype(BF16)
    rest = x - high.astype(F32)
    mid = rest.astype(BF16)
    return high, mid, (rest - mid.astype(F32)).astype(BF16)


def mm(a, b):
    return jnp.dot(a, b, preferred_element_type=F32)


def right_dft(re, im, dft, sign):
    top = jnp.concatenate([re, sign * im], axis=1)
    bottom = jnp.concatenate([im, -sign * re], axis=1)
    high, low = split2(jnp.concatenate([top, bottom], axis=0))
    t_high = jnp.concatenate([dft[0], dft[1]], axis=0)
    t_low = jnp.concatenate([dft[3], dft[4]], axis=0)
    return mm(high, t_high) + mm(low, t_high) + mm(high, t_low)


def left_dft(stacked, dft, sign):
    plus, minus = (1, 2) if sign > 0 else (2, 1)
    high, low = split2(stacked)

    def table(base):
        top = jnp.concatenate([dft[base], dft[base + plus]], axis=1)
        bottom = jnp.concatenate([dft[base + minus], dft[base]], axis=1)
        return jnp.concatenate([top, bottom], axis=0)

    t_high, t_low = table(0), table(3)
    return mm(t_high, high) + mm(t_high, low) + mm(t_low, high)


def labels(positions, length):
    out = jnp.ones(positions.shape, F32)
    for level in range(1, LEVELS + 1):
        out = out + jnp.where(positions < length >> level, 1.0, 0.0)
    return out


def exact_left(signs, parts):
    return sum(mm(signs, part) for part in parts)


def exact_right(parts, signs):
    return sum(mm(part, signs) for part in parts)


def shrink(re, im, thr_ref, haar, last_rows=None):
    n = re.shape[0]
    block = 2**LEVELS
    col_pos = lax.broadcasted_iota(jnp.int32, (n, 1), 0)
    row_pos = lax.broadcasted_iota(jnp.int32, (1, n), 1) % block
    col_label, row_label = labels(col_pos, n), labels(row_pos, block)
    col_scale = jnp.exp2(-0.5 * jnp.minimum(col_label, LEVELS))
    row_scale = jnp.exp2(-0.5 * jnp.minimum(row_label, LEVELS))
    band = jnp.minimum(col_label, row_label)
    limits = jnp.full((n, n), 1.0, F32)
    for level in range(LEVELS):
        limits = jnp.where(band == level + 1, thr_ref[level], limits)
    scale = col_scale * row_scale
    coeffs = []
    for part in (re, im):
        half = exact_left(haar[0], split3(part))
        coeffs.append(exact_right(split3(half), haar[2]) * scale)
    magnitude = jnp.sqrt(coeffs[0] * coeffs[0] + coeffs[1] * coeffs[1])
    factor = jnp.maximum(magnitude - limits, 0.0) / jnp.maximum(magnitude, limits)
    factor = jnp.where(band <= LEVELS, factor, 1.0) * scale
    out = []
    for part in coeffs:
        half = exact_left(haar[1], split3(part * factor))
        if last_rows is None:
            out.append(exact_right(split3(half), haar[3]))
        else:
            out.append(
                sum(
                    lax.dot_general(last_rows, p, (((1,), (1,)), ((), ())), preferred_element_type=F32)
                    for p in split3(half)
                )
            )
    return out


def density_of(ro, n, live_total):
    lane = lax.broadcasted_iota(jnp.int32, (1, ro), 1)
    offset = jnp.abs(lane - ro // 2).astype(F32)
    return (offset + 0.5) * (n / (3.0 * ro * live_total))


def smear(col_table, weighted):
    col = col_table.astype(F32)
    both = [(col * weighted[p : p + 1]).astype(BF16) for p in range(2)]
    return jnp.concatenate(both, axis=0)


def grid_dot(smeared, row_table):
    return lax.dot_general(smeared, row_table, (((1,), (1,)), ((), ())), preferred_element_type=F32)


def adjoint(gridded, dft):
    half = left_dft(gridded, dft, -1)
    n = gridded.shape[0] // 2
    return right_dft(half[:n], half[n:], dft, -1)


def first_kernel(share, first_of, places_of, live_total, pieces, spk_dev, fields, n, *refs):
    piece_refs, refs = refs[:pieces], refs[pieces:]
    dft_ref, rows_s, cols_s, data_out, back_out, slots, grid_s, list_s = refs
    blocks, ro = slots.shape[0] // spk_dev, slots.shape[-1]
    groups = share // GROUP
    for piece, at in zip(piece_refs, places_of(), strict=True):
        for i, place in enumerate(at):
            block = piece[i].astype(F32)
            for depth in range(spk_dev):
                slots[place * spk_dev + depth, 0:fields, :] = block[depth * fields : (depth + 1) * fields]
    taken = jnp.int32(0)
    for block in range(blocks):
        count = jnp.max(slots[block * spk_dev, fields - 1 : fields, :]).astype(jnp.int32)
        for depth in range(spk_dev):
            list_s[taken] = block * spk_dev + depth
            taken = taken + (depth < count).astype(jnp.int32)
    start = first_of()
    density = density_of(ro, n, live_total)
    cells = lax.broadcasted_iota(jnp.int32, (n, ro), 0).astype(F32)
    grid_s[...] = jnp.zeros_like(grid_s)

    def table(at, weights):
        before = jnp.where(at == 0, n - 1.0, at - 1)
        after = jnp.where(at == n - 1, 0.0, at + 1)
        out = jnp.where(cells == after, weights[2:3], 0.0)
        out = jnp.where(cells == at, weights[1:2], out)
        return jnp.where(cells == before, weights[0:1], out).astype(BF16)

    def group_step(group, carry):
        smeared = []
        for j in range(GROUP):
            slot = slots[list_s[start + group * GROUP + j]]
            rows_s[group, :, j * ro : (j + 1) * ro] = table(slot[6:7], slot[0:3])
            col_table = table(slot[7:8], slot[3:6])
            cols_s[group, :, j * ro : (j + 1) * ro] = col_table
            data = slot[8:10]
            data_out[group * GROUP + j] = data
            smeared.append(smear(col_table, -density * data))
        grid_s[...] += grid_dot(jnp.concatenate(smeared, axis=1), rows_s[group])
        return carry

    lax.fori_loop(0, groups, group_step, 0)
    back_out[...] = adjoint(grid_s[...], dft_ref)


def target_of(est_ref, part_refs):
    out = []
    for p in range(2):
        gradient = sum(part[p] for part in part_refs)
        out.append((0.0 if est_ref is None else est_ref[p]) - STEP_SIZE * gradient)
    return out


def step_kernel(share, live_total, n_est, n_parts, *refs):
    thr_ref, refs = refs[0], refs[1:]
    est_ref, refs = refs[0] if n_est else None, refs[n_est:]
    part_refs, refs = refs[:n_parts], refs[n_parts:]
    map_ref, data_ref, dft_ref, haar_ref, rows_s, cols_s, est_out, part_out, weighted_s, grid_s = refs
    groups = share // GROUP
    n = map_ref.shape[1]
    ro = data_ref.shape[-1]
    target = target_of(est_ref, part_refs)
    re, im = shrink(target[0], target[1], thr_ref, haar_ref)
    est_out[0] = re
    est_out[1] = im
    mre, mim = map_ref[0], map_ref[1]
    half = right_dft(mre * re - mim * im, mre * im + mim * re, dft_ref, 1)
    kspace = left_dft(half, dft_ref, 1).astype(BF16)
    density = density_of(ro, n, live_total)
    grid_s[...] = jnp.zeros_like(grid_s)

    def sample_group(group, carry):
        for j in range(GROUP):
            inner = mm(kspace, rows_s[group, :, j * ro : (j + 1) * ro])
            col = cols_s[group, :, j * ro : (j + 1) * ro].astype(F32)
            data = data_ref[group * GROUP + j]
            model = [jnp.sum(inner[p * n : (p + 1) * n] * col, axis=0, keepdims=True) for p in range(2)]
            weighted_s[group * GROUP + j] = density * (jnp.concatenate(model, axis=0) - data)
        return carry

    lax.fori_loop(0, groups, sample_group, 0)

    def grid_group(group, carry):
        smeared = [
            smear(cols_s[group, :, j * ro : (j + 1) * ro], weighted_s[group * GROUP + j]) for j in range(GROUP)
        ]
        grid_s[...] += grid_dot(jnp.concatenate(smeared, axis=1), rows_s[group])
        return carry

    lax.fori_loop(0, groups, grid_group, 0)
    back = adjoint(grid_s[...], dft_ref)
    conj_map(map_ref[0], map_ref[1], back, part_out)


def conj_map(mre, mim, back, part_out):
    n = mre.shape[0]
    bre, bim = back[:n], back[n:]
    part_out[0] = mre * bre + mim * bim
    part_out[1] = mre * bim - mim * bre


def map_kernel(places_of, pieces, *refs):
    piece_refs, (back_ref, map_out, part_out, full) = refs[:pieces], refs[pieces:]
    rows = piece_refs[0].shape[1]
    for piece, at in zip(piece_refs, places_of(), strict=True):
        for i, place in enumerate(at):
            for p in range(2):
                full[p, pl.ds(place * rows, rows), :] = piece[i, :, p, :]
    for p in range(2):
        map_out[p] = full[p].T
    conj_map(map_out[0], map_out[1], back_ref[...], part_out)


def last_kernel(n_parts, rows, mine_of, thr_ref, est_ref, *refs):
    part_refs, (haar_ref, out_ref) = refs[:n_parts], refs[n_parts:]
    n = est_ref.shape[1]
    target = target_of(est_ref, part_refs)
    mine = mine_of()
    pick = lax.broadcasted_iota(jnp.int32, (rows, n), 1) == (
        lax.broadcasted_iota(jnp.int32, (rows, n), 0) + mine * rows
    )
    own = mm(jnp.where(pick, 1.0, 0.0).astype(BF16), haar_ref[2]).astype(BF16)
    re, im = shrink(target[0], target[1], thr_ref, haar_ref, own)
    out_ref[:, 0, :] = re
    out_ref[:, 1, :] = im


def local(coil_maps, kspace_data, interp_weights, sample_bins, spoke_count, thresholds):
    n_tile, n_coil, n_spk = (lax.axis_size(name) for name in ("tile", "coil", "spk"))
    blocks = n_tile * n_spk
    rows, _, n = coil_maps.shape[1:]
    spk_dev, ro = sample_bins.shape
    live_total = blocks * spk_dev // 2
    own_map = coil_maps[0]
    by_core = n_coil == n_spk == 2
    cells = jnp.stack([sample_bins // n, sample_bins % n], axis=1).astype(BF16)
    count = jnp.broadcast_to(spoke_count.astype(BF16)[:, None, None], (spk_dev, 1, ro))
    bundle = jnp.concatenate([interp_weights, cells, kspace_data[0], count], axis=1)
    fields = bundle.shape[1]
    bundle = bundle.reshape(spk_dev * fields, ro)

    if by_core:
        onto = [(0, 2), (3, 1), (1, 0), (2, 3)]
        across = [(1, 2), (2, 1)]
        is_own = lax.axis_index("coil") == lax.axis_index("spk")

        def collect(value):
            near = lax.ppermute(value, ("coil", "spk"), onto)
            far = lax.ppermute(value, ("coil", "spk"), across)
            return jnp.stack([jnp.where(is_own, value, far), near])

        def spread(value):
            out = [value]
            for shift in range(1, n_tile):
                out.append(lax.ppermute(value, "tile", [(i, (i + shift) % n_tile) for i in range(n_tile)]))
            return out

        def places_of():
            tile, coil = lax.axis_index("tile"), lax.axis_index("coil")
            sent = [(tile - shift + n_tile) % n_tile for shift in range(n_tile)]
            return [[at * 2 + coil, at * 2 + 1 - coil] for at in sent]

        pair, map_pair = collect(bundle), collect(own_map)
        spokes = spread(pair)
        spokes, map_pair = lax.optimization_barrier((spokes, map_pair))
        maps = spread(map_pair)
        share, first_of = live_total, lambda: jnp.int32(0)

        def parts_of(part):
            return [part, lax.ppermute(part, "spk", [(0, 1), (1, 0)])]
    else:
        spokes = [lax.all_gather(bundle, ("tile", "spk"), axis=0, tiled=False)]
        maps = [lax.all_gather(own_map, ("tile", "spk"), axis=0, tiled=False)]
        places_of = lambda: [list(range(blocks))]
        share = live_total // blocks
        first_of = lambda: (lax.axis_index("tile") * n_spk + lax.axis_index("spk")) * share

        def parts_of(part):
            return [lax.psum(part, ("tile", "coil", "spk"))]

    groups = share // GROUP
    dft = jnp.asarray(dft_tables(n))
    haar = jnp.asarray(haar_tables(n))
    tables = jax.ShapeDtypeStruct((groups, n, GROUP * ro), BF16)
    image = jax.ShapeDtypeStruct((2, n, n), F32)
    vmem = pl.BlockSpec(memory_space=pltpu.VMEM)
    smem = pl.BlockSpec(memory_space=pltpu.SMEM)
    row_tab, col_tab, data, back = pl.pallas_call(
        functools.partial(first_kernel, share, first_of, places_of, live_total, len(spokes), spk_dev, fields, n),
        out_shape=[tables, tables, jax.ShapeDtypeStruct((share, 2, ro), F32), jax.ShapeDtypeStruct((2 * n, n), F32)],
        in_specs=[vmem] * (len(spokes) + 1),
        out_specs=[vmem] * 4,
        scratch_shapes=[
            pltpu.VMEM((blocks * spk_dev, 16, ro), F32),
            pltpu.VMEM((2 * n, n), F32),
            pltpu.SMEM((blocks * spk_dev + 1,), jnp.int32),
        ],
        compiler_params=PARAMS,
    )(*spokes, dft)
    map_t, part = pl.pallas_call(
        functools.partial(map_kernel, places_of, len(maps)),
        out_shape=[image, image],
        in_specs=[vmem] * (len(maps) + 1),
        out_specs=[vmem, vmem],
        scratch_shapes=[pltpu.VMEM((2, n, n), F32)],
        compiler_params=PARAMS,
    )(*maps, back)
    estimate = []
    parts = parts_of(part)
    for _ in range(1, ITERS):
        inputs = (*estimate, *parts, map_t, data, dft, haar, row_tab, col_tab)
        *estimate, part = pl.pallas_call(
            functools.partial(step_kernel, share, live_total, len(estimate), len(parts)),
            out_shape=[image, image],
            in_specs=[smem] + [vmem] * len(inputs),
            out_specs=[vmem, vmem],
            scratch_shapes=[pltpu.VMEM((share, 2, ro), F32), pltpu.VMEM((2 * n, n), F32)],
            compiler_params=PARAMS,
        )(thresholds, *inputs)
        parts = parts_of(part)
    mine_of = lambda: lax.axis_index("tile") * n_spk + lax.axis_index("spk")
    return pl.pallas_call(
        functools.partial(last_kernel, len(parts), rows, mine_of),
        out_shape=jax.ShapeDtypeStruct((rows, 2, n), F32),
        in_specs=[smem] + [vmem] * (len(parts) + 2),
        out_specs=vmem,
        compiler_params=PARAMS,
    )(thresholds, *estimate, *parts, haar)


def solution(mesh):
    placed = (
        P("coil", ("grp", "tile", "spk"), None, None),
        P("coil", ("grp", "tile", "spk"), None, None),
        P(("grp", "tile", "spk"), None, None),
        P(("grp", "tile", "spk"), None),
        P(("grp", "tile", "spk")),
        P(),
    )
    return jax.shard_map(
        local,
        mesh=mesh,
        in_specs=placed,
        out_specs=P(("grp", "tile", "spk"), None, None),
        check_vma=False,
    )
```

```python
import functools
import math

import jax
import jax.numpy as jnp
import numpy as np
from jax import lax
from jax.experimental import pallas as pl
from jax.experimental.pallas import tpu as pltpu
from jax.sharding import PartitionSpec as P

LEVELS = 3
ITERS = 4
STEP_SIZE = 0.5
GROUP = 8
MARGIN = 8
PARAMS = pltpu.CompilerParams(vmem_limit_bytes=26 * 2**20)
F32 = jnp.float32
BF16 = jnp.bfloat16


def split_host(table):
    high = table.astype(BF16)
    low = (table - high.astype(np.float64)).astype(BF16)
    return high, low


def dft_tables(n):
    idx = np.arange(n)
    angles = 2.0 * math.pi / n * (np.outer(idx, idx) % n)
    scale = 1.0 / math.sqrt(n)
    parts = [np.cos(angles) * scale, np.sin(angles) * scale, -np.sin(angles) * scale]
    pairs = [split_host(part) for part in parts]
    return np.stack([pair[0] for pair in pairs] + [pair[1] for pair in pairs])


def haar_signs(n):
    mat = np.eye(n)
    for level in range(LEVELS):
        span, half = n >> level, n >> (level + 1)
        step = np.eye(n)
        step[:span] = 0.0
        for i in range(half):
            step[i, 2 * i] = step[i, 2 * i + 1] = 1.0
            step[half + i, 2 * i], step[half + i, 2 * i + 1] = 1.0, -1.0
        mat = step @ mat
    return mat


def haar_tables(n):
    col = haar_signs(n)
    row = np.kron(np.eye(n // 2**LEVELS), haar_signs(2**LEVELS))
    return np.stack([col, col.T, row.T, row]).astype(BF16)


def split2(x):
    high = x.astype(BF16)
    return high, (x - high.astype(F32)).astype(BF16)


def mm(a, b):
    return jnp.dot(a, b, preferred_element_type=F32)


def mm_t(a, b):
    return lax.dot_general(a, b, (((1,), (1,)), ((), ())), preferred_element_type=F32)


def joined(parts, axis):
    return jnp.concatenate(parts, axis=axis)


def right_dft(re, im, dft, sign):
    re_h, re_l = split2(re)
    im_h, im_l = split2(im)
    if sign > 0:
        top, bottom = (re_h, im_h, re_l, im_l, re_h, im_h), (im_h, -re_h, im_l, -re_l, im_h, -re_h)
    else:
        top, bottom = (re_h, -im_h, re_l, -im_l, re_h, -im_h), (im_h, re_h, im_l, re_l, im_h, re_h)
    values = joined([joined(top, 1), joined(bottom, 1)], 0)
    return mm(values, joined([dft[0], dft[1], dft[0], dft[1], dft[3], dft[4]], 0))


def left_dft(stacked, dft, sign):
    plus, minus = (1, 2) if sign > 0 else (2, 1)
    high, low = split2(stacked)

    def table(base):
        top = joined([dft[base], dft[base + plus]], 1)
        bottom = joined([dft[base + minus], dft[base]], 1)
        return joined([top, bottom], 0)

    return mm(joined([table(0), table(0), table(3)], 1), joined([high, low, high], 0))


def labels(positions, length):
    out = jnp.ones(positions.shape, F32)
    for level in range(1, LEVELS + 1):
        out = out + jnp.where(positions < length >> level, 1.0, 0.0)
    return out


def shrink(re, im, thr_ref, haar, last_rows=None):
    n = re.shape[0]
    block = 2**LEVELS
    col_pos = lax.broadcasted_iota(jnp.int32, (n, 1), 0)
    row_pos = lax.broadcasted_iota(jnp.int32, (1, n), 1) % block
    col_label, row_label = labels(col_pos, n), labels(row_pos, block)
    col_scale = jnp.exp2(-0.5 * jnp.minimum(col_label, LEVELS))
    row_scale = jnp.exp2(-0.5 * jnp.minimum(row_label, LEVELS))
    band = jnp.minimum(col_label, row_label)
    limits = jnp.full((n, n), 1.0, F32)
    for level in range(LEVELS):
        limits = jnp.where(band == level + 1, thr_ref[level], limits)
    scale = col_scale * row_scale
    half = mm(joined([haar[0]] * 2, 1), joined(split2(joined([re, im], 1)), 0))
    half = joined([half[:, :n], half[:, n:]], 0)
    full = mm(joined(split2(half), 1), joined([haar[2]] * 2, 0))
    coeffs = [full[:n] * scale, full[n:] * scale]
    magnitude = jnp.sqrt(coeffs[0] * coeffs[0] + coeffs[1] * coeffs[1])
    factor = jnp.maximum(magnitude - limits, 0.0) / jnp.maximum(magnitude, limits)
    factor = jnp.where(band <= LEVELS, factor, 1.0) * scale
    kept = joined([coeffs[0] * factor, coeffs[1] * factor], 1)
    half = mm(joined([haar[1]] * 2, 1), joined(split2(kept), 0))
    half = joined([half[:, :n], half[:, n:]], 0)
    if last_rows is None:
        full = mm(joined(split2(half), 1), joined([haar[3]] * 2, 0))
        return full[:n], full[n:]
    full = mm_t(joined([last_rows] * 2, 1), joined(split2(half), 1))
    return full[:, :n], full[:, n:]


def density_of(ro, n, live_total):
    lane = lax.broadcasted_iota(jnp.int32, (1, ro), 1)
    offset = jnp.abs(lane - ro // 2).astype(F32)
    return (offset + 0.5) * (n / (3.0 * ro * live_total))


def smear(col_table, weighted):
    col = col_table.astype(F32)
    return joined([(col * weighted[p : p + 1]).astype(BF16) for p in range(2)], 0)


def grid_group(group, rows_s, cols_s, weighted_s, grid_s):
    span = cols_s.shape[-1]
    for side in range(2):
        smeared = smear(cols_s[group, side], weighted_s[group, side])
        grid_s[side] += mm_t(smeared, rows_s[group, :, side * span : (side + 1) * span])


def to_sides(kspace):
    n = kspace.shape[0] // 2
    mid = n // 2
    low, high = [], []
    for part in (kspace[:n], kspace[n:]):
        low += [part[n - MARGIN :], part[: mid + MARGIN]]
        high += [part[mid - MARGIN :], part[:MARGIN]]
    return joined(low, 0), joined(high, 0)


def from_sides(grid_s):
    span = grid_s.shape[1] // 2
    mid, m = span - 2 * MARGIN, MARGIN
    out = []
    for p in range(2):
        low, high = grid_s[0, p * span : (p + 1) * span], grid_s[1, p * span : (p + 1) * span]
        out += [
            low[m : 2 * m] + high[mid + m :],
            low[2 * m : mid],
            low[mid:] + high[: 2 * m],
            high[2 * m : mid],
            high[mid : mid + m] + low[:m],
        ]
    return joined(out, 0)


def adjoint(gridded, dft):
    half = left_dft(gridded, dft, -1)
    n = gridded.shape[0] // 2
    return right_dft(half[:n], half[n:], dft, -1)


def first_kernel(share, first_of, places_of, live_total, pieces, spk_dev, fields, n, *refs):
    piece_refs, refs = refs[:pieces], refs[pieces:]
    dft_ref, rows_s, cols_s, data_out, back_out, slots, weighted_s, grid_s, list_s = refs
    blocks, ro = slots.shape[0], slots.shape[-1]
    groups, _, _, span = weighted_s.shape
    per_group, half = 2 * span // ro, ro // 2
    for piece, at in zip(piece_refs, places_of(), strict=True):
        for i, place in enumerate(at):
            slots[place] = piece[i].astype(F32)
    taken = jnp.int32(0)
    for block in range(blocks):
        count = jnp.max(slots[block, spk_dev * (fields - 1) :, :]).astype(jnp.int32)
        for depth in range(spk_dev):
            list_s[0, taken] = block
            list_s[1, taken] = depth
            taken = taken + (depth < count).astype(jnp.int32)
    start = first_of()
    density = density_of(ro, n, live_total)
    row_cells = lax.broadcasted_iota(jnp.int32, (n, ro), 0).astype(F32)
    side_rows = n // 2 + 2 * MARGIN
    low_cells = lax.broadcasted_iota(jnp.int32, (side_rows, half), 0) + (n - MARGIN)
    side_cells = [((low_cells + side * (n // 2)) % n).astype(F32) for side in range(2)]
    grid_s[...] = jnp.zeros_like(grid_s)

    def table(cells, at, weights):
        before = jnp.where(at == 0, n - 1.0, at - 1)
        after = jnp.where(at == n - 1, 0.0, at + 1)
        out = jnp.where(cells == after, weights[2], 0.0)
        out = jnp.where(cells == at, weights[1], out)
        return jnp.where(cells == before, weights[0], out).astype(BF16)

    def build(group):
        for j in range(per_group):
            which = start + group * per_group + j
            block, depth = list_s[0, which], list_s[1, which]
            slot = [slots[block, pl.ds(f * spk_dev + depth, 1), :] for f in range(fields - 1)]
            low_first = slot[7][:, 1:2] <= n // 2
            slot = [jnp.where(low_first, f, joined([f[:, half:], f[:, :half]], 1)) for f in slot + [density]]
            rows = table(row_cells, slot[6], slot[0:3])
            for side in range(2):
                lanes = slice(side * half, (side + 1) * half)
                to = slice(j * half, (j + 1) * half)
                rows_s[group, :, side * span + j * half : side * span + (j + 1) * half] = rows[:, lanes]
                cols_s[group, side, :, to] = table(side_cells[side], slot[7][:, lanes], [w[:, lanes] for w in slot[3:6]])
                data = joined([slot[8][:, lanes], slot[9][:, lanes]], 0)
                data_out[group, side, 0:2, to] = data
                data_out[group, side, 2:3, to] = slot[10][:, lanes]
                weighted_s[group, side, :, to] = -slot[10][:, lanes] * data

    build(0)

    def group_step(group, carry):
        grid_group(group - 1, rows_s, cols_s, weighted_s, grid_s)
        build(group)
        return carry

    lax.fori_loop(1, groups, group_step, 0)
    grid_group(groups - 1, rows_s, cols_s, weighted_s, grid_s)
    back_out[...] = adjoint(from_sides(grid_s), dft_ref)


def target_of(est_ref, part_refs):
    out = []
    for p in range(2):
        gradient = sum(part[p] for part in part_refs)
        out.append((0.0 if est_ref is None else est_ref[p]) - STEP_SIZE * gradient)
    return out


def step_kernel(n_est, n_parts, *refs):
    thr_ref, refs = refs[0], refs[1:]
    est_ref, refs = refs[0] if n_est else None, refs[n_est:]
    part_refs, refs = refs[:n_parts], refs[n_parts:]
    map_ref, data_ref, dft_ref, haar_ref, rows_s, cols_s, est_out, part_out, sides_s, weighted_s, grid_s = refs
    groups, _, _, span = weighted_s.shape
    n, rows = map_ref.shape[1], cols_s.shape[2]
    target = target_of(est_ref, part_refs)
    re, im = shrink(target[0], target[1], thr_ref, haar_ref)
    est_out[0] = re
    est_out[1] = im
    mre, mim = map_ref[0], map_ref[1]
    half = right_dft(mre * re - mim * im, mre * im + mim * re, dft_ref, 1)
    for side, values in enumerate(to_sides(left_dft(half, dft_ref, 1))):
        sides_s[side] = values.astype(BF16)
    grid_s[...] = jnp.zeros_like(grid_s)

    def sample_group(group):
        width = min(n, span)
        for side in range(2):
            for at in range(0, span, width):
                lanes = slice(at, at + width)
                inner = mm(sides_s[side], rows_s[group, :, side * span + at : side * span + at + width])
                col = cols_s[group, side, :, lanes].astype(F32)
                model = [jnp.sum(inner[p * rows : (p + 1) * rows] * col, axis=0, keepdims=True) for p in range(2)]
                data = data_ref[group, side, :, lanes]
                weighted_s[group, side, :, lanes] = data[2:3] * (joined(model, 0) - data[0:2])

    sample_group(0)

    def group_step(group, carry):
        grid_group(group - 1, rows_s, cols_s, weighted_s, grid_s)
        sample_group(group)
        return carry

    lax.fori_loop(1, groups, group_step, 0)
    grid_group(groups - 1, rows_s, cols_s, weighted_s, grid_s)
    back = adjoint(from_sides(grid_s), dft_ref)
    conj_map(map_ref[0], map_ref[1], back, part_out)


def conj_map(mre, mim, back, part_out):
    n = mre.shape[0]
    bre, bim = back[:n], back[n:]
    part_out[0] = mre * bre + mim * bim
    part_out[1] = mre * bim - mim * bre


def map_kernel(places_of, pieces, *refs):
    piece_refs, (back_ref, map_out, part_out, full) = refs[:pieces], refs[pieces:]
    rows = piece_refs[0].shape[1]
    for piece, at in zip(piece_refs, places_of(), strict=True):
        for i, place in enumerate(at):
            for p in range(2):
                full[p, pl.ds(place * rows, rows), :] = piece[i, :, p, :]
    for p in range(2):
        map_out[p] = full[p].T
    conj_map(map_out[0], map_out[1], back_ref[...], part_out)


def last_kernel(n_parts, rows, mine_of, thr_ref, est_ref, *refs):
    part_refs, (haar_ref, out_ref) = refs[:n_parts], refs[n_parts:]
    n = est_ref.shape[1]
    target = target_of(est_ref, part_refs)
    mine = mine_of()
    pick = lax.broadcasted_iota(jnp.int32, (rows, n), 1) == (
        lax.broadcasted_iota(jnp.int32, (rows, n), 0) + mine * rows
    )
    own = mm(jnp.where(pick, 1.0, 0.0).astype(BF16), haar_ref[2]).astype(BF16)
    re, im = shrink(target[0], target[1], thr_ref, haar_ref, own)
    out_ref[:, 0, :] = re
    out_ref[:, 1, :] = im


def local(coil_maps, kspace_data, interp_weights, sample_bins, spoke_count, thresholds):
    n_tile, n_coil, n_spk = (lax.axis_size(name) for name in ("tile", "coil", "spk"))
    blocks = n_tile * n_spk
    rows, _, n = coil_maps.shape[1:]
    spk_dev, ro = sample_bins.shape
    live_total = blocks * spk_dev // 2
    own_map = coil_maps[0]
    by_core = n_coil == n_spk == 2
    count = jnp.broadcast_to(spoke_count.astype(BF16)[:, None, None], (1, spk_dev, ro))
    cells = jnp.stack([sample_bins // n, sample_bins % n]).astype(BF16)
    by_field = [jnp.swapaxes(interp_weights, 0, 1), cells, jnp.swapaxes(kspace_data[0], 0, 1), count]
    bundle = jnp.concatenate(by_field, axis=0)
    fields = bundle.shape[0]
    bundle = bundle.reshape(fields * spk_dev, ro)

    if by_core:
        onto = [(0, 2), (3, 1), (1, 0), (2, 3)]
        across = [(1, 2), (2, 1)]
        is_own = lax.axis_index("coil") == lax.axis_index("spk")

        def collect(value):
            near = lax.ppermute(value, ("coil", "spk"), onto)
            far = lax.ppermute(value, ("coil", "spk"), across)
            return jnp.stack([jnp.where(is_own, value, far), near])

        def spread(value):
            out = [value]
            for shift in range(1, n_tile):
                out.append(lax.ppermute(value, "tile", [(i, (i + shift) % n_tile) for i in range(n_tile)]))
            return out

        def places_of():
            tile, coil = lax.axis_index("tile"), lax.axis_index("coil")
            sent = [(tile - shift + n_tile) % n_tile for shift in range(n_tile)]
            return [[at * 2 + coil, at * 2 + 1 - coil] for at in sent]

        pair, map_pair = collect(bundle), collect(own_map)
        spokes = spread(pair)
        spokes, map_pair = lax.optimization_barrier((spokes, map_pair))
        maps = spread(map_pair)
        share, first_of = live_total, lambda: jnp.int32(0)

        def parts_of(part):
            return [part, lax.ppermute(part, "spk", [(0, 1), (1, 0)])]
    else:
        spokes = [lax.all_gather(bundle, ("tile", "spk"), axis=0, tiled=False)]
        maps = [lax.all_gather(own_map, ("tile", "spk"), axis=0, tiled=False)]
        places_of = lambda: [list(range(blocks))]
        share = live_total // blocks
        first_of = lambda: (lax.axis_index("tile") * n_spk + lax.axis_index("spk")) * share

        def parts_of(part):
            return [lax.psum(part, ("tile", "coil", "spk"))]

    per_group = min(GROUP, share)
    groups, span, side_rows = share // per_group, per_group * ro // 2, n // 2 + 2 * MARGIN
    dft = jnp.asarray(dft_tables(n))
    haar = jnp.asarray(haar_tables(n))
    image = jax.ShapeDtypeStruct((2, n, n), F32)
    weighted = pltpu.VMEM((groups, 2, 2, span), F32)
    gridded = pltpu.VMEM((2, 2 * side_rows, n), F32)
    vmem = pl.BlockSpec(memory_space=pltpu.VMEM)
    smem = pl.BlockSpec(memory_space=pltpu.SMEM)
    row_tab, col_tab, data, back = pl.pallas_call(
        functools.partial(first_kernel, share, first_of, places_of, live_total, len(spokes), spk_dev, fields, n),
        out_shape=[
            jax.ShapeDtypeStruct((groups, n, 2 * span), BF16),
            jax.ShapeDtypeStruct((groups, 2, side_rows, span), BF16),
            jax.ShapeDtypeStruct((groups, 2, 3, span), F32),
            jax.ShapeDtypeStruct((2 * n, n), F32),
        ],
        in_specs=[vmem] * (len(spokes) + 1),
        out_specs=[vmem] * 4,
        scratch_shapes=[
            pltpu.VMEM((blocks, fields * spk_dev, ro), F32),
            weighted,
            gridded,
            pltpu.SMEM((2, blocks * spk_dev + 1), jnp.int32),
        ],
        compiler_params=PARAMS,
    )(*spokes, dft)
    map_t, part = pl.pallas_call(
        functools.partial(map_kernel, places_of, len(maps)),
        out_shape=[image, image],
        in_specs=[vmem] * (len(maps) + 1),
        out_specs=[vmem, vmem],
        scratch_shapes=[pltpu.VMEM((2, n, n), F32)],
        compiler_params=PARAMS,
    )(*maps, back)
    estimate = []
    parts = parts_of(part)
    for _ in range(1, ITERS):
        inputs = (*estimate, *parts, map_t, data, dft, haar, row_tab, col_tab)
        *estimate, part = pl.pallas_call(
            functools.partial(step_kernel, len(estimate), len(parts)),
            out_shape=[image, image],
            in_specs=[smem] + [vmem] * len(inputs),
            out_specs=[vmem, vmem],
            scratch_shapes=[pltpu.VMEM((2, 2 * side_rows, n), BF16), weighted, gridded],
            compiler_params=PARAMS,
        )(thresholds, *inputs)
        parts = parts_of(part)
    mine_of = lambda: lax.axis_index("tile") * n_spk + lax.axis_index("spk")
    return pl.pallas_call(
        functools.partial(last_kernel, len(parts), rows, mine_of),
        out_shape=jax.ShapeDtypeStruct((rows, 2, n), F32),
        in_specs=[smem] + [vmem] * (len(parts) + 2),
        out_specs=vmem,
        compiler_params=PARAMS,
    )(thresholds, *estimate, *parts, haar)


def solution(mesh):
    placed = (
        P("coil", ("grp", "tile", "spk"), None, None),
        P("coil", ("grp", "tile", "spk"), None, None),
        P(("grp", "tile", "spk"), None, None),
        P(("grp", "tile", "spk"), None),
        P(("grp", "tile", "spk")),
        P(),
    )
    return jax.shard_map(
        local,
        mesh=mesh,
        in_specs=placed,
        out_specs=P(("grp", "tile", "spk"), None, None),
        check_vma=False,
    )
```

```python
import functools
import math

import jax
import jax.numpy as jnp
import numpy as np
from jax import lax
from jax.experimental import pallas as pl
from jax.experimental.pallas import tpu as pltpu
from jax.sharding import PartitionSpec as P

LEVELS = 3
ITERS = 4
STEP_SIZE = 0.5
GROUP = 8
MARGIN = 8
PARAMS = pltpu.CompilerParams(vmem_limit_bytes=26 * 2**20)
F32 = jnp.float32
BF16 = jnp.bfloat16


def split_host(table):
    high = table.astype(BF16)
    low = (table - high.astype(np.float64)).astype(BF16)
    return high, low


def dft_tables(n):
    idx = np.arange(n)
    angles = 2.0 * math.pi / n * (np.outer(idx, idx) % n)
    scale = 1.0 / math.sqrt(n)
    parts = [np.cos(angles) * scale, np.sin(angles) * scale, -np.sin(angles) * scale]
    pairs = [split_host(part) for part in parts]
    return np.stack([pair[0] for pair in pairs] + [pair[1] for pair in pairs])


def haar_signs(n):
    mat = np.eye(n)
    for level in range(LEVELS):
        span, half = n >> level, n >> (level + 1)
        step = np.eye(n)
        step[:span] = 0.0
        for i in range(half):
            step[i, 2 * i] = step[i, 2 * i + 1] = 1.0
            step[half + i, 2 * i], step[half + i, 2 * i + 1] = 1.0, -1.0
        mat = step @ mat
    return mat


def haar_tables(n):
    col = haar_signs(n)
    row = np.kron(np.eye(n // 2**LEVELS), haar_signs(2**LEVELS))
    return np.stack([col, col.T, row.T, row]).astype(BF16)


def split2(x):
    high = x.astype(BF16)
    return high, (x - high.astype(F32)).astype(BF16)


def mm(a, b):
    return jnp.dot(a, b, preferred_element_type=F32)


def mm_t(a, b):
    return lax.dot_general(a, b, (((1,), (1,)), ((), ())), preferred_element_type=F32)


def joined(parts, axis):
    return jnp.concatenate(parts, axis=axis)


def right_dft(re, im, dft, sign):
    re_h, re_l = split2(re)
    im_h, im_l = split2(im)
    if sign > 0:
        top, bottom = (re_h, im_h, re_l, im_l, re_h, im_h), (im_h, -re_h, im_l, -re_l, im_h, -re_h)
    else:
        top, bottom = (re_h, -im_h, re_l, -im_l, re_h, -im_h), (im_h, re_h, im_l, re_l, im_h, re_h)
    values = joined([joined(top, 1), joined(bottom, 1)], 0)
    return mm(values, joined([dft[0], dft[1], dft[0], dft[1], dft[3], dft[4]], 0))


def left_dft(stacked, dft, sign):
    plus, minus = (1, 2) if sign > 0 else (2, 1)
    high, low = split2(stacked)

    def table(base):
        top = joined([dft[base], dft[base + plus]], 1)
        bottom = joined([dft[base + minus], dft[base]], 1)
        return joined([top, bottom], 0)

    return mm(joined([table(0), table(0), table(3)], 1), joined([high, low, high], 0))


def labels(positions, length):
    out = jnp.ones(positions.shape, F32)
    for level in range(1, LEVELS + 1):
        out = out + jnp.where(positions < length >> level, 1.0, 0.0)
    return out


def shrink(re, im, thr_ref, haar, last_rows=None):
    n = re.shape[0]
    block = 2**LEVELS
    col_pos = lax.broadcasted_iota(jnp.int32, (n, 1), 0)
    row_pos = lax.broadcasted_iota(jnp.int32, (1, n), 1) % block
    col_label, row_label = labels(col_pos, n), labels(row_pos, block)
    col_scale = jnp.exp2(-0.5 * jnp.minimum(col_label, LEVELS))
    row_scale = jnp.exp2(-0.5 * jnp.minimum(row_label, LEVELS))
    band = jnp.minimum(col_label, row_label)
    limits = jnp.full((n, n), 1.0, F32)
    for level in range(LEVELS):
        limits = jnp.where(band == level + 1, thr_ref[level : level + 1, :], limits)
    scale = col_scale * row_scale
    half = mm(joined([haar[0]] * 2, 1), joined(split2(joined([re, im], 1)), 0))
    half = joined([half[:, :n], half[:, n:]], 0)
    full = mm(joined(split2(half), 1), joined([haar[2]] * 2, 0))
    coeffs = [full[:n] * scale, full[n:] * scale]
    magnitude = jnp.sqrt(coeffs[0] * coeffs[0] + coeffs[1] * coeffs[1])
    factor = jnp.maximum(magnitude - limits, 0.0) / jnp.maximum(magnitude, limits)
    factor = jnp.where(band <= LEVELS, factor, 1.0) * scale
    kept = joined([coeffs[0] * factor, coeffs[1] * factor], 1)
    half = mm(joined([haar[1]] * 2, 1), joined(split2(kept), 0))
    half = joined([half[:, :n], half[:, n:]], 0)
    if last_rows is None:
        full = mm(joined(split2(half), 1), joined([haar[3]] * 2, 0))
        return full[:n], full[n:]
    full = mm_t(joined([last_rows] * 2, 1), joined(split2(half), 1))
    return full[:, :n], full[:, n:]


def density_of(ro, n, live_total):
    lane = lax.broadcasted_iota(jnp.int32, (1, ro), 1)
    offset = jnp.abs(lane - ro // 2).astype(F32)
    return (offset + 0.5) * (n / (3.0 * ro * live_total))


def smear(col_table, weighted):
    col = col_table.astype(F32)
    return joined([(col * weighted[p : p + 1]).astype(BF16) for p in range(2)], 0)


def grid_group(group, rows_s, cols_s, weighted_s, grid_s):
    span = cols_s.shape[-1]
    for side in range(2):
        smeared = smear(cols_s[group, side], weighted_s[group, side])
        grid_s[side] += mm_t(smeared, rows_s[group, :, side * span : (side + 1) * span])


def to_sides(kspace):
    n = kspace.shape[0] // 2
    mid = n // 2
    low, high = [], []
    for part in (kspace[:n], kspace[n:]):
        low += [part[n - MARGIN :], part[: mid + MARGIN]]
        high += [part[mid - MARGIN :], part[:MARGIN]]
    return joined(low, 0), joined(high, 0)


def from_sides(grid_s):
    span = grid_s.shape[1] // 2
    mid, m = span - 2 * MARGIN, MARGIN
    out = []
    for p in range(2):
        low, high = grid_s[0, p * span : (p + 1) * span], grid_s[1, p * span : (p + 1) * span]
        out += [
            low[m : 2 * m] + high[mid + m :],
            low[2 * m : mid],
            low[mid:] + high[: 2 * m],
            high[2 * m : mid],
            high[mid : mid + m] + low[:m],
        ]
    return joined(out, 0)


def adjoint(gridded, dft):
    half = left_dft(gridded, dft, -1)
    n = gridded.shape[0] // 2
    return right_dft(half[:n], half[n:], dft, -1)


def pack_kernel(data_ref, weight_ref, bins_ref, count_ref, out_ref):
    slots, ro = bins_ref.shape
    n = ro
    bins = bins_ref[...]
    fields = [data_ref[:, p, :].astype(F32) for p in range(2)]
    fields += [weight_ref[i].astype(F32) for i in range(weight_ref.shape[0])]
    fields += [(bins // n).astype(F32), (bins % n).astype(F32)]
    fields.append(jnp.full((slots, ro), count_ref[0].astype(F32)))
    out_ref[...] = joined(fields, 0).astype(BF16)


def join_kernel(data_rows, *refs):
    pieces, (data_out, spoke_out) = refs[:-2], refs[-2:]
    for i, piece in enumerate(pieces):
        data_out[i] = piece[:data_rows]
        spoke_out[i] = piece[data_rows:]


def stack_kernel(*refs):
    for i, piece in enumerate(refs[:-1]):
        refs[-1][i] = piece[...]


def constants_kernel(thr_ref, dft_ref, haar_ref, thr_out, dft_out, haar_out):
    for level in range(LEVELS):
        thr_out[level : level + 1, :] = jnp.full((1, thr_out.shape[1]), thr_ref[level])
    dft_out[...] = dft_ref[...]
    haar_out[...] = haar_ref[...]


def live_list(slots, spk_dev, list_s):
    taken = jnp.int32(0)
    for block in range(slots.shape[0]):
        count = jnp.max(slots[block, slots.shape[1] - spk_dev :, :]).astype(jnp.int32)
        for depth in range(spk_dev):
            list_s[0, taken] = block
            list_s[1, taken] = depth
            taken = taken + (depth < count).astype(jnp.int32)


def table_kernel(first_of, blocks_of, live_total, pieces, spk_dev, n, *refs):
    spoke_refs, refs = refs[:pieces], refs[pieces:]
    rows_s, cols_s, flags_out, list_out, slots = refs
    ro = slots.shape[-1]
    groups, _, _, span = flags_out.shape
    per_group, half = 2 * span // ro, ro // 2
    for place, value in blocks_of(spoke_refs):
        slots[place] = value.astype(F32)
    live_list(slots, spk_dev, list_out)
    start = first_of()
    density = density_of(ro, n, live_total)
    row_cells = lax.broadcasted_iota(jnp.int32, (n, ro), 0).astype(F32)
    side_rows = n // 2 + 2 * MARGIN
    low_cells = lax.broadcasted_iota(jnp.int32, (side_rows, half), 0) + (n - MARGIN)
    side_cells = [((low_cells + side * (n // 2)) % n).astype(F32) for side in range(2)]

    def table(cells, at, weights):
        before = jnp.where(at == 0, n - 1.0, at - 1)
        after = jnp.where(at == n - 1, 0.0, at + 1)
        out = jnp.where(cells == after, weights[2], 0.0)
        out = jnp.where(cells == at, weights[1], out)
        return jnp.where(cells == before, weights[0], out).astype(BF16)

    def build(group, carry):
        for j in range(per_group):
            which = start + group * per_group + j
            block, depth = list_out[0, which], list_out[1, which]
            slot = [slots[block, pl.ds(f * spk_dev + depth, 1), :] for f in range(8)]
            low_first = slot[7][:, 1:2] <= n // 2
            slot = slot + [density, jnp.where(low_first, jnp.ones_like(density), 0.0)]
            slot = [jnp.where(low_first, f, joined([f[:, half:], f[:, :half]], 1)) for f in slot]
            rows = table(row_cells, slot[6], slot[0:3])
            for side in range(2):
                lanes = slice(side * half, (side + 1) * half)
                to = slice(j * half, (j + 1) * half)
                rows_s[group, :, side * span + j * half : side * span + (j + 1) * half] = rows[:, lanes]
                cols_s[group, side, :, to] = table(side_cells[side], slot[7][:, lanes], [w[:, lanes] for w in slot[3:6]])
                flags_out[group, side, :, to] = joined([f[:, lanes] for f in slot[8:10]], 0)
        return carry

    lax.fori_loop(0, groups, build, 0)


def first_kernel(first_of, blocks_of, pieces, spk_dev, *refs):
    data_refs, refs = refs[:pieces], refs[pieces:]
    list_ref, flags_ref, rows_s, cols_s, dft_ref, data_out, back_out, slots, weighted_s, grid_s = refs
    ro = slots.shape[-1]
    groups, _, _, span = weighted_s.shape
    per_group, half = 2 * span // ro, ro // 2
    for place, value in blocks_of(data_refs):
        slots[place] = value.astype(F32)
    start = first_of()
    grid_s[...] = jnp.zeros_like(grid_s)

    def pick(group):
        for j in range(per_group):
            which = start + group * per_group + j
            block, depth = list_ref[0, which], list_ref[1, which]
            data = joined([slots[block, pl.ds(p * spk_dev + depth, 1), :] for p in range(2)], 0)
            to = slice(j * half, (j + 1) * half)
            low_first = flags_ref[group, 0, 1:2, to] > 0.5
            halves = [data[:, :half], data[:, half:]]
            for side in range(2):
                mine = jnp.where(low_first, halves[side], halves[1 - side])
                density = flags_ref[group, side, 0:1, to]
                data_out[group, side, 0:2, to] = mine
                data_out[group, side, 2:3, to] = density
                weighted_s[group, side, :, to] = -density * mine

    pick(0)

    def group_step(group, carry):
        grid_group(group - 1, rows_s, cols_s, weighted_s, grid_s)
        pick(group)
        return carry

    lax.fori_loop(1, groups, group_step, 0)
    grid_group(groups - 1, rows_s, cols_s, weighted_s, grid_s)
    back_out[...] = adjoint(from_sides(grid_s), dft_ref)


def target_of(est_ref, part_refs):
    out = []
    for p in range(2):
        gradient = sum(part[p] for part in part_refs)
        out.append((0.0 if est_ref is None else est_ref[p]) - STEP_SIZE * gradient)
    return out


def step_kernel(n_est, n_parts, *refs):
    thr_ref, refs = refs[0], refs[1:]
    est_ref, refs = refs[0] if n_est else None, refs[n_est:]
    part_refs, refs = refs[:n_parts], refs[n_parts:]
    map_ref, data_ref, dft_ref, haar_ref, rows_s, cols_s, est_out, part_out, sides_s, weighted_s, grid_s = refs
    groups, _, _, span = weighted_s.shape
    n, rows = map_ref.shape[1], cols_s.shape[2]
    target = target_of(est_ref, part_refs)
    re, im = shrink(target[0], target[1], thr_ref, haar_ref)
    est_out[0] = re
    est_out[1] = im
    mre, mim = map_ref[0], map_ref[1]
    half = right_dft(mre * re - mim * im, mre * im + mim * re, dft_ref, 1)
    for side, values in enumerate(to_sides(left_dft(half, dft_ref, 1))):
        sides_s[side] = values.astype(BF16)
    grid_s[...] = jnp.zeros_like(grid_s)

    def sample_group(group):
        width = min(n, span)
        for side in range(2):
            for at in range(0, span, width):
                lanes = slice(at, at + width)
                inner = mm(sides_s[side], rows_s[group, :, side * span + at : side * span + at + width])
                col = cols_s[group, side, :, lanes].astype(F32)
                model = [jnp.sum(inner[p * rows : (p + 1) * rows] * col, axis=0, keepdims=True) for p in range(2)]
                data = data_ref[group, side, :, lanes]
                weighted_s[group, side, :, lanes] = data[2:3] * (joined(model, 0) - data[0:2])

    sample_group(0)

    def group_step(group, carry):
        grid_group(group - 1, rows_s, cols_s, weighted_s, grid_s)
        sample_group(group)
        return carry

    lax.fori_loop(1, groups, group_step, 0)
    grid_group(groups - 1, rows_s, cols_s, weighted_s, grid_s)
    back = adjoint(from_sides(grid_s), dft_ref)
    conj_map(map_ref[0], map_ref[1], back, part_out)


def conj_map(mre, mim, back, part_out):
    n = mre.shape[0]
    bre, bim = back[:n], back[n:]
    part_out[0] = mre * bre + mim * bim
    part_out[1] = mre * bim - mim * bre


def map_kernel(blocks_of, pieces, *refs):
    piece_refs, (back_ref, map_out, part_out, full) = refs[:pieces], refs[pieces:]
    rows = piece_refs[0].shape[1]
    for place, value in blocks_of(piece_refs):
        for p in range(2):
            full[p, pl.ds(place * rows, rows), :] = value[:, p, :]
    for p in range(2):
        map_out[p] = full[p].T
    conj_map(map_out[0], map_out[1], back_ref[...], part_out)


def last_kernel(n_parts, rows, mine_of, thr_ref, est_ref, *refs):
    part_refs, (haar_ref, out_ref) = refs[:n_parts], refs[n_parts:]
    n = est_ref.shape[1]
    target = target_of(est_ref, part_refs)
    mine = mine_of()
    pick = lax.broadcasted_iota(jnp.int32, (rows, n), 1) == (
        lax.broadcasted_iota(jnp.int32, (rows, n), 0) + mine * rows
    )
    own = mm(jnp.where(pick, 1.0, 0.0).astype(BF16), haar_ref[2]).astype(BF16)
    re, im = shrink(target[0], target[1], thr_ref, haar_ref, own)
    out_ref[:, 0, :] = re
    out_ref[:, 1, :] = im


def local(coil_maps, kspace_data, interp_weights, sample_bins, spoke_count, thresholds):
    n_tile, n_coil, n_spk = (lax.axis_size(name) for name in ("tile", "coil", "spk"))
    blocks = n_tile * n_spk
    rows, _, n = coil_maps.shape[1:]
    spk_dev, ro = sample_bins.shape
    live_total = blocks * spk_dev // 2
    own_map = coil_maps[0]
    by_core = n_coil == n_spk == 2
    vmem = pl.BlockSpec(memory_space=pltpu.VMEM)
    smem = pl.BlockSpec(memory_space=pltpu.SMEM)
    data_rows, fields = 2 * spk_dev, 11
    spoke_rows = fields * spk_dev - data_rows
    bundle = pl.pallas_call(
        pack_kernel,
        out_shape=jax.ShapeDtypeStruct((fields * spk_dev, ro), BF16),
        in_specs=[vmem, vmem, vmem, smem],
        out_specs=vmem,
        compiler_params=PARAMS,
    )(kspace_data[0], jnp.swapaxes(interp_weights, 0, 1), sample_bins, spoke_count)

    dft, haar = dft_tables(n), haar_tables(n)
    limits, dft, haar = pl.pallas_call(
        constants_kernel,
        out_shape=[
            jax.ShapeDtypeStruct((LEVELS, n), F32),
            jax.ShapeDtypeStruct(dft.shape, BF16),
            jax.ShapeDtypeStruct(haar.shape, BF16),
        ],
        in_specs=[smem, vmem, vmem],
        out_specs=[vmem] * 3,
        compiler_params=PARAMS,
    )(thresholds, jnp.asarray(dft), jnp.asarray(haar))

    if by_core:
        onto = [(0, 2), (3, 1), (1, 0), (2, 3)]
        across = [(1, 2), (2, 1)]

        def spread(value):
            out = [value]
            for shift in range(1, n_tile):
                out.append(lax.ppermute(value, "tile", [(i, (i + shift) % n_tile) for i in range(n_tile)]))
            return out

        def to_coil(value):
            return [value, lax.ppermute(value, ("coil", "spk"), across), lax.ppermute(value, ("coil", "spk"), onto)]

        def senders():
            tile = lax.axis_index("tile")
            return [(tile - shift + n_tile) % n_tile for shift in range(n_tile)]

        def spoke_blocks(refs):
            own, other = refs
            spk = lax.axis_index("spk")
            for i, at in enumerate(senders()):
                yield at * 2 + spk, own[i]
                yield at * 2 + 1 - spk, other[i]

        def coil_blocks(refs):
            own, far, near = refs
            coil = lax.axis_index("coil")
            is_own = coil == lax.axis_index("spk")
            for i, at in enumerate(senders()):
                yield at * 2 + coil, jnp.where(is_own, own[i], far[i])
                yield at * 2 + 1 - coil, near[i]

        swap = [(0, 1), (1, 0)]
        pieces = spread(bundle)
        own_map, bundle = lax.optimization_barrier((own_map, bundle))
        map_pieces = spread(own_map)
        pieces, limits, dft, haar = lax.optimization_barrier((pieces, limits, dft, haar))
        own_data, own_spokes = pl.pallas_call(
            functools.partial(join_kernel, data_rows),
            out_shape=[
                jax.ShapeDtypeStruct((n_tile, data_rows, ro), BF16),
                jax.ShapeDtypeStruct((n_tile, spoke_rows, ro), BF16),
            ],
            in_specs=[vmem] * n_tile,
            out_specs=[vmem] * 2,
            compiler_params=PARAMS,
        )(*pieces)
        other_spokes = lax.ppermute(own_spokes, "spk", swap)
        coil_data = to_coil(own_data)
        map_pieces, own_spokes, own_data = lax.optimization_barrier((map_pieces, own_spokes, own_data))
        own_maps = pl.pallas_call(
            stack_kernel,
            out_shape=jax.ShapeDtypeStruct((n_tile, *own_map.shape), F32),
            in_specs=[vmem] * n_tile,
            out_specs=vmem,
            compiler_params=PARAMS,
        )(*map_pieces)
        maps = to_coil(own_maps)
        spokes = [own_spokes, other_spokes]
        share, first_of = live_total, lambda: jnp.int32(0)

        def parts_of(part):
            return [part, lax.ppermute(part, "spk", swap)]
    else:
        def gather(value):
            return [lax.all_gather(value, ("tile", "spk"), axis=0, tiled=False)]

        def spoke_blocks(refs):
            return ((i, refs[0][i]) for i in range(blocks))

        coil_blocks = spoke_blocks
        spokes, coil_data, maps = gather(bundle[data_rows:]), gather(bundle[:data_rows]), gather(own_map)
        share = live_total // blocks
        first_of = lambda: (lax.axis_index("tile") * n_spk + lax.axis_index("spk")) * share

        def parts_of(part):
            return [lax.psum(part, ("tile", "coil", "spk"))]

    per_group = min(GROUP, share)
    groups, span, side_rows = share // per_group, per_group * ro // 2, n // 2 + 2 * MARGIN
    image = jax.ShapeDtypeStruct((2, n, n), F32)
    weighted = pltpu.VMEM((groups, 2, 2, span), F32)
    gridded = pltpu.VMEM((2, 2 * side_rows, n), F32)
    row_tab, col_tab, flags, live = pl.pallas_call(
        functools.partial(table_kernel, first_of, spoke_blocks, live_total, len(spokes), spk_dev, n),
        out_shape=[
            jax.ShapeDtypeStruct((groups, n, 2 * span), BF16),
            jax.ShapeDtypeStruct((groups, 2, side_rows, span), BF16),
            jax.ShapeDtypeStruct((groups, 2, 2, span), F32),
            jax.ShapeDtypeStruct((2, blocks * spk_dev + 1), jnp.int32),
        ],
        in_specs=[vmem] * len(spokes),
        out_specs=[vmem, vmem, vmem, smem],
        scratch_shapes=[pltpu.VMEM((blocks, spoke_rows, ro), F32)],
        compiler_params=PARAMS,
    )(*spokes)
    data, back = pl.pallas_call(
        functools.partial(first_kernel, first_of, coil_blocks, len(coil_data), spk_dev),
        out_shape=[
            jax.ShapeDtypeStruct((groups, 2, 3, span), F32),
            jax.ShapeDtypeStruct((2 * n, n), F32),
        ],
        in_specs=[vmem] * len(coil_data) + [smem] + [vmem] * 4,
        out_specs=[vmem] * 2,
        scratch_shapes=[pltpu.VMEM((blocks, data_rows, ro), F32), weighted, gridded],
        compiler_params=PARAMS,
    )(*coil_data, live, flags, row_tab, col_tab, dft)
    map_t, part = pl.pallas_call(
        functools.partial(map_kernel, coil_blocks, len(maps)),
        out_shape=[image, image],
        in_specs=[vmem] * (len(maps) + 1),
        out_specs=[vmem, vmem],
        scratch_shapes=[pltpu.VMEM((2, n, n), F32)],
        compiler_params=PARAMS,
    )(*maps, back)
    estimate = []
    parts = parts_of(part)
    for _ in range(1, ITERS):
        inputs = (*estimate, *parts, map_t, data, dft, haar, row_tab, col_tab)
        *estimate, part = pl.pallas_call(
            functools.partial(step_kernel, len(estimate), len(parts)),
            out_shape=[image, image],
            in_specs=[vmem] * (len(inputs) + 1),
            out_specs=[vmem, vmem],
            scratch_shapes=[pltpu.VMEM((2, 2 * side_rows, n), BF16), weighted, gridded],
            compiler_params=PARAMS,
        )(limits, *inputs)
        parts = parts_of(part)
    mine_of = lambda: lax.axis_index("tile") * n_spk + lax.axis_index("spk")
    return pl.pallas_call(
        functools.partial(last_kernel, len(parts), rows, mine_of),
        out_shape=jax.ShapeDtypeStruct((rows, 2, n), F32),
        in_specs=[vmem] * (len(parts) + 3),
        out_specs=vmem,
        compiler_params=PARAMS,
    )(limits, *estimate, *parts, haar)


def solution(mesh):
    placed = (
        P("coil", ("grp", "tile", "spk"), None, None),
        P("coil", ("grp", "tile", "spk"), None, None),
        P(("grp", "tile", "spk"), None, None),
        P(("grp", "tile", "spk"), None),
        P(("grp", "tile", "spk")),
        P(),
    )

    return jax.shard_map(
        local,
        mesh=mesh,
        in_specs=placed,
        out_specs=P(("grp", "tile", "spk"), None, None),
        check_vma=False,
    )
```

```python
import functools
import math

import jax
import jax.numpy as jnp
import numpy as np
from jax import lax
from jax.experimental import pallas as pl
from jax.experimental.pallas import tpu as pltpu
from jax.sharding import PartitionSpec as P

LEVELS = 3
ITERS = 4
STEP_SIZE = 0.5
GROUP = 8
MARGIN = 8
PARAMS = pltpu.CompilerParams(vmem_limit_bytes=26 * 2**20)
F32 = jnp.float32
BF16 = jnp.bfloat16


def split_host(table):
    high = table.astype(BF16)
    low = (table - high.astype(np.float64)).astype(BF16)
    return high, low


def dft_tables(n):
    idx = np.arange(n)
    angles = 2.0 * math.pi / n * (np.outer(idx, idx) % n)
    scale = 1.0 / math.sqrt(n)
    parts = [np.cos(angles) * scale, np.sin(angles) * scale, -np.sin(angles) * scale]
    pairs = [split_host(part) for part in parts]
    return np.stack([pair[0] for pair in pairs] + [pair[1] for pair in pairs])


def haar_signs(n):
    mat = np.eye(n)
    for level in range(LEVELS):
        span, half = n >> level, n >> (level + 1)
        step = np.eye(n)
        step[:span] = 0.0
        for i in range(half):
            step[i, 2 * i] = step[i, 2 * i + 1] = 1.0
            step[half + i, 2 * i], step[half + i, 2 * i + 1] = 1.0, -1.0
        mat = step @ mat
    return mat


def haar_tables(n):
    col = haar_signs(n)
    row = np.kron(np.eye(n // 2**LEVELS), haar_signs(2**LEVELS))
    return np.stack([col, col.T, row.T, row]).astype(BF16)


def split2(x):
    high = x.astype(BF16)
    return high, (x - high.astype(F32)).astype(BF16)


def mm(a, b):
    return jnp.dot(a, b, preferred_element_type=F32)


def mm_t(a, b):
    return lax.dot_general(a, b, (((1,), (1,)), ((), ())), preferred_element_type=F32)


def joined(parts, axis):
    return jnp.concatenate(parts, axis=axis)


def right_dft(re, im, dft, sign):
    re_h, re_l = split2(re)
    im_h, im_l = split2(im)
    if sign > 0:
        top, bottom = (re_h, im_h, re_l, im_l, re_h, im_h), (im_h, -re_h, im_l, -re_l, im_h, -re_h)
    else:
        top, bottom = (re_h, -im_h, re_l, -im_l, re_h, -im_h), (im_h, re_h, im_l, re_l, im_h, re_h)
    values = joined([joined(top, 1), joined(bottom, 1)], 0)
    return mm(values, joined([dft[0], dft[1], dft[0], dft[1], dft[3], dft[4]], 0))


def left_dft(stacked, dft, sign):
    plus, minus = (1, 2) if sign > 0 else (2, 1)
    high, low = split2(stacked)

    def table(base):
        top = joined([dft[base], dft[base + plus]], 1)
        bottom = joined([dft[base + minus], dft[base]], 1)
        return joined([top, bottom], 0)

    return mm(joined([table(0), table(0), table(3)], 1), joined([high, low, high], 0))


def labels(positions, length):
    out = jnp.ones(positions.shape, F32)
    for level in range(1, LEVELS + 1):
        out = out + jnp.where(positions < length >> level, 1.0, 0.0)
    return out


def shrink(re, im, thr_ref, const, last_rows=None):
    n = re.shape[0]
    block = 2**LEVELS
    col_pos = lax.broadcasted_iota(jnp.int32, (n, 1), 0)
    row_pos = lax.broadcasted_iota(jnp.int32, (1, n), 1) % block
    col_label, row_label = labels(col_pos, n), labels(row_pos, block)
    col_scale = jnp.exp2(-0.5 * jnp.minimum(col_label, LEVELS))
    row_scale = jnp.exp2(-0.5 * jnp.minimum(row_label, LEVELS))
    band = jnp.minimum(col_label, row_label)
    limits = jnp.full((n, n), 1.0, F32)
    for level in range(LEVELS):
        limits = jnp.where(band == level + 1, thr_ref[level : level + 1, :], limits)
    scale = col_scale * row_scale
    half = mm(joined([const[6]] * 2, 1), joined(split2(joined([re, im], 1)), 0))
    half = joined([half[:, :n], half[:, n:]], 0)
    full = mm(joined(split2(half), 1), joined([const[8]] * 2, 0))
    coeffs = [full[:n] * scale, full[n:] * scale]
    magnitude = jnp.sqrt(coeffs[0] * coeffs[0] + coeffs[1] * coeffs[1])
    factor = jnp.maximum(magnitude - limits, 0.0) / jnp.maximum(magnitude, limits)
    factor = jnp.where(band <= LEVELS, factor, 1.0) * scale
    kept = joined([coeffs[0] * factor, coeffs[1] * factor], 1)
    half = mm(joined([const[7]] * 2, 1), joined(split2(kept), 0))
    half = joined([half[:, :n], half[:, n:]], 0)
    if last_rows is None:
        full = mm(joined(split2(half), 1), joined([const[9]] * 2, 0))
        return full[:n], full[n:]
    full = mm_t(joined([last_rows] * 2, 1), joined(split2(half), 1))
    return full[:, :n], full[:, n:]


def density_of(ro, n, live_total):
    lane = lax.broadcasted_iota(jnp.int32, (1, ro), 1)
    offset = jnp.abs(lane - ro // 2).astype(F32)
    return (offset + 0.5) * (n / (3.0 * ro * live_total))


def smear(col_table, weighted):
    col = col_table.astype(F32)
    return joined([(col * weighted[p : p + 1]).astype(BF16) for p in range(2)], 0)


def grid_group(group, rows_s, cols_s, weighted_s, grid_s):
    span = cols_s.shape[-1]
    for side in range(2):
        smeared = smear(cols_s[group, side], weighted_s[group, side])
        grid_s[side] += mm_t(smeared, rows_s[group, :, side * span : (side + 1) * span])


def to_sides(kspace):
    n = kspace.shape[0] // 2
    mid = n // 2
    low, high = [], []
    for part in (kspace[:n], kspace[n:]):
        low += [part[n - MARGIN :], part[: mid + MARGIN]]
        high += [part[mid - MARGIN :], part[:MARGIN]]
    return joined(low, 0), joined(high, 0)


def from_sides(grid_s):
    span = grid_s.shape[1] // 2
    mid, m = span - 2 * MARGIN, MARGIN
    out = []
    for p in range(2):
        low, high = grid_s[0, p * span : (p + 1) * span], grid_s[1, p * span : (p + 1) * span]
        out += [
            low[m : 2 * m] + high[mid + m :],
            low[2 * m : mid],
            low[mid:] + high[: 2 * m],
            high[2 * m : mid],
            high[mid : mid + m] + low[:m],
        ]
    return joined(out, 0)


def adjoint(gridded, dft):
    half = left_dft(gridded, dft, -1)
    n = gridded.shape[0] // 2
    return right_dft(half[:n], half[n:], dft, -1)


def pack_kernel(data_ref, weight_ref, bins_ref, count_ref, out_ref):
    slots, ro = bins_ref.shape
    n = ro
    bins = bins_ref[...]
    fields = [data_ref[:, p, :].astype(F32) for p in range(2)]
    fields += [weight_ref[i].astype(F32) for i in range(weight_ref.shape[0])]
    fields += [(bins // n).astype(F32), (bins % n).astype(F32)]
    fields.append(jnp.full((slots, ro), count_ref[0].astype(F32)))
    out_ref[...] = joined(fields, 0).astype(BF16)


def join_kernel(data_rows, *refs):
    pieces, (data_out, spoke_out) = refs[:-2], refs[-2:]
    for i, piece in enumerate(pieces):
        data_out[i] = piece[:data_rows]
        spoke_out[i] = piece[data_rows:]


def stack_kernel(*refs):
    for i, piece in enumerate(refs[:-1]):
        refs[-1][i] = piece[...]


def constants_kernel(thr_ref, const_ref, thr_out, const_out):
    for level in range(LEVELS):
        thr_out[level : level + 1, :] = jnp.full((1, thr_out.shape[1]), thr_ref[level])
    const_out[...] = const_ref[...]


def first_kernel(first_of, spoke_blocks, coil_blocks, live_total, counts, spk_dev, n, *refs):
    spoke_refs, data_refs, refs = refs[: counts[0]], refs[counts[0] : sum(counts)], refs[sum(counts) :]
    const_ref, rows_s, cols_s, data_out, back_out, slots, weighted_s, grid_s, list_s = refs
    spoke_rows = slots.shape[1] - 2 * spk_dev
    ro = slots.shape[-1]
    groups, _, _, span = weighted_s.shape
    per_group, half = 2 * span // ro, ro // 2
    for place, value in spoke_blocks(spoke_refs):
        slots[place, 0:spoke_rows] = value.astype(F32)
    for place, value in coil_blocks(data_refs):
        slots[place, spoke_rows:] = value.astype(F32)
    taken = jnp.int32(0)
    for block in range(slots.shape[0]):
        count = jnp.max(slots[block, spoke_rows - spk_dev : spoke_rows, :]).astype(jnp.int32)
        for depth in range(spk_dev):
            list_s[0, taken] = block
            list_s[1, taken] = depth
            taken = taken + (depth < count).astype(jnp.int32)
    start = first_of()
    density = density_of(ro, n, live_total)
    row_cells = lax.broadcasted_iota(jnp.int32, (n, ro), 0).astype(F32).astype(BF16)
    side_rows = n // 2 + 2 * MARGIN
    low_cells = lax.broadcasted_iota(jnp.int32, (side_rows, half), 0) + (n - MARGIN)
    side_cells = [((low_cells + side * (n // 2)) % n).astype(F32).astype(BF16) for side in range(2)]
    grid_s[...] = jnp.zeros_like(grid_s)

    def table(cells, at, weights):
        before = jnp.where(at == 0, n - 1.0, at - 1)
        after = jnp.where(at == n - 1, 0.0, at + 1)
        before, at, after = (t.astype(BF16) for t in (before, at, after))
        weights = [w.astype(BF16) for w in weights]
        out = jnp.where(cells == after, weights[2], jnp.zeros((), BF16))
        out = jnp.where(cells == at, weights[1], out)
        return jnp.where(cells == before, weights[0], out)

    def build(group):
        for j in range(per_group):
            which = start + group * per_group + j
            block, depth = list_s[0, which], list_s[1, which]
            slot = [slots[block, pl.ds(f * spk_dev + depth, 1), :] for f in (0, 1, 2, 3, 4, 5, 6, 7, 9, 10)]
            low_first = slot[7][:, 1:2] <= n // 2
            slot = [jnp.where(low_first, f, joined([f[:, half:], f[:, :half]], 1)) for f in slot + [density]]
            rows = table(row_cells, slot[6], slot[0:3])
            for side in range(2):
                lanes = slice(side * half, (side + 1) * half)
                to = slice(j * half, (j + 1) * half)
                rows_s[group, :, side * span + j * half : side * span + (j + 1) * half] = rows[:, lanes]
                cols_s[group, side, :, to] = table(side_cells[side], slot[7][:, lanes], [w[:, lanes] for w in slot[3:6]])
                data = joined([slot[8][:, lanes], slot[9][:, lanes]], 0)
                data_out[group, side, 0:2, to] = data
                data_out[group, side, 2:3, to] = slot[10][:, lanes]
                weighted_s[group, side, :, to] = -slot[10][:, lanes] * data

    build(0)

    def group_step(group, carry):
        grid_group(group - 1, rows_s, cols_s, weighted_s, grid_s)
        build(group)
        return carry

    lax.fori_loop(1, groups, group_step, 0)
    grid_group(groups - 1, rows_s, cols_s, weighted_s, grid_s)
    back_out[...] = adjoint(from_sides(grid_s), const_ref)


def target_of(est_ref, part_refs):
    out = []
    for p in range(2):
        gradient = sum(part[p] for part in part_refs)
        out.append((0.0 if est_ref is None else est_ref[p]) - STEP_SIZE * gradient)
    return out


def step_kernel(n_est, n_parts, *refs):
    thr_ref, refs = refs[0], refs[1:]
    est_ref, refs = refs[0] if n_est else None, refs[n_est:]
    part_refs, refs = refs[:n_parts], refs[n_parts:]
    map_ref, data_ref, const_ref, rows_s, cols_s, est_out, part_out, sides_s, weighted_s, grid_s = refs
    groups, _, _, span = weighted_s.shape
    n, rows = map_ref.shape[1], cols_s.shape[2]
    target = target_of(est_ref, part_refs)
    re, im = shrink(target[0], target[1], thr_ref, const_ref)
    est_out[0] = re
    est_out[1] = im
    mre, mim = map_ref[0], map_ref[1]
    half = right_dft(mre * re - mim * im, mre * im + mim * re, const_ref, 1)
    for side, values in enumerate(to_sides(left_dft(half, const_ref, 1))):
        sides_s[side] = values.astype(BF16)
    grid_s[...] = jnp.zeros_like(grid_s)

    def sample_group(group):
        width = min(n, span)
        for side in range(2):
            for at in range(0, span, width):
                lanes = slice(at, at + width)
                inner = mm(sides_s[side], rows_s[group, :, side * span + at : side * span + at + width])
                col = cols_s[group, side, :, lanes].astype(F32)
                model = [jnp.sum(inner[p * rows : (p + 1) * rows] * col, axis=0, keepdims=True) for p in range(2)]
                data = data_ref[group, side, :, lanes]
                weighted_s[group, side, :, lanes] = data[2:3] * (joined(model, 0) - data[0:2])

    sample_group(0)

    def group_step(group, carry):
        grid_group(group - 1, rows_s, cols_s, weighted_s, grid_s)
        sample_group(group)
        return carry

    lax.fori_loop(1, groups, group_step, 0)
    grid_group(groups - 1, rows_s, cols_s, weighted_s, grid_s)
    back = adjoint(from_sides(grid_s), const_ref)
    conj_map(map_ref[0], map_ref[1], back, part_out)


def conj_map(mre, mim, back, part_out):
    n = mre.shape[0]
    bre, bim = back[:n], back[n:]
    part_out[0] = mre * bre + mim * bim
    part_out[1] = mre * bim - mim * bre


def map_kernel(blocks_of, pieces, *refs):
    piece_refs, (back_ref, map_out, part_out, full) = refs[:pieces], refs[pieces:]
    rows = piece_refs[0].shape[1]
    for place, value in blocks_of(piece_refs):
        for p in range(2):
            full[p, pl.ds(place * rows, rows), :] = value[:, p, :]
    for p in range(2):
        map_out[p] = full[p].T
    conj_map(map_out[0], map_out[1], back_ref[...], part_out)


def last_kernel(n_parts, rows, mine_of, thr_ref, est_ref, *refs):
    part_refs, (const_ref, out_ref) = refs[:n_parts], refs[n_parts:]
    n = est_ref.shape[1]
    target = target_of(est_ref, part_refs)
    mine = mine_of()
    pick = lax.broadcasted_iota(jnp.int32, (rows, n), 1) == (
        lax.broadcasted_iota(jnp.int32, (rows, n), 0) + mine * rows
    )
    own = mm(jnp.where(pick, 1.0, 0.0).astype(BF16), const_ref[8]).astype(BF16)
    re, im = shrink(target[0], target[1], thr_ref, const_ref, own)
    out_ref[:, 0, :] = re
    out_ref[:, 1, :] = im


def local(coil_maps, kspace_data, interp_weights, sample_bins, spoke_count, thresholds):
    n_tile, n_coil, n_spk = (lax.axis_size(name) for name in ("tile", "coil", "spk"))
    blocks = n_tile * n_spk
    rows, _, n = coil_maps.shape[1:]
    spk_dev, ro = sample_bins.shape
    live_total = blocks * spk_dev // 2
    own_map = coil_maps[0]
    by_core = n_coil == n_spk == 2 and n_tile & (n_tile - 1) == 0
    vmem = pl.BlockSpec(memory_space=pltpu.VMEM)
    smem = pl.BlockSpec(memory_space=pltpu.SMEM)
    data_rows, fields = 2 * spk_dev, 11
    spoke_rows = fields * spk_dev - data_rows
    bundle = pl.pallas_call(
        pack_kernel,
        out_shape=jax.ShapeDtypeStruct((fields * spk_dev, ro), BF16),
        in_specs=[vmem, vmem, vmem, smem],
        out_specs=vmem,
        compiler_params=PARAMS,
    )(kspace_data[0], jnp.swapaxes(interp_weights, 0, 1), sample_bins, spoke_count)

    const = np.concatenate([dft_tables(n), haar_tables(n)])
    limits, const = pl.pallas_call(
        constants_kernel,
        out_shape=[jax.ShapeDtypeStruct((LEVELS, n), F32), jax.ShapeDtypeStruct(const.shape, BF16)],
        in_specs=[smem, vmem],
        out_specs=[vmem] * 2,
        compiler_params=PARAMS,
    )(thresholds, jnp.asarray(const))

    if by_core:
        onto = [(0, 2), (3, 1), (1, 0), (2, 3)]
        across = [(1, 2), (2, 1)]

        def spread(value):
            out = [value]
            for shift in range(1, n_tile):
                out.append(lax.ppermute(value, "tile", [(i, i ^ shift) for i in range(n_tile)]))
            return out

        def to_coil(value):
            return [value, lax.ppermute(value, ("coil", "spk"), across), lax.ppermute(value, ("coil", "spk"), onto)]

        def senders():
            tile = lax.axis_index("tile")
            return [tile ^ shift for shift in range(n_tile)]

        def spoke_blocks(refs):
            own, other = refs
            spk = lax.axis_index("spk")
            for i, at in enumerate(senders()):
                yield at * 2 + spk, own[i]
                yield at * 2 + 1 - spk, other[i]

        def coil_blocks(refs):
            own, far, near = refs
            coil = lax.axis_index("coil")
            is_own = coil == lax.axis_index("spk")
            for i, at in enumerate(senders()):
                yield at * 2 + coil, jnp.where(is_own, own[i], far[i])
                yield at * 2 + 1 - coil, near[i]

        swap = [(0, 1), (1, 0)]
        pieces = spread(bundle)
        own_map, bundle = lax.optimization_barrier((own_map, bundle))
        map_pieces = spread(own_map)
        pieces, limits, const = lax.optimization_barrier((pieces, limits, const))
        own_data, own_spokes = pl.pallas_call(
            functools.partial(join_kernel, data_rows),
            out_shape=[
                jax.ShapeDtypeStruct((n_tile, data_rows, ro), BF16),
                jax.ShapeDtypeStruct((n_tile, spoke_rows, ro), BF16),
            ],
            in_specs=[vmem] * n_tile,
            out_specs=[vmem] * 2,
            compiler_params=PARAMS,
        )(*pieces)
        other_spokes = lax.ppermute(own_spokes, "spk", swap)
        coil_data = to_coil(own_data)
        map_pieces, own_spokes, own_data = lax.optimization_barrier((map_pieces, own_spokes, own_data))
        own_maps = pl.pallas_call(
            stack_kernel,
            out_shape=jax.ShapeDtypeStruct((n_tile, *own_map.shape), F32),
            in_specs=[vmem] * n_tile,
            out_specs=vmem,
            compiler_params=PARAMS,
        )(*map_pieces)
        maps = to_coil(own_maps)
        spokes = [own_spokes, other_spokes]
        share, first_of = live_total, lambda: jnp.int32(0)

        def parts_of(part):
            return [part, lax.ppermute(part, "spk", swap)]
    else:
        def gather(value):
            return [lax.all_gather(value, ("tile", "spk"), axis=0, tiled=False)]

        def spoke_blocks(refs):
            return ((i, refs[0][i]) for i in range(blocks))

        coil_blocks = spoke_blocks
        spokes, coil_data, maps = gather(bundle[data_rows:]), gather(bundle[:data_rows]), gather(own_map)
        share = live_total // blocks
        first_of = lambda: (lax.axis_index("tile") * n_spk + lax.axis_index("spk")) * share

        def parts_of(part):
            return [lax.psum(part, ("tile", "coil", "spk"))]

    per_group = min(GROUP, share)
    groups, span, side_rows = share // per_group, per_group * ro // 2, n // 2 + 2 * MARGIN
    image = jax.ShapeDtypeStruct((2, n, n), F32)
    weighted = pltpu.VMEM((groups, 2, 2, span), F32)
    gridded = pltpu.VMEM((2, 2 * side_rows, n), F32)
    counts = (len(spokes), len(coil_data))
    row_tab, col_tab, data, back = pl.pallas_call(
        functools.partial(first_kernel, first_of, spoke_blocks, coil_blocks, live_total, counts, spk_dev, n),
        out_shape=[
            jax.ShapeDtypeStruct((groups, n, 2 * span), BF16),
            jax.ShapeDtypeStruct((groups, 2, side_rows, span), BF16),
            jax.ShapeDtypeStruct((groups, 2, 3, span), F32),
            jax.ShapeDtypeStruct((2 * n, n), F32),
        ],
        in_specs=[vmem] * (sum(counts) + 1),
        out_specs=[vmem] * 4,
        scratch_shapes=[
            pltpu.VMEM((blocks, fields * spk_dev, ro), F32),
            weighted,
            gridded,
            pltpu.SMEM((2, blocks * spk_dev + 1), jnp.int32),
        ],
        compiler_params=PARAMS,
    )(*spokes, *coil_data, const)
    map_t, part = pl.pallas_call(
        functools.partial(map_kernel, coil_blocks, len(maps)),
        out_shape=[image, image],
        in_specs=[vmem] * (len(maps) + 1),
        out_specs=[vmem, vmem],
        scratch_shapes=[pltpu.VMEM((2, n, n), F32)],
        compiler_params=PARAMS,
    )(*maps, back)
    estimate = []
    parts = parts_of(part)
    for _ in range(1, ITERS):
        inputs = (*estimate, *parts, map_t, data, const, row_tab, col_tab)
        *estimate, part = pl.pallas_call(
            functools.partial(step_kernel, len(estimate), len(parts)),
            out_shape=[image, image],
            in_specs=[vmem] * (len(inputs) + 1),
            out_specs=[vmem, vmem],
            scratch_shapes=[pltpu.VMEM((2, 2 * side_rows, n), BF16), weighted, gridded],
            compiler_params=PARAMS,
        )(limits, *inputs)
        parts = parts_of(part)
    mine_of = lambda: lax.axis_index("tile") * n_spk + lax.axis_index("spk")
    return pl.pallas_call(
        functools.partial(last_kernel, len(parts), rows, mine_of),
        out_shape=jax.ShapeDtypeStruct((rows, 2, n), F32),
        in_specs=[vmem] * (len(parts) + 3),
        out_specs=vmem,
        compiler_params=PARAMS,
    )(limits, *estimate, *parts, const)


def solution(mesh):
    placed = (
        P("coil", ("grp", "tile", "spk"), None, None),
        P("coil", ("grp", "tile", "spk"), None, None),
        P(("grp", "tile", "spk"), None, None),
        P(("grp", "tile", "spk"), None),
        P(("grp", "tile", "spk")),
        P(),
    )

    return jax.shard_map(
        local,
        mesh=mesh,
        in_specs=placed,
        out_specs=P(("grp", "tile", "spk"), None, None),
        check_vma=False,
    )
```

```python
import functools
import math

import jax
import jax.numpy as jnp
import numpy as np
from jax import lax
from jax.experimental import pallas as pl
from jax.experimental.pallas import tpu as pltpu
from jax.sharding import PartitionSpec as P

LEVELS = 3
ITERS = 4
STEP_SIZE = 0.5
GROUP = 8
MARGIN = 8
PARAMS = pltpu.CompilerParams(vmem_limit_bytes=26 * 2**20)
F32 = jnp.float32
BF16 = jnp.bfloat16


def split_host(table):
    high = table.astype(BF16)
    low = (table - high.astype(np.float64)).astype(BF16)
    return high, low


def dft_tables(n):
    half = n // 2
    idx = np.arange(n)
    angles = 2.0 * math.pi / n * (np.outer(idx, idx) % n)
    scale = 1.0 / math.sqrt(n)
    small = 2.0 * math.pi / half * (np.outer(idx[:half], idx[:half]) % half)
    cos, sin = np.cos(small) * scale, np.sin(small) * scale
    folded = np.block([[cos, -sin], [sin, cos]])
    pairs = [split_host(part) for part in (np.cos(angles) * scale, np.sin(angles) * scale, folded)]
    twiddle = np.zeros((n, n))
    for i, values in enumerate((np.cos, np.sin)):
        rest = values(2.0 * math.pi / n * idx)
        for part in range(3):
            twiddle[3 * i + part] = rest.astype(BF16)
            rest = rest - twiddle[3 * i + part]
    order = [pairs[0][0], pairs[1][0], pairs[0][1], pairs[1][1], *pairs[2], twiddle.astype(BF16)]
    return np.stack(order)


def haar_rows(positions, length):
    block, within = positions // length * length, positions % length
    hits = [(block + (within >> LEVELS), jnp.ones(positions.shape, F32))]
    for level in range(1, LEVELS + 1):
        sign = jnp.where((within >> (level - 1)) % 2 == 0, 1.0, -1.0)
        hits.append((block + (length >> level) + (within >> level), sign))
    return hits


def haar_signs(n, length, flipped):
    rows = lax.broadcasted_iota(jnp.int32, (1, n) if flipped else (n, 1), int(flipped))
    positions = lax.broadcasted_iota(jnp.int32, (n, 1) if flipped else (1, n), int(not flipped))
    out = jnp.zeros((n, n), F32)
    for row, sign in haar_rows(positions, length):
        out = jnp.where(rows == row, sign, out)
    return out.astype(BF16)


def split2(x):
    high = x.astype(BF16)
    return high, (x - high.astype(F32)).astype(BF16)


def mm(a, b):
    return jnp.dot(a, b, preferred_element_type=F32)


def mm_t(a, b):
    return lax.dot_general(a, b, (((1,), (1,)), ((), ())), preferred_element_type=F32)


def joined(parts, axis):
    return jnp.concatenate(parts, axis=axis)


def twiddles(const, half):
    rows = const[6, 0:8, 0:half].astype(F32)
    return rows[0:1] + rows[1:2] + rows[2:3], rows[3:4] + rows[4:5] + rows[5:6]


def half_dfts(first, second, const):
    high, low = split2(joined([first, second], 0))
    return mm(joined([high, low, high], 1), joined([const[4], const[4], const[5]], 0))


def right_dft(re, im, const):
    n = re.shape[0]
    half = n // 2
    cos, sin = twiddles(const, half)
    sum_re, sum_im = re[:, :half] + re[:, half:], im[:, :half] + im[:, half:]
    dif_re, dif_im = re[:, :half] - re[:, half:], im[:, :half] - im[:, half:]
    turned = joined([dif_re * cos + dif_im * sin, dif_im * cos - dif_re * sin], 1)
    out = half_dfts(joined([sum_re, sum_im], 1), turned, const)
    return joined([joined([out[:n, lo : lo + half], out[n:, lo : lo + half]], 1) for lo in (0, half)], 0)


def right_idft(re, im, const):
    n = re.shape[0]
    half = n // 2
    cos, sin = twiddles(const, half)
    even, odd = (joined([re[:, lo : lo + half], -im[:, lo : lo + half]], 1) for lo in (0, half))
    out = half_dfts(even, odd, const)
    even_re, even_im, odd_re, odd_im = out[:n, :half], -out[:n, half:], out[n:, :half], -out[n:, half:]
    turn_re, turn_im = odd_re * cos - odd_im * sin, odd_im * cos + odd_re * sin
    out_re = joined([even_re + turn_re, even_re - turn_re], 1)
    return joined([out_re, joined([even_im + turn_im, even_im - turn_im], 1)], 0)


def left_dft(stacked, const, sign):
    high, low = split2(stacked)

    def table(base):
        cos, sin = const[base], const[base + 1]
        top, bottom = ((cos, sin), (-sin, cos)) if sign > 0 else ((cos, -sin), (sin, cos))
        return joined([joined(top, 1), joined(bottom, 1)], 0)

    return mm(joined([table(0), table(0), table(2)], 1), joined([high, low, high], 0))


def labels(positions, length):
    out = jnp.ones(positions.shape, F32)
    for level in range(1, LEVELS + 1):
        out = out + jnp.where(positions < length >> level, 1.0, 0.0)
    return out


def shrink(re, im, thr_ref, const, last_rows=None):
    n = re.shape[0]
    block = 2**LEVELS
    col_pos = lax.broadcasted_iota(jnp.int32, (n, 1), 0)
    row_pos = lax.broadcasted_iota(jnp.int32, (1, n), 1) % block
    col_label, row_label = labels(col_pos, n), labels(row_pos, block)
    col_scale = jnp.exp2(-0.5 * jnp.minimum(col_label, LEVELS))
    row_scale = jnp.exp2(-0.5 * jnp.minimum(row_label, LEVELS))
    band = jnp.minimum(col_label, row_label)
    limits = jnp.full((n, n), 1.0, F32)
    for level in range(LEVELS):
        limits = jnp.where(band == level + 1, thr_ref[level : level + 1, :], limits)
    scale = col_scale * row_scale
    half = mm(joined([const[7]] * 2, 1), joined(split2(joined([re, im], 1)), 0))
    half = joined([half[:, :n], half[:, n:]], 0)
    full = mm(joined(split2(half), 1), joined([const[9]] * 2, 0))
    coeffs = [full[:n] * scale, full[n:] * scale]
    magnitude = jnp.sqrt(coeffs[0] * coeffs[0] + coeffs[1] * coeffs[1])
    factor = jnp.maximum(magnitude - limits, 0.0) / jnp.maximum(magnitude, limits)
    factor = jnp.where(band <= LEVELS, factor, 1.0) * scale
    kept = joined([coeffs[0] * factor, coeffs[1] * factor], 1)
    half = mm(joined([const[8]] * 2, 1), joined(split2(kept), 0))
    half = joined([half[:, :n], half[:, n:]], 0)
    if last_rows is None:
        full = mm(joined(split2(half), 1), joined([const[10]] * 2, 0))
        return full[:n], full[n:]
    full = mm_t(joined([last_rows] * 2, 1), joined(split2(half), 1))
    return full[:, :n], full[:, n:]


def density_of(ro, n, live_total):
    lane = lax.broadcasted_iota(jnp.int32, (1, ro), 1)
    offset = jnp.abs(lane - ro // 2).astype(F32)
    return (offset + 0.5) * (n / (3.0 * ro * live_total))


def smear(col_table, weighted):
    col = col_table.astype(F32)
    return joined([(col * weighted[p : p + 1]).astype(BF16) for p in range(2)], 0)


def grid_group(group, rows_s, cols_s, weighted_s, grid_s):
    span = cols_s.shape[-1]
    for side in range(2):
        smeared = smear(cols_s[group, side], weighted_s[group, side])
        grid_s[side] += mm_t(smeared, rows_s[group, :, side * span : (side + 1) * span])


def to_sides(kspace):
    n = kspace.shape[0] // 2
    mid = n // 2
    low, high = [], []
    for part in (kspace[:n], kspace[n:]):
        low += [part[n - MARGIN :], part[: mid + MARGIN]]
        high += [part[mid - MARGIN :], part[:MARGIN]]
    return joined(low, 0), joined(high, 0)


def from_sides(grid_s):
    span = grid_s.shape[1] // 2
    mid, m = span - 2 * MARGIN, MARGIN
    out = []
    for p in range(2):
        low, high = grid_s[0, p * span : (p + 1) * span], grid_s[1, p * span : (p + 1) * span]
        out += [
            low[m : 2 * m] + high[mid + m :],
            low[2 * m : mid],
            low[mid:] + high[: 2 * m],
            high[2 * m : mid],
            high[mid : mid + m] + low[:m],
        ]
    return joined(out, 0)


def adjoint(gridded, const):
    half = left_dft(gridded, const, -1)
    n = gridded.shape[0] // 2
    return right_idft(half[:n], half[n:], const)


def pack_kernel(data_ref, weight_ref, bins_ref, count_ref, out_ref):
    slots, ro = bins_ref.shape
    n = ro
    bins = bins_ref[...]
    fields = [data_ref[:, p, :].astype(F32) for p in range(2)]
    fields += [weight_ref[i].astype(F32) for i in range(weight_ref.shape[0])]
    fields += [(bins // n).astype(F32), (bins % n).astype(F32)]
    fields.append(jnp.full((slots, ro), count_ref[0].astype(F32)))
    out_ref[...] = joined(fields, 0).astype(BF16)


def join_kernel(data_rows, *refs):
    pieces, (data_out, spoke_out) = refs[:-2], refs[-2:]
    for i, piece in enumerate(pieces):
        data_out[i] = piece[:data_rows]
        spoke_out[i] = piece[data_rows:]


def stack_kernel(*refs):
    for i, piece in enumerate(refs[:-1]):
        refs[-1][i] = piece[...]


def constants_kernel(thr_ref, const_ref, thr_out, const_out):
    for level in range(LEVELS):
        thr_out[level : level + 1, :] = jnp.full((1, thr_out.shape[1]), thr_ref[level])
    given, n = const_ref.shape[0], const_ref.shape[1]
    const_out[0:given] = const_ref[...]
    for i, (length, flipped) in enumerate(((n, False), (n, True), (2**LEVELS, True), (2**LEVELS, False))):
        const_out[given + i] = haar_signs(n, length, flipped)


def first_kernel(first_of, spoke_blocks, coil_blocks, live_total, counts, spk_dev, n, *refs):
    spoke_refs, data_refs, refs = refs[: counts[0]], refs[counts[0] : sum(counts)], refs[sum(counts) :]
    const_ref, rows_s, cols_s, data_out, back_out, slots, weighted_s, grid_s, list_s = refs
    spoke_rows = slots.shape[1] - 2 * spk_dev
    ro = slots.shape[-1]
    groups, _, _, span = weighted_s.shape
    per_group, half = 2 * span // ro, ro // 2
    for place, value in spoke_blocks(spoke_refs):
        slots[place, 0:spoke_rows] = value.astype(F32)
    for place, value in coil_blocks(data_refs):
        slots[place, spoke_rows:] = value.astype(F32)
    taken = jnp.int32(0)
    for block in range(slots.shape[0]):
        count = jnp.max(slots[block, spoke_rows - spk_dev : spoke_rows, :]).astype(jnp.int32)
        for depth in range(spk_dev):
            list_s[0, taken] = block
            list_s[1, taken] = depth
            taken = taken + (depth < count).astype(jnp.int32)
    start = first_of()
    density = density_of(ro, n, live_total)
    row_order = lax.broadcasted_iota(jnp.int32, (n, ro), 0)
    row_order = jnp.where(row_order < n // 2, 2 * row_order, 2 * row_order - n + 1)
    row_cells = row_order.astype(F32).astype(BF16)
    side_rows = n // 2 + 2 * MARGIN
    low_cells = lax.broadcasted_iota(jnp.int32, (side_rows, half), 0) + (n - MARGIN)
    side_cells = [((low_cells + side * (n // 2)) % n).astype(F32).astype(BF16) for side in range(2)]
    grid_s[...] = jnp.zeros_like(grid_s)

    def table(cells, at, weights):
        before = jnp.where(at == 0, n - 1.0, at - 1)
        after = jnp.where(at == n - 1, 0.0, at + 1)
        before, at, after = (t.astype(BF16) for t in (before, at, after))
        weights = [w.astype(BF16) for w in weights]
        out = jnp.where(cells == after, weights[2], jnp.zeros((), BF16))
        out = jnp.where(cells == at, weights[1], out)
        return jnp.where(cells == before, weights[0], out)

    def build(group):
        for j in range(per_group):
            which = start + group * per_group + j
            block, depth = list_s[0, which], list_s[1, which]
            slot = [slots[block, pl.ds(f * spk_dev + depth, 1), :] for f in (0, 1, 2, 3, 4, 5, 6, 7, 9, 10)]
            low_first = slot[7][:, 1:2] <= n // 2
            slot = [jnp.where(low_first, f, joined([f[:, half:], f[:, :half]], 1)) for f in slot + [density]]
            rows = table(row_cells, slot[6], slot[0:3])
            for side in range(2):
                lanes = slice(side * half, (side + 1) * half)
                to = slice(j * half, (j + 1) * half)
                rows_s[group, :, side * span + j * half : side * span + (j + 1) * half] = rows[:, lanes]
                cols_s[group, side, :, to] = table(side_cells[side], slot[7][:, lanes], [w[:, lanes] for w in slot[3:6]])
                data = joined([slot[8][:, lanes], slot[9][:, lanes]], 0)
                data_out[group, side, 0:2, to] = data
                data_out[group, side, 2:3, to] = slot[10][:, lanes]
                weighted_s[group, side, :, to] = -slot[10][:, lanes] * data

    build(0)

    def group_step(group, carry):
        grid_group(group - 1, rows_s, cols_s, weighted_s, grid_s)
        build(group)
        return carry

    lax.fori_loop(1, groups, group_step, 0)
    grid_group(groups - 1, rows_s, cols_s, weighted_s, grid_s)
    back_out[...] = adjoint(from_sides(grid_s), const_ref)


def target_of(est_ref, part_refs):
    out = []
    for p in range(2):
        gradient = sum(part[p] for part in part_refs)
        out.append((0.0 if est_ref is None else est_ref[p]) - STEP_SIZE * gradient)
    return out


def step_kernel(n_est, n_parts, *refs):
    thr_ref, refs = refs[0], refs[1:]
    est_ref, refs = refs[0] if n_est else None, refs[n_est:]
    part_refs, refs = refs[:n_parts], refs[n_parts:]
    map_ref, data_ref, const_ref, rows_s, cols_s, est_out, part_out, sides_s, weighted_s, grid_s = refs
    groups, _, _, span = weighted_s.shape
    n, rows = map_ref.shape[1], cols_s.shape[2]
    target = target_of(est_ref, part_refs)
    re, im = shrink(target[0], target[1], thr_ref, const_ref)
    est_out[0] = re
    est_out[1] = im
    mre, mim = map_ref[0], map_ref[1]
    half = right_dft(mre * re - mim * im, mre * im + mim * re, const_ref)
    for side, values in enumerate(to_sides(left_dft(half, const_ref, 1))):
        sides_s[side] = values.astype(BF16)
    grid_s[...] = jnp.zeros_like(grid_s)

    def sample_group(group):
        width = min(n, span)
        for side in range(2):
            for at in range(0, span, width):
                lanes = slice(at, at + width)
                inner = mm(sides_s[side], rows_s[group, :, side * span + at : side * span + at + width])
                col = cols_s[group, side, :, lanes].astype(F32)
                model = [jnp.sum(inner[p * rows : (p + 1) * rows] * col, axis=0, keepdims=True) for p in range(2)]
                data = data_ref[group, side, :, lanes]
                weighted_s[group, side, :, lanes] = data[2:3] * (joined(model, 0) - data[0:2])

    sample_group(0)

    def group_step(group, carry):
        grid_group(group - 1, rows_s, cols_s, weighted_s, grid_s)
        sample_group(group)
        return carry

    lax.fori_loop(1, groups, group_step, 0, unroll=True)
    grid_group(groups - 1, rows_s, cols_s, weighted_s, grid_s)
    back = adjoint(from_sides(grid_s), const_ref)
    conj_map(map_ref[0], map_ref[1], back, part_out)


def conj_map(mre, mim, back, part_out):
    n = mre.shape[0]
    bre, bim = back[:n], back[n:]
    part_out[0] = mre * bre + mim * bim
    part_out[1] = mre * bim - mim * bre


def map_kernel(blocks_of, pieces, *refs):
    piece_refs, (back_ref, map_out, part_out, full) = refs[:pieces], refs[pieces:]
    rows = piece_refs[0].shape[1]
    for place, value in blocks_of(piece_refs):
        for p in range(2):
            full[p, pl.ds(place * rows, rows), :] = value[:, p, :]
    for p in range(2):
        map_out[p] = full[p].T
    conj_map(map_out[0], map_out[1], back_ref[...], part_out)


def last_kernel(n_parts, rows, mine_of, thr_ref, est_ref, *refs):
    part_refs, (const_ref, out_ref) = refs[:n_parts], refs[n_parts:]
    n = est_ref.shape[1]
    target = target_of(est_ref, part_refs)
    mine = mine_of()
    pick = lax.broadcasted_iota(jnp.int32, (rows, n), 1) == (
        lax.broadcasted_iota(jnp.int32, (rows, n), 0) + mine * rows
    )
    own = mm(jnp.where(pick, 1.0, 0.0).astype(BF16), const_ref[9]).astype(BF16)
    re, im = shrink(target[0], target[1], thr_ref, const_ref, own)
    out_ref[:, 0, :] = re
    out_ref[:, 1, :] = im


def local(coil_maps, kspace_data, interp_weights, sample_bins, spoke_count, thresholds):
    n_tile, n_coil, n_spk = (lax.axis_size(name) for name in ("tile", "coil", "spk"))
    blocks = n_tile * n_spk
    rows, _, n = coil_maps.shape[1:]
    spk_dev, ro = sample_bins.shape
    live_total = blocks * spk_dev // 2
    own_map = coil_maps[0]
    by_core = n_coil == n_spk == 2 and n_tile & (n_tile - 1) == 0
    vmem = pl.BlockSpec(memory_space=pltpu.VMEM)
    smem = pl.BlockSpec(memory_space=pltpu.SMEM)
    data_rows, fields = 2 * spk_dev, 11
    spoke_rows = fields * spk_dev - data_rows
    bundle = pl.pallas_call(
        pack_kernel,
        out_shape=jax.ShapeDtypeStruct((fields * spk_dev, ro), BF16),
        in_specs=[vmem, vmem, vmem, smem],
        out_specs=vmem,
        compiler_params=PARAMS,
    )(kspace_data[0], jnp.swapaxes(interp_weights, 0, 1), sample_bins, spoke_count)

    const = dft_tables(n)
    limits, const = pl.pallas_call(
        constants_kernel,
        out_shape=[jax.ShapeDtypeStruct((LEVELS, n), F32), jax.ShapeDtypeStruct((const.shape[0] + 4, n, n), BF16)],
        in_specs=[smem, vmem],
        out_specs=[vmem] * 2,
        compiler_params=PARAMS,
    )(thresholds, jnp.asarray(const))

    if by_core:
        onto = [(0, 2), (3, 1), (1, 0), (2, 3)]
        across = [(1, 2), (2, 1)]

        def spread(value):
            out = [value]
            for shift in range(1, n_tile):
                out.append(lax.ppermute(value, "tile", [(i, i ^ shift) for i in range(n_tile)]))
            return out

        def to_coil(value):
            return [value, lax.ppermute(value, ("coil", "spk"), across), lax.ppermute(value, ("coil", "spk"), onto)]

        def senders():
            tile = lax.axis_index("tile")
            return [tile ^ shift for shift in range(n_tile)]

        def spoke_blocks(refs):
            own, other = refs
            spk = lax.axis_index("spk")
            for i, at in enumerate(senders()):
                yield at * 2 + spk, own[i]
                yield at * 2 + 1 - spk, other[i]

        def coil_blocks(refs):
            own, far, near = refs
            coil = lax.axis_index("coil")
            is_own = coil == lax.axis_index("spk")
            for i, at in enumerate(senders()):
                yield at * 2 + coil, jnp.where(is_own, own[i], far[i])
                yield at * 2 + 1 - coil, near[i]

        swap = [(0, 1), (1, 0)]
        pieces = spread(bundle)
        own_map, bundle = lax.optimization_barrier((own_map, bundle))
        map_pieces = spread(own_map)
        pieces, limits, const = lax.optimization_barrier((pieces, limits, const))
        own_data, own_spokes = pl.pallas_call(
            functools.partial(join_kernel, data_rows),
            out_shape=[
                jax.ShapeDtypeStruct((n_tile, data_rows, ro), BF16),
                jax.ShapeDtypeStruct((n_tile, spoke_rows, ro), BF16),
            ],
            in_specs=[vmem] * n_tile,
            out_specs=[vmem] * 2,
            compiler_params=PARAMS,
        )(*pieces)
        other_spokes = lax.ppermute(own_spokes, "spk", swap)
        coil_data = to_coil(own_data)
        map_pieces, own_spokes, own_data = lax.optimization_barrier((map_pieces, own_spokes, own_data))
        own_maps = pl.pallas_call(
            stack_kernel,
            out_shape=jax.ShapeDtypeStruct((n_tile, *own_map.shape), F32),
            in_specs=[vmem] * n_tile,
            out_specs=vmem,
            compiler_params=PARAMS,
        )(*map_pieces)
        maps = to_coil(own_maps)
        spokes = [own_spokes, other_spokes]
        share, first_of = live_total, lambda: jnp.int32(0)

        def parts_of(part):
            return [part, lax.ppermute(part, "spk", swap)]
    else:
        def gather(value):
            return [lax.all_gather(value, ("tile", "spk"), axis=0, tiled=False)]

        def spoke_blocks(refs):
            return ((i, refs[0][i]) for i in range(blocks))

        coil_blocks = spoke_blocks
        spokes, coil_data, maps = gather(bundle[data_rows:]), gather(bundle[:data_rows]), gather(own_map)
        share = live_total // blocks
        first_of = lambda: (lax.axis_index("tile") * n_spk + lax.axis_index("spk")) * share

        def parts_of(part):
            return [lax.psum(part, ("tile", "coil", "spk"))]

    per_group = min(GROUP, share)
    groups, span, side_rows = share // per_group, per_group * ro // 2, n // 2 + 2 * MARGIN
    image = jax.ShapeDtypeStruct((2, n, n), F32)
    weighted = pltpu.VMEM((groups, 2, 2, span), F32)
    gridded = pltpu.VMEM((2, 2 * side_rows, n), F32)
    counts = (len(spokes), len(coil_data))
    row_tab, col_tab, data, back = pl.pallas_call(
        functools.partial(first_kernel, first_of, spoke_blocks, coil_blocks, live_total, counts, spk_dev, n),
        out_shape=[
            jax.ShapeDtypeStruct((groups, n, 2 * span), BF16),
            jax.ShapeDtypeStruct((groups, 2, side_rows, span), BF16),
            jax.ShapeDtypeStruct((groups, 2, 3, span), F32),
            jax.ShapeDtypeStruct((2 * n, n), F32),
        ],
        in_specs=[vmem] * (sum(counts) + 1),
        out_specs=[vmem] * 4,
        scratch_shapes=[
            pltpu.VMEM((blocks, fields * spk_dev, ro), F32),
            weighted,
            gridded,
            pltpu.SMEM((2, blocks * spk_dev + 1), jnp.int32),
        ],
        compiler_params=PARAMS,
    )(*spokes, *coil_data, const)
    map_t, part = pl.pallas_call(
        functools.partial(map_kernel, coil_blocks, len(maps)),
        out_shape=[image, image],
        in_specs=[vmem] * (len(maps) + 1),
        out_specs=[vmem, vmem],
        scratch_shapes=[pltpu.VMEM((2, n, n), F32)],
        compiler_params=PARAMS,
    )(*maps, back)
    estimate = []
    parts = parts_of(part)
    for _ in range(1, ITERS):
        inputs = (*estimate, *parts, map_t, data, const, row_tab, col_tab)
        *estimate, part = pl.pallas_call(
            functools.partial(step_kernel, len(estimate), len(parts)),
            out_shape=[image, image],
            in_specs=[vmem] * (len(inputs) + 1),
            out_specs=[vmem, vmem],
            scratch_shapes=[pltpu.VMEM((2, 2 * side_rows, n), BF16), weighted, gridded],
            compiler_params=PARAMS,
        )(limits, *inputs)
        parts = parts_of(part)
    mine_of = lambda: lax.axis_index("tile") * n_spk + lax.axis_index("spk")
    return pl.pallas_call(
        functools.partial(last_kernel, len(parts), rows, mine_of),
        out_shape=jax.ShapeDtypeStruct((rows, 2, n), F32),
        in_specs=[vmem] * (len(parts) + 3),
        out_specs=vmem,
        compiler_params=PARAMS,
    )(limits, *estimate, *parts, const)


def solution(mesh):
    placed = (
        P("coil", ("grp", "tile", "spk"), None, None),
        P("coil", ("grp", "tile", "spk"), None, None),
        P(("grp", "tile", "spk"), None, None),
        P(("grp", "tile", "spk"), None),
        P(("grp", "tile", "spk")),
        P(),
    )

    return jax.shard_map(
        local,
        mesh=mesh,
        in_specs=placed,
        out_specs=P(("grp", "tile", "spk"), None, None),
        check_vma=False,
    )
```

```python
import functools
import math

import jax
import jax.numpy as jnp
import numpy as np
from jax import lax
from jax.experimental import pallas as pl
from jax.experimental.pallas import tpu as pltpu
from jax.sharding import PartitionSpec as P

LEVELS = 3
ITERS = 4
STEP_SIZE = 0.5
GROUP = 8
MARGIN = 8
PARAMS = pltpu.CompilerParams(vmem_limit_bytes=26 * 2**20)
F32 = jnp.float32
BF16 = jnp.bfloat16


STRIDE = 16


def dft_seeds(n):
    coarse, fine = STRIDE * np.arange(n // STRIDE), np.arange(STRIDE)
    rows = []
    for positions, scale in ((coarse, 1.0), (fine, 1.0 / math.sqrt(n)), (2 * fine, 1.0 / math.sqrt(n))):
        angles = 2.0 * math.pi / n * (np.outer(positions, np.arange(n)) % n)
        rows += [np.cos(angles) * scale, np.sin(angles) * scale]
    return np.concatenate(rows).astype(np.float32)


def dft_kernel(seed_ref, out_ref):
    n = seed_ref.shape[1]
    half, coarse = n // 2, n // STRIDE
    at = [0, coarse, 2 * coarse, 2 * coarse + STRIDE, 2 * coarse + 2 * STRIDE, 2 * coarse + 3 * STRIDE]
    fine = [seed_ref[start : start + STRIDE, :] for start in at[2:]]

    def turned(i, cos, sin):
        big_cos, big_sin = (seed_ref[start + i : start + i + 1, :] for start in at[:2])
        return big_cos * cos - big_sin * sin, big_sin * cos + big_cos * sin

    for i in range(coarse):
        rows = slice(i * STRIDE, (i + 1) * STRIDE)
        for plane, values in enumerate(turned(i, fine[0], fine[1])):
            out_ref[plane, rows, :], out_ref[plane + 2, rows, :] = split2(values)
    for i in range(coarse // 2):
        cos, sin = (values[:, :half] for values in turned(2 * i, fine[2], fine[3]))
        for start, values in ((0, (cos, -sin)), (half, (sin, cos))):
            rows = slice(start + i * STRIDE, start + (i + 1) * STRIDE)
            out_ref[4, rows, :], out_ref[5, rows, :] = split2(joined(values, 1))
    parts = [part.astype(F32) for values in fine[:2] for part in split3(values[1:2] * math.sqrt(n))]
    parts.append(jnp.zeros((STRIDE - len(parts), n), F32))
    out_ref[6, 0:STRIDE, :] = joined(parts, 0).astype(BF16)


def haar_rows(positions, length):
    block, within = positions // length * length, positions % length
    hits = [(block + (within >> LEVELS), jnp.ones(positions.shape, F32))]
    for level in range(1, LEVELS + 1):
        sign = jnp.where((within >> (level - 1)) % 2 == 0, 1.0, -1.0)
        hits.append((block + (length >> level) + (within >> level), sign))
    return hits


def haar_signs(n, length, flipped):
    rows = lax.broadcasted_iota(jnp.int32, (1, n) if flipped else (n, 1), int(flipped))
    positions = lax.broadcasted_iota(jnp.int32, (n, 1) if flipped else (1, n), int(not flipped))
    out = jnp.zeros((n, n), F32)
    for row, sign in haar_rows(positions, length):
        out = jnp.where(rows == row, sign, out)
    return out.astype(BF16)


def split2(x):
    high = x.astype(BF16)
    return high, (x - high.astype(F32)).astype(BF16)


def split3(x):
    high, mid = split2(x)
    return high, mid, (x - high.astype(F32) - mid.astype(F32)).astype(BF16)


def mm(a, b):
    return jnp.dot(a, b, preferred_element_type=F32)


def mm_t(a, b):
    return lax.dot_general(a, b, (((1,), (1,)), ((), ())), preferred_element_type=F32)


def joined(parts, axis):
    return jnp.concatenate(parts, axis=axis)


def twiddles(const, half):
    rows = const[6, 0:8, 0:half].astype(F32)
    return rows[0:1] + rows[1:2] + rows[2:3], rows[3:4] + rows[4:5] + rows[5:6]


def half_dfts(first, second, const):
    high, low = split2(joined([first, second], 0))
    return mm(joined([high, low, high], 1), joined([const[4], const[4], const[5]], 0))


def right_dft(re, im, const):
    n = re.shape[0]
    half = n // 2
    cos, sin = twiddles(const, half)
    sum_re, sum_im = re[:, :half] + re[:, half:], im[:, :half] + im[:, half:]
    dif_re, dif_im = re[:, :half] - re[:, half:], im[:, :half] - im[:, half:]
    turned = joined([dif_re * cos + dif_im * sin, dif_im * cos - dif_re * sin], 1)
    out = half_dfts(joined([sum_re, sum_im], 1), turned, const)
    return joined([joined([out[:n, lo : lo + half], out[n:, lo : lo + half]], 1) for lo in (0, half)], 0)


def right_idft(re, im, const):
    n = re.shape[0]
    half = n // 2
    cos, sin = twiddles(const, half)
    even, odd = (joined([re[:, lo : lo + half], -im[:, lo : lo + half]], 1) for lo in (0, half))
    out = half_dfts(even, odd, const)
    even_re, even_im, odd_re, odd_im = out[:n, :half], -out[:n, half:], out[n:, :half], -out[n:, half:]
    turn_re, turn_im = odd_re * cos - odd_im * sin, odd_im * cos + odd_re * sin
    out_re = joined([even_re + turn_re, even_re - turn_re], 1)
    return joined([out_re, joined([even_im + turn_im, even_im - turn_im], 1)], 0)


def left_dft(stacked, const, sign):
    high, low = split2(stacked)

    def table(base):
        cos, sin = const[base], const[base + 1]
        top, bottom = ((cos, sin), (-sin, cos)) if sign > 0 else ((cos, -sin), (sin, cos))
        return joined([joined(top, 1), joined(bottom, 1)], 0)

    return mm(joined([table(0), table(0), table(2)], 1), joined([high, low, high], 0))


def labels(positions, length):
    out = jnp.ones(positions.shape, F32)
    for level in range(1, LEVELS + 1):
        out = out + jnp.where(positions < length >> level, 1.0, 0.0)
    return out


def shrink(re, im, thr_ref, haar, last_rows=None):
    n = re.shape[0]
    block = 2**LEVELS
    col_pos = lax.broadcasted_iota(jnp.int32, (n, 1), 0)
    row_pos = lax.broadcasted_iota(jnp.int32, (1, n), 1) % block
    col_label, row_label = labels(col_pos, n), labels(row_pos, block)
    col_scale = jnp.exp2(-0.5 * jnp.minimum(col_label, LEVELS))
    row_scale = jnp.exp2(-0.5 * jnp.minimum(row_label, LEVELS))
    band = jnp.minimum(col_label, row_label)
    limits = jnp.full((n, n), 1.0, F32)
    for level in range(LEVELS):
        limits = jnp.where(band == level + 1, thr_ref[level : level + 1, :], limits)
    scale = col_scale * row_scale
    half = mm(joined([haar[0]] * 2, 1), joined(split2(joined([re, im], 1)), 0))
    half = joined([half[:, :n], half[:, n:]], 0)
    full = mm(joined(split2(half), 1), joined([haar[2]] * 2, 0))
    coeffs = [full[:n] * scale, full[n:] * scale]
    magnitude = jnp.sqrt(coeffs[0] * coeffs[0] + coeffs[1] * coeffs[1])
    factor = jnp.maximum(magnitude - limits, 0.0) / jnp.maximum(magnitude, limits)
    factor = jnp.where(band <= LEVELS, factor, 1.0) * scale
    kept = joined([coeffs[0] * factor, coeffs[1] * factor], 1)
    half = mm(joined([haar[1]] * 2, 1), joined(split2(kept), 0))
    half = joined([half[:, :n], half[:, n:]], 0)
    if last_rows is None:
        full = mm(joined(split2(half), 1), joined([haar[3]] * 2, 0))
        return full[:n], full[n:]
    full = mm_t(joined([last_rows] * 2, 1), joined(split2(half), 1))
    return full[:, :n], full[:, n:]


def density_of(ro, n, live_total):
    lane = lax.broadcasted_iota(jnp.int32, (1, ro), 1)
    offset = jnp.abs(lane - ro // 2).astype(F32)
    return (offset + 0.5) * (n / (3.0 * ro * live_total))


def smear(col_table, weighted):
    col = col_table.astype(F32)
    return joined([(col * weighted[p : p + 1]).astype(BF16) for p in range(2)], 0)


def grid_group(group, rows_s, cols_s, weighted_s, grid_s):
    span = cols_s.shape[-1]
    for side in range(2):
        smeared = smear(cols_s[group, side], weighted_s[group, side])
        grid_s[side] += mm_t(smeared, rows_s[group, :, side * span : (side + 1) * span])


def to_sides(kspace):
    n = kspace.shape[0] // 2
    mid = n // 2
    low, high = [], []
    for part in (kspace[:n], kspace[n:]):
        low += [part[n - MARGIN :], part[: mid + MARGIN]]
        high += [part[mid - MARGIN :], part[:MARGIN]]
    return joined(low, 0), joined(high, 0)


def from_sides(grid_s):
    span = grid_s.shape[1] // 2
    mid, m = span - 2 * MARGIN, MARGIN
    out = []
    for p in range(2):
        low, high = grid_s[0, p * span : (p + 1) * span], grid_s[1, p * span : (p + 1) * span]
        out += [
            low[m : 2 * m] + high[mid + m :],
            low[2 * m : mid],
            low[mid:] + high[: 2 * m],
            high[2 * m : mid],
            high[mid : mid + m] + low[:m],
        ]
    return joined(out, 0)


def adjoint(gridded, const):
    half = left_dft(gridded, const, -1)
    n = gridded.shape[0] // 2
    return right_idft(half[:n], half[n:], const)


def pack_kernel(data_ref, weight_ref, bins_ref, count_ref, out_ref):
    slots, ro = bins_ref.shape
    n = ro
    bins = bins_ref[...]
    fields = [data_ref[:, p, :].astype(F32) for p in range(2)]
    fields += [weight_ref[i].astype(F32) for i in range(weight_ref.shape[0])]
    fields += [(bins // n).astype(F32), (bins % n).astype(F32)]
    fields.append(jnp.full((slots, ro), count_ref[0].astype(F32)))
    out_ref[...] = joined(fields, 0).astype(BF16)


def join_kernel(data_rows, *refs):
    pieces, (data_out, spoke_out) = refs[:-2], refs[-2:]
    for i, piece in enumerate(pieces):
        data_out[i] = piece[:data_rows]
        spoke_out[i] = piece[data_rows:]


def stack_kernel(*refs):
    for i, piece in enumerate(refs[:-1]):
        refs[-1][i] = piece[...]


def haar_kernel(thr_ref, thr_out, haar_out):
    n = haar_out.shape[1]
    for level in range(LEVELS):
        thr_out[level : level + 1, :] = jnp.full((1, n), thr_ref[level])
    for i, (length, flipped) in enumerate(((n, False), (n, True), (2**LEVELS, True), (2**LEVELS, False))):
        haar_out[i] = haar_signs(n, length, flipped)


def first_kernel(first_of, spoke_blocks, coil_blocks, live_total, counts, spk_dev, n, *refs):
    spoke_refs, data_refs, refs = refs[: counts[0]], refs[counts[0] : sum(counts)], refs[sum(counts) :]
    const_ref, rows_s, cols_s, data_out, back_out, slots, weighted_s, grid_s, list_s = refs
    spoke_rows = slots.shape[1] - 2 * spk_dev
    ro = slots.shape[-1]
    groups, _, _, span = weighted_s.shape
    per_group, half = 2 * span // ro, ro // 2
    for place, value in spoke_blocks(spoke_refs):
        slots[place, 0:spoke_rows] = value.astype(F32)
    for place, value in coil_blocks(data_refs):
        slots[place, spoke_rows:] = value.astype(F32)
    taken = jnp.int32(0)
    for block in range(slots.shape[0]):
        count = jnp.max(slots[block, spoke_rows - spk_dev : spoke_rows, :]).astype(jnp.int32)
        for depth in range(spk_dev):
            list_s[0, taken] = block
            list_s[1, taken] = depth
            taken = taken + (depth < count).astype(jnp.int32)
    start = first_of()
    density = density_of(ro, n, live_total)
    row_order = lax.broadcasted_iota(jnp.int32, (n, ro), 0)
    row_order = jnp.where(row_order < n // 2, 2 * row_order, 2 * row_order - n + 1)
    row_cells = row_order.astype(F32).astype(BF16)
    side_rows = n // 2 + 2 * MARGIN
    low_cells = lax.broadcasted_iota(jnp.int32, (side_rows, half), 0) + (n - MARGIN)
    side_cells = [((low_cells + side * (n // 2)) % n).astype(F32).astype(BF16) for side in range(2)]
    grid_s[...] = jnp.zeros_like(grid_s)

    def table(cells, at, weights):
        before = jnp.where(at == 0, n - 1.0, at - 1)
        after = jnp.where(at == n - 1, 0.0, at + 1)
        before, at, after = (t.astype(BF16) for t in (before, at, after))
        weights = [w.astype(BF16) for w in weights]
        out = jnp.where(cells == after, weights[2], jnp.zeros((), BF16))
        out = jnp.where(cells == at, weights[1], out)
        return jnp.where(cells == before, weights[0], out)

    def build(group):
        for j in range(per_group):
            which = start + group * per_group + j
            block, depth = list_s[0, which], list_s[1, which]
            slot = [slots[block, pl.ds(f * spk_dev + depth, 1), :] for f in (0, 1, 2, 3, 4, 5, 6, 7, 9, 10)]
            low_first = slot[7][:, 1:2] <= n // 2
            slot = [jnp.where(low_first, f, joined([f[:, half:], f[:, :half]], 1)) for f in slot + [density]]
            rows = table(row_cells, slot[6], slot[0:3])
            for side in range(2):
                lanes = slice(side * half, (side + 1) * half)
                to = slice(j * half, (j + 1) * half)
                rows_s[group, :, side * span + j * half : side * span + (j + 1) * half] = rows[:, lanes]
                cols_s[group, side, :, to] = table(side_cells[side], slot[7][:, lanes], [w[:, lanes] for w in slot[3:6]])
                data = joined([slot[8][:, lanes], slot[9][:, lanes]], 0)
                data_out[group, side, 0:2, to] = data
                data_out[group, side, 2:3, to] = slot[10][:, lanes]
                weighted_s[group, side, :, to] = -slot[10][:, lanes] * data

    build(0)

    def group_step(group, carry):
        grid_group(group - 1, rows_s, cols_s, weighted_s, grid_s)
        build(group)
        return carry

    lax.fori_loop(1, groups, group_step, 0)
    grid_group(groups - 1, rows_s, cols_s, weighted_s, grid_s)
    back_out[...] = adjoint(from_sides(grid_s), const_ref)


def target_of(est_ref, part_refs):
    out = []
    for p in range(2):
        gradient = sum(part[p] for part in part_refs)
        out.append((0.0 if est_ref is None else est_ref[p]) - STEP_SIZE * gradient)
    return out


def step_kernel(n_est, n_parts, *refs):
    thr_ref, refs = refs[0], refs[1:]
    est_ref, refs = refs[0] if n_est else None, refs[n_est:]
    part_refs, refs = refs[:n_parts], refs[n_parts:]
    map_ref, data_ref, const_ref, haar_ref, rows_s, cols_s, est_out, part_out, sides_s, weighted_s, grid_s = refs
    groups, _, _, span = weighted_s.shape
    n, rows = map_ref.shape[1], cols_s.shape[2]
    target = target_of(est_ref, part_refs)
    re, im = shrink(target[0], target[1], thr_ref, haar_ref)
    est_out[0] = re
    est_out[1] = im
    mre, mim = map_ref[0], map_ref[1]
    half = right_dft(mre * re - mim * im, mre * im + mim * re, const_ref)
    for side, values in enumerate(to_sides(left_dft(half, const_ref, 1))):
        sides_s[side] = values.astype(BF16)
    grid_s[...] = jnp.zeros_like(grid_s)

    def sample_group(group):
        width = min(n, span)
        for side in range(2):
            for at in range(0, span, width):
                lanes = slice(at, at + width)
                inner = mm(sides_s[side], rows_s[group, :, side * span + at : side * span + at + width])
                col = cols_s[group, side, :, lanes].astype(F32)
                model = [jnp.sum(inner[p * rows : (p + 1) * rows] * col, axis=0, keepdims=True) for p in range(2)]
                data = data_ref[group, side, :, lanes]
                weighted_s[group, side, :, lanes] = data[2:3] * (joined(model, 0) - data[0:2])

    sample_group(0)

    def group_step(group, carry):
        grid_group(group - 1, rows_s, cols_s, weighted_s, grid_s)
        sample_group(group)
        return carry

    lax.fori_loop(1, groups, group_step, 0, unroll=True)
    grid_group(groups - 1, rows_s, cols_s, weighted_s, grid_s)
    back = adjoint(from_sides(grid_s), const_ref)
    conj_map(map_ref[0], map_ref[1], back, part_out)


def conj_map(mre, mim, back, part_out):
    n = mre.shape[0]
    bre, bim = back[:n], back[n:]
    part_out[0] = mre * bre + mim * bim
    part_out[1] = mre * bim - mim * bre


def map_kernel(blocks_of, pieces, *refs):
    piece_refs, (back_ref, map_out, part_out, full) = refs[:pieces], refs[pieces:]
    rows = piece_refs[0].shape[1]
    for place, value in blocks_of(piece_refs):
        for p in range(2):
            full[p, pl.ds(place * rows, rows), :] = value[:, p, :]
    for p in range(2):
        map_out[p] = full[p].T
    conj_map(map_out[0], map_out[1], back_ref[...], part_out)


def last_kernel(n_parts, rows, mine_of, thr_ref, est_ref, *refs):
    part_refs, (haar_ref, out_ref) = refs[:n_parts], refs[n_parts:]
    n = est_ref.shape[1]
    target = target_of(est_ref, part_refs)
    mine = mine_of()
    pick = lax.broadcasted_iota(jnp.int32, (rows, n), 1) == (
        lax.broadcasted_iota(jnp.int32, (rows, n), 0) + mine * rows
    )
    own = mm(jnp.where(pick, 1.0, 0.0).astype(BF16), haar_ref[2]).astype(BF16)
    re, im = shrink(target[0], target[1], thr_ref, haar_ref, own)
    out_ref[:, 0, :] = re
    out_ref[:, 1, :] = im


def local(coil_maps, kspace_data, interp_weights, sample_bins, spoke_count, thresholds):
    n_tile, n_coil, n_spk = (lax.axis_size(name) for name in ("tile", "coil", "spk"))
    blocks = n_tile * n_spk
    rows, _, n = coil_maps.shape[1:]
    spk_dev, ro = sample_bins.shape
    live_total = blocks * spk_dev // 2
    own_map = coil_maps[0]
    by_core = n_coil == n_spk == 2 and n_tile & (n_tile - 1) == 0
    vmem = pl.BlockSpec(memory_space=pltpu.VMEM)
    smem = pl.BlockSpec(memory_space=pltpu.SMEM)
    data_rows, fields = 2 * spk_dev, 11
    spoke_rows = fields * spk_dev - data_rows
    bundle = pl.pallas_call(
        pack_kernel,
        out_shape=jax.ShapeDtypeStruct((fields * spk_dev, ro), BF16),
        in_specs=[vmem, vmem, vmem, smem],
        out_specs=vmem,
        compiler_params=PARAMS,
    )(kspace_data[0], jnp.swapaxes(interp_weights, 0, 1), sample_bins, spoke_count)

    const = pl.pallas_call(
        dft_kernel,
        out_shape=jax.ShapeDtypeStruct((7, n, n), BF16),
        in_specs=[vmem],
        out_specs=vmem,
        compiler_params=PARAMS,
    )(jnp.asarray(dft_seeds(n)))

    if by_core:
        onto = [(0, 2), (3, 1), (1, 0), (2, 3)]
        across = [(1, 2), (2, 1)]

        def spread(value):
            out = [value]
            for shift in range(1, n_tile):
                out.append(lax.ppermute(value, "tile", [(i, i ^ shift) for i in range(n_tile)]))
            return out

        def to_coil(value):
            return [value, lax.ppermute(value, ("coil", "spk"), across), lax.ppermute(value, ("coil", "spk"), onto)]

        def senders():
            tile = lax.axis_index("tile")
            return [tile ^ shift for shift in range(n_tile)]

        def spoke_blocks(refs):
            own, other = refs
            spk = lax.axis_index("spk")
            for i, at in enumerate(senders()):
                yield at * 2 + spk, own[i]
                yield at * 2 + 1 - spk, other[i]

        def coil_blocks(refs):
            own, far, near = refs
            coil = lax.axis_index("coil")
            is_own = coil == lax.axis_index("spk")
            for i, at in enumerate(senders()):
                yield at * 2 + coil, jnp.where(is_own, own[i], far[i])
                yield at * 2 + 1 - coil, near[i]

        swap = [(0, 1), (1, 0)]
        pieces = spread(bundle)
        own_map, bundle = lax.optimization_barrier((own_map, bundle))
        map_pieces = spread(own_map)
        pieces, const = lax.optimization_barrier((pieces, const))
        own_data, own_spokes = pl.pallas_call(
            functools.partial(join_kernel, data_rows),
            out_shape=[
                jax.ShapeDtypeStruct((n_tile, data_rows, ro), BF16),
                jax.ShapeDtypeStruct((n_tile, spoke_rows, ro), BF16),
            ],
            in_specs=[vmem] * n_tile,
            out_specs=[vmem] * 2,
            compiler_params=PARAMS,
        )(*pieces)
        other_spokes = lax.ppermute(own_spokes, "spk", swap)
        coil_data = to_coil(own_data)
        map_pieces, own_spokes, own_data = lax.optimization_barrier((map_pieces, own_spokes, own_data))
        own_maps = pl.pallas_call(
            stack_kernel,
            out_shape=jax.ShapeDtypeStruct((n_tile, *own_map.shape), F32),
            in_specs=[vmem] * n_tile,
            out_specs=vmem,
            compiler_params=PARAMS,
        )(*map_pieces)
        maps = to_coil(own_maps)
        spokes = [own_spokes, other_spokes]
        share, first_of = live_total, lambda: jnp.int32(0)

        def parts_of(part):
            return [part, lax.ppermute(part, "spk", swap)]
    else:
        def gather(value):
            return [lax.all_gather(value, ("tile", "spk"), axis=0, tiled=False)]

        def spoke_blocks(refs):
            return ((i, refs[0][i]) for i in range(blocks))

        coil_blocks = spoke_blocks
        spokes, coil_data, maps = gather(bundle[data_rows:]), gather(bundle[:data_rows]), gather(own_map)
        share = live_total // blocks
        first_of = lambda: (lax.axis_index("tile") * n_spk + lax.axis_index("spk")) * share

        def parts_of(part):
            return [lax.psum(part, ("tile", "coil", "spk"))]

    per_group = min(GROUP, share)
    groups, span, side_rows = share // per_group, per_group * ro // 2, n // 2 + 2 * MARGIN
    image = jax.ShapeDtypeStruct((2, n, n), F32)
    weighted = pltpu.VMEM((groups, 2, 2, span), F32)
    gridded = pltpu.VMEM((2, 2 * side_rows, n), F32)
    counts = (len(spokes), len(coil_data))
    row_tab, col_tab, data, back = pl.pallas_call(
        functools.partial(first_kernel, first_of, spoke_blocks, coil_blocks, live_total, counts, spk_dev, n),
        out_shape=[
            jax.ShapeDtypeStruct((groups, n, 2 * span), BF16),
            jax.ShapeDtypeStruct((groups, 2, side_rows, span), BF16),
            jax.ShapeDtypeStruct((groups, 2, 3, span), F32),
            jax.ShapeDtypeStruct((2 * n, n), F32),
        ],
        in_specs=[vmem] * (sum(counts) + 1),
        out_specs=[vmem] * 4,
        scratch_shapes=[
            pltpu.VMEM((blocks, fields * spk_dev, ro), F32),
            weighted,
            gridded,
            pltpu.SMEM((2, blocks * spk_dev + 1), jnp.int32),
        ],
        compiler_params=PARAMS,
    )(*spokes, *coil_data, const)
    map_t, part = pl.pallas_call(
        functools.partial(map_kernel, coil_blocks, len(maps)),
        out_shape=[image, image],
        in_specs=[vmem] * (len(maps) + 1),
        out_specs=[vmem, vmem],
        scratch_shapes=[pltpu.VMEM((2, n, n), F32)],
        compiler_params=PARAMS,
    )(*maps, back)
    estimate = []
    part, thresholds = lax.optimization_barrier((part, thresholds))
    limits, haar = pl.pallas_call(
        haar_kernel,
        out_shape=[jax.ShapeDtypeStruct((LEVELS, n), F32), jax.ShapeDtypeStruct((4, n, n), BF16)],
        in_specs=[smem],
        out_specs=[vmem] * 2,
        compiler_params=PARAMS,
    )(thresholds)
    parts = parts_of(part)
    for _ in range(1, ITERS):
        inputs = (*estimate, *parts, map_t, data, const, haar, row_tab, col_tab)
        *estimate, part = pl.pallas_call(
            functools.partial(step_kernel, len(estimate), len(parts)),
            out_shape=[image, image],
            in_specs=[vmem] * (len(inputs) + 1),
            out_specs=[vmem, vmem],
            scratch_shapes=[pltpu.VMEM((2, 2 * side_rows, n), BF16), weighted, gridded],
            compiler_params=PARAMS,
        )(limits, *inputs)
        parts = parts_of(part)
    mine_of = lambda: lax.axis_index("tile") * n_spk + lax.axis_index("spk")
    return pl.pallas_call(
        functools.partial(last_kernel, len(parts), rows, mine_of),
        out_shape=jax.ShapeDtypeStruct((rows, 2, n), F32),
        in_specs=[vmem] * (len(parts) + 3),
        out_specs=vmem,
        compiler_params=PARAMS,
    )(limits, *estimate, *parts, haar)


def solution(mesh):
    placed = (
        P("coil", ("grp", "tile", "spk"), None, None),
        P("coil", ("grp", "tile", "spk"), None, None),
        P(("grp", "tile", "spk"), None, None),
        P(("grp", "tile", "spk"), None),
        P(("grp", "tile", "spk")),
        P(),
    )

    return jax.shard_map(
        local,
        mesh=mesh,
        in_specs=placed,
        out_specs=P(("grp", "tile", "spk"), None, None),
        check_vma=False,
    )
```

```python
import functools
import math

import jax
import jax.numpy as jnp
import numpy as np
from jax import lax
from jax.experimental import pallas as pl
from jax.experimental.pallas import tpu as pltpu
from jax.sharding import PartitionSpec as P

LEVELS = 3
ITERS = 4
STEP_SIZE = 0.5
GROUP = 8
MARGIN = 8
PARAMS = pltpu.CompilerParams(vmem_limit_bytes=26 * 2**20)
F32 = jnp.float32
BF16 = jnp.bfloat16


STRIDE = 16


def dft_seeds(n):
    coarse, fine = STRIDE * np.arange(n // STRIDE), np.arange(STRIDE)
    rows = []
    for positions, scale in ((coarse, 1.0), (fine, 1.0 / math.sqrt(n)), (2 * fine, 1.0 / math.sqrt(n))):
        angles = 2.0 * math.pi / n * (np.outer(positions, np.arange(n)) % n)
        rows += [np.cos(angles) * scale, np.sin(angles) * scale]
    return np.concatenate(rows).astype(np.float32)


def dft_kernel(seed_ref, out_ref):
    n = seed_ref.shape[1]
    half, coarse = n // 2, n // STRIDE
    at = [0, coarse, 2 * coarse, 2 * coarse + STRIDE, 2 * coarse + 2 * STRIDE, 2 * coarse + 3 * STRIDE]
    fine = [seed_ref[start : start + STRIDE, :] for start in at[2:]]

    def turned(i, cos, sin):
        big_cos, big_sin = (seed_ref[start + i : start + i + 1, :] for start in at[:2])
        return big_cos * cos - big_sin * sin, big_sin * cos + big_cos * sin

    for i in range(coarse):
        rows = slice(i * STRIDE, (i + 1) * STRIDE)
        for plane, values in enumerate(turned(i, fine[0], fine[1])):
            out_ref[plane, rows, :], out_ref[plane + 2, rows, :] = split2(values)
    for i in range(coarse // 2):
        cos, sin = (values[:, :half] for values in turned(2 * i, fine[2], fine[3]))
        for start, values in ((0, (cos, -sin)), (half, (sin, cos))):
            rows = slice(start + i * STRIDE, start + (i + 1) * STRIDE)
            out_ref[4, rows, :], out_ref[5, rows, :] = split2(joined(values, 1))
    parts = [part.astype(F32) for values in fine[:2] for part in split3(values[1:2] * math.sqrt(n))]
    parts.append(jnp.zeros((STRIDE - len(parts), n), F32))
    out_ref[6, 0:STRIDE, :] = joined(parts, 0).astype(BF16)


def haar_rows(positions, length):
    block, within = positions // length * length, positions % length
    hits = [(block + (within >> LEVELS), jnp.ones(positions.shape, F32))]
    for level in range(1, LEVELS + 1):
        sign = jnp.where((within >> (level - 1)) % 2 == 0, 1.0, -1.0)
        hits.append((block + (length >> level) + (within >> level), sign))
    return hits


def haar_signs(n, length, flipped):
    rows = lax.broadcasted_iota(jnp.int32, (1, n) if flipped else (n, 1), int(flipped))
    positions = lax.broadcasted_iota(jnp.int32, (n, 1) if flipped else (1, n), int(not flipped))
    out = jnp.zeros((n, n), F32)
    for row, sign in haar_rows(positions, length):
        out = jnp.where(rows == row, sign, out)
    return out.astype(BF16)


def split2(x):
    high = x.astype(BF16)
    return high, (x - high.astype(F32)).astype(BF16)


def split3(x):
    high, mid = split2(x)
    return high, mid, (x - high.astype(F32) - mid.astype(F32)).astype(BF16)


def mm(a, b):
    return jnp.dot(a, b, preferred_element_type=F32)


def mm_t(a, b):
    return lax.dot_general(a, b, (((1,), (1,)), ((), ())), preferred_element_type=F32)


def joined(parts, axis):
    return jnp.concatenate(parts, axis=axis)


def twiddles(const, half):
    rows = const[6, 0:8, 0:half].astype(F32)
    return rows[0:1] + rows[1:2] + rows[2:3], rows[3:4] + rows[4:5] + rows[5:6]


def half_dfts(first, second, const):
    high, low = split2(joined([first, second], 0))
    return mm(joined([high, low, high], 1), joined([const[4], const[4], const[5]], 0))


def right_dft(re, im, const):
    n = re.shape[0]
    half = n // 2
    cos, sin = twiddles(const, half)
    sum_re, sum_im = re[:, :half] + re[:, half:], im[:, :half] + im[:, half:]
    dif_re, dif_im = re[:, :half] - re[:, half:], im[:, :half] - im[:, half:]
    turned = joined([dif_re * cos + dif_im * sin, dif_im * cos - dif_re * sin], 1)
    out = half_dfts(joined([sum_re, sum_im], 1), turned, const)
    return joined([joined([out[:n, lo : lo + half], out[n:, lo : lo + half]], 1) for lo in (0, half)], 0)


def right_idft(re, im, const):
    n = re.shape[0]
    half = n // 2
    cos, sin = twiddles(const, half)
    even, odd = (joined([re[:, lo : lo + half], -im[:, lo : lo + half]], 1) for lo in (0, half))
    out = half_dfts(even, odd, const)
    even_re, even_im, odd_re, odd_im = out[:n, :half], -out[:n, half:], out[n:, :half], -out[n:, half:]
    turn_re, turn_im = odd_re * cos - odd_im * sin, odd_im * cos + odd_re * sin
    out_re = joined([even_re + turn_re, even_re - turn_re], 1)
    return joined([out_re, joined([even_im + turn_im, even_im - turn_im], 1)], 0)


def left_dft(stacked, const, sign):
    high, low = split2(stacked)

    def table(base):
        cos, sin = const[base], const[base + 1]
        top, bottom = ((cos, sin), (-sin, cos)) if sign > 0 else ((cos, -sin), (sin, cos))
        return joined([joined(top, 1), joined(bottom, 1)], 0)

    return mm(joined([table(0), table(0), table(2)], 1), joined([high, low, high], 0))


def labels(positions, length):
    out = jnp.ones(positions.shape, F32)
    for level in range(1, LEVELS + 1):
        out = out + jnp.where(positions < length >> level, 1.0, 0.0)
    return out


def band_tables(col_pos, row_pos, n, thr_ref, thr_lanes):
    col_label, row_label = labels(col_pos, n), labels(row_pos % 2**LEVELS, 2**LEVELS)
    scale = jnp.exp2(-0.5 * jnp.minimum(col_label, LEVELS)) * jnp.exp2(-0.5 * jnp.minimum(row_label, LEVELS))
    band = jnp.minimum(col_label, row_label)
    limits = jnp.full(band.shape, 1.0, F32)
    for level in range(LEVELS):
        limits = jnp.where(band == level + 1, thr_ref[level : level + 1, :thr_lanes], limits)
    return limits, scale, band


def shrunk(re, im, limits, scale, band):
    re, im = re * scale, im * scale
    magnitude = jnp.sqrt(re * re + im * im)
    factor = jnp.maximum(magnitude - limits, 0.0) / jnp.maximum(magnitude, limits)
    factor = jnp.where(band <= LEVELS, factor, 1.0) * scale
    return re * factor, im * factor


def shrink(re, im, thr_ref, haar):
    n = re.shape[0]
    col_pos = lax.broadcasted_iota(jnp.int32, (n, 1), 0)
    row_pos = lax.broadcasted_iota(jnp.int32, (1, n), 1)
    tables = band_tables(col_pos, row_pos, n, thr_ref, n)
    half = mm(joined([haar[0]] * 2, 1), joined(split2(joined([re, im], 1)), 0))
    half = joined([half[:, :n], half[:, n:]], 0)
    full = mm(joined(split2(half), 1), joined([haar[2]] * 2, 0))
    kept = joined(shrunk(full[:n], full[n:], *tables), 1)
    half = mm(joined([haar[1]] * 2, 1), joined(split2(kept), 0))
    half = joined([half[:, :n], half[:, n:]], 0)
    full = mm(joined(split2(half), 1), joined([haar[3]] * 2, 0))
    return full[:n], full[n:]


def density_of(ro, n, live_total):
    lane = lax.broadcasted_iota(jnp.int32, (1, ro), 1)
    offset = jnp.abs(lane - ro // 2).astype(F32)
    return (offset + 0.5) * (n / (3.0 * ro * live_total))


def smear(col_table, weighted):
    col = col_table.astype(F32)
    return joined([(col * weighted[p : p + 1]).astype(BF16) for p in range(2)], 0)


def grid_group(group, rows_s, cols_s, weighted_s, grid_s):
    span = cols_s.shape[-1]
    for side in range(2):
        smeared = smear(cols_s[group, side], weighted_s[group, side])
        grid_s[side] += mm_t(smeared, rows_s[group, :, side * span : (side + 1) * span])


def to_sides(kspace):
    n = kspace.shape[0] // 2
    mid = n // 2
    low, high = [], []
    for part in (kspace[:n], kspace[n:]):
        low += [part[n - MARGIN :], part[: mid + MARGIN]]
        high += [part[mid - MARGIN :], part[:MARGIN]]
    return joined(low, 0), joined(high, 0)


def from_sides(grid_s):
    span = grid_s.shape[1] // 2
    mid, m = span - 2 * MARGIN, MARGIN
    out = []
    for p in range(2):
        low, high = grid_s[0, p * span : (p + 1) * span], grid_s[1, p * span : (p + 1) * span]
        out += [
            low[m : 2 * m] + high[mid + m :],
            low[2 * m : mid],
            low[mid:] + high[: 2 * m],
            high[2 * m : mid],
            high[mid : mid + m] + low[:m],
        ]
    return joined(out, 0)


def adjoint(gridded, const):
    half = left_dft(gridded, const, -1)
    n = gridded.shape[0] // 2
    return right_idft(half[:n], half[n:], const)


def pack_kernel(data_ref, weight_ref, bins_ref, count_ref, out_ref):
    slots, ro = bins_ref.shape
    n = ro
    bins = bins_ref[...]
    fields = [data_ref[:, p, :].astype(F32) for p in range(2)]
    fields += [weight_ref[i].astype(F32) for i in range(weight_ref.shape[0])]
    fields += [(bins // n).astype(F32), (bins % n).astype(F32)]
    fields.append(jnp.full((slots, ro), count_ref[0].astype(F32)))
    out_ref[...] = joined(fields, 0).astype(BF16)


def join_kernel(data_rows, *refs):
    pieces, (data_out, spoke_out) = refs[:-2], refs[-2:]
    for i, piece in enumerate(pieces):
        data_out[i] = piece[:data_rows]
        spoke_out[i] = piece[data_rows:]


def stack_kernel(*refs):
    for i, piece in enumerate(refs[:-1]):
        refs[-1][i] = piece[...]


def haar_kernel(thr_ref, thr_out, haar_out):
    n = haar_out.shape[1]
    for level in range(LEVELS):
        thr_out[level : level + 1, :] = jnp.full((1, n), thr_ref[level])
    for i, (length, flipped) in enumerate(((n, False), (n, True), (2**LEVELS, True), (2**LEVELS, False))):
        haar_out[i] = haar_signs(n, length, flipped)


def first_kernel(first_of, spoke_blocks, coil_blocks, live_total, counts, spk_dev, n, *refs):
    spoke_refs, data_refs, refs = refs[: counts[0]], refs[counts[0] : sum(counts)], refs[sum(counts) :]
    const_ref, rows_s, cols_s, data_out, back_out, slots, weighted_s, grid_s, list_s = refs
    spoke_rows = slots.shape[1] - 2 * spk_dev
    ro = slots.shape[-1]
    groups, _, _, span = weighted_s.shape
    per_group, half = 2 * span // ro, ro // 2
    for place, value in spoke_blocks(spoke_refs):
        slots[place, 0:spoke_rows] = value.astype(F32)
    for place, value in coil_blocks(data_refs):
        slots[place, spoke_rows:] = value.astype(F32)
    taken = jnp.int32(0)
    for block in range(slots.shape[0]):
        count = jnp.max(slots[block, spoke_rows - spk_dev : spoke_rows, :]).astype(jnp.int32)
        for depth in range(spk_dev):
            list_s[0, taken] = block
            list_s[1, taken] = depth
            taken = taken + (depth < count).astype(jnp.int32)
    start = first_of()
    density = density_of(ro, n, live_total)
    row_order = lax.broadcasted_iota(jnp.int32, (n, ro), 0)
    row_order = jnp.where(row_order < n // 2, 2 * row_order, 2 * row_order - n + 1)
    row_cells = row_order.astype(F32).astype(BF16)
    side_rows = n // 2 + 2 * MARGIN
    low_cells = lax.broadcasted_iota(jnp.int32, (side_rows, half), 0) + (n - MARGIN)
    side_cells = [((low_cells + side * (n // 2)) % n).astype(F32).astype(BF16) for side in range(2)]
    grid_s[...] = jnp.zeros_like(grid_s)

    def table(cells, at, weights):
        before = jnp.where(at == 0, n - 1.0, at - 1)
        after = jnp.where(at == n - 1, 0.0, at + 1)
        before, at, after = (t.astype(BF16) for t in (before, at, after))
        weights = [w.astype(BF16) for w in weights]
        out = jnp.where(cells == after, weights[2], jnp.zeros((), BF16))
        out = jnp.where(cells == at, weights[1], out)
        return jnp.where(cells == before, weights[0], out)

    def build(group):
        for j in range(per_group):
            which = start + group * per_group + j
            block, depth = list_s[0, which], list_s[1, which]
            slot = [slots[block, pl.ds(f * spk_dev + depth, 1), :] for f in (0, 1, 2, 3, 4, 5, 6, 7, 9, 10)]
            low_first = slot[7][:, 1:2] <= n // 2
            slot = [jnp.where(low_first, f, joined([f[:, half:], f[:, :half]], 1)) for f in slot + [density]]
            rows = table(row_cells, slot[6], slot[0:3])
            for side in range(2):
                lanes = slice(side * half, (side + 1) * half)
                to = slice(j * half, (j + 1) * half)
                rows_s[group, :, side * span + j * half : side * span + (j + 1) * half] = rows[:, lanes]
                cols_s[group, side, :, to] = table(side_cells[side], slot[7][:, lanes], [w[:, lanes] for w in slot[3:6]])
                data = joined([slot[8][:, lanes], slot[9][:, lanes]], 0)
                data_out[group, side, 0:2, to] = data
                data_out[group, side, 2:3, to] = slot[10][:, lanes]
                weighted_s[group, side, :, to] = -slot[10][:, lanes] * data

    build(0)

    def group_step(group, carry):
        grid_group(group - 1, rows_s, cols_s, weighted_s, grid_s)
        build(group)
        return carry

    lax.fori_loop(1, groups, group_step, 0, unroll=True)
    grid_group(groups - 1, rows_s, cols_s, weighted_s, grid_s)
    back_out[...] = adjoint(from_sides(grid_s), const_ref)


def target_of(est_ref, part_refs):
    out = []
    for p in range(2):
        gradient = sum(part[p] for part in part_refs)
        out.append((0.0 if est_ref is None else est_ref[p]) - STEP_SIZE * gradient)
    return out


def step_kernel(n_est, n_parts, *refs):
    thr_ref, refs = refs[0], refs[1:]
    est_ref, refs = refs[0] if n_est else None, refs[n_est:]
    part_refs, refs = refs[:n_parts], refs[n_parts:]
    map_ref, data_ref, const_ref, haar_ref, rows_s, cols_s, est_out, part_out, sides_s, weighted_s, grid_s = refs
    groups, _, _, span = weighted_s.shape
    n, rows = map_ref.shape[1], cols_s.shape[2]
    target = target_of(est_ref, part_refs)
    re, im = shrink(target[0], target[1], thr_ref, haar_ref)
    est_out[0] = re
    est_out[1] = im
    mre, mim = map_ref[0], map_ref[1]
    half = right_dft(mre * re - mim * im, mre * im + mim * re, const_ref)
    for side, values in enumerate(to_sides(left_dft(half, const_ref, 1))):
        sides_s[side] = values.astype(BF16)
    grid_s[...] = jnp.zeros_like(grid_s)

    def sample_group(group):
        width = min(n, span)
        for side in range(2):
            for at in range(0, span, width):
                lanes = slice(at, at + width)
                inner = mm(sides_s[side], rows_s[group, :, side * span + at : side * span + at + width])
                col = cols_s[group, side, :, lanes].astype(F32)
                model = [jnp.sum(inner[p * rows : (p + 1) * rows] * col, axis=0, keepdims=True) for p in range(2)]
                data = data_ref[group, side, :, lanes]
                weighted_s[group, side, :, lanes] = data[2:3] * (joined(model, 0) - data[0:2])

    sample_group(0)

    def group_step(group, carry):
        grid_group(group - 1, rows_s, cols_s, weighted_s, grid_s)
        sample_group(group)
        return carry

    lax.fori_loop(1, groups, group_step, 0, unroll=True)
    grid_group(groups - 1, rows_s, cols_s, weighted_s, grid_s)
    back = adjoint(from_sides(grid_s), const_ref)
    conj_map(map_ref[0], map_ref[1], back, part_out)


def conj_map(mre, mim, back, part_out):
    n = mre.shape[0]
    bre, bim = back[:n], back[n:]
    part_out[0] = mre * bre + mim * bim
    part_out[1] = mre * bim - mim * bre


def map_kernel(blocks_of, pieces, *refs):
    piece_refs, (back_ref, map_out, part_out, full) = refs[:pieces], refs[pieces:]
    rows = piece_refs[0].shape[1]
    for place, value in blocks_of(piece_refs):
        for p in range(2):
            full[p, pl.ds(place * rows, rows), :] = value[:, p, :]
    for p in range(2):
        map_out[p] = full[p].T
    conj_map(map_out[0], map_out[1], back_ref[...], part_out)


def last_kernel(n_parts, rows, mine_of, thr_ref, est_ref, *refs):
    part_refs, (haar_ref, out_ref) = refs[:n_parts], refs[n_parts:]
    n = est_ref.shape[1]
    target = target_of(est_ref, part_refs)
    pick = lax.broadcasted_iota(jnp.int32, (rows, n), 1) == (
        lax.broadcasted_iota(jnp.int32, (rows, n), 0) + mine_of() * rows
    )
    pick = jnp.where(pick, 1.0, 0.0).astype(BF16)
    own = mm_t(joined([pick] * 3, 1), joined(split3(joined(target, 0)), 1))
    row_pos = lax.broadcasted_iota(jnp.int32, (rows, 1), 0)
    col_pos = lax.broadcasted_iota(jnp.int32, (1, n), 1)
    tables = band_tables(col_pos, row_pos, n, thr_ref, n)
    row_haar, row_back = haar_ref[3][:rows, :rows], haar_ref[2][:rows, :rows]

    def by_rows(signs, wide):
        return mm(signs, split2(wide)[0]) + mm(signs, split2(wide)[1])

    half = by_rows(row_haar, own)
    half = joined([half[:, :n], half[:, n:]], 0)
    full = mm(joined(split2(half), 1), joined([haar_ref[1]] * 2, 0))
    kept = joined(shrunk(full[:rows], full[rows:], *tables), 0)
    half = mm(joined(split2(kept), 1), joined([haar_ref[0]] * 2, 0))
    full = by_rows(row_back, joined([half[:rows], half[rows:]], 1))
    out_ref[:, 0, :] = full[:, :n]
    out_ref[:, 1, :] = full[:, n:]


def local(coil_maps, kspace_data, interp_weights, sample_bins, spoke_count, thresholds):
    n_tile, n_coil, n_spk = (lax.axis_size(name) for name in ("tile", "coil", "spk"))
    blocks = n_tile * n_spk
    rows, _, n = coil_maps.shape[1:]
    spk_dev, ro = sample_bins.shape
    live_total = blocks * spk_dev // 2
    own_map = coil_maps[0]
    by_core = n_coil == n_spk == 2 and n_tile & (n_tile - 1) == 0
    vmem = pl.BlockSpec(memory_space=pltpu.VMEM)
    smem = pl.BlockSpec(memory_space=pltpu.SMEM)
    data_rows, fields = 2 * spk_dev, 11
    spoke_rows = fields * spk_dev - data_rows
    bundle = pl.pallas_call(
        pack_kernel,
        out_shape=jax.ShapeDtypeStruct((fields * spk_dev, ro), BF16),
        in_specs=[vmem, vmem, vmem, smem],
        out_specs=vmem,
        compiler_params=PARAMS,
    )(kspace_data[0], jnp.swapaxes(interp_weights, 0, 1), sample_bins, spoke_count)

    const = pl.pallas_call(
        dft_kernel,
        out_shape=jax.ShapeDtypeStruct((7, n, n), BF16),
        in_specs=[vmem],
        out_specs=vmem,
        compiler_params=PARAMS,
    )(jnp.asarray(dft_seeds(n)))

    if by_core:
        onto = [(0, 2), (3, 1), (1, 0), (2, 3)]
        across = [(1, 2), (2, 1)]

        def spread(value):
            out = [value]
            for shift in range(1, n_tile):
                out.append(lax.ppermute(value, "tile", [(i, i ^ shift) for i in range(n_tile)]))
            return out

        def to_coil(value):
            return [value, lax.ppermute(value, ("coil", "spk"), across), lax.ppermute(value, ("coil", "spk"), onto)]

        def senders():
            tile = lax.axis_index("tile")
            return [tile ^ shift for shift in range(n_tile)]

        def spoke_blocks(refs):
            own, other = refs
            spk = lax.axis_index("spk")
            for i, at in enumerate(senders()):
                yield at * 2 + spk, own[i]
                yield at * 2 + 1 - spk, other[i]

        def coil_blocks(refs):
            own, far, near = refs
            coil = lax.axis_index("coil")
            is_own = coil == lax.axis_index("spk")
            for i, at in enumerate(senders()):
                yield at * 2 + coil, jnp.where(is_own, own[i], far[i])
                yield at * 2 + 1 - coil, near[i]

        swap = [(0, 1), (1, 0)]
        pieces = spread(bundle)
        own_map, bundle = lax.optimization_barrier((own_map, bundle))
        map_pieces = spread(own_map)
        pieces, const = lax.optimization_barrier((pieces, const))
        own_data, own_spokes = pl.pallas_call(
            functools.partial(join_kernel, data_rows),
            out_shape=[
                jax.ShapeDtypeStruct((n_tile, data_rows, ro), BF16),
                jax.ShapeDtypeStruct((n_tile, spoke_rows, ro), BF16),
            ],
            in_specs=[vmem] * n_tile,
            out_specs=[vmem] * 2,
            compiler_params=PARAMS,
        )(*pieces)
        other_spokes = lax.ppermute(own_spokes, "spk", swap)
        coil_data = to_coil(own_data)
        map_pieces, own_spokes, own_data = lax.optimization_barrier((map_pieces, own_spokes, own_data))
        own_maps = pl.pallas_call(
            stack_kernel,
            out_shape=jax.ShapeDtypeStruct((n_tile, *own_map.shape), F32),
            in_specs=[vmem] * n_tile,
            out_specs=vmem,
            compiler_params=PARAMS,
        )(*map_pieces)
        maps = to_coil(own_maps)
        spokes = [own_spokes, other_spokes]
        share, first_of = live_total, lambda: jnp.int32(0)

        def parts_of(part):
            return [part, lax.ppermute(part, "spk", swap)]
    else:
        def gather(value):
            return [lax.all_gather(value, ("tile", "spk"), axis=0, tiled=False)]

        def spoke_blocks(refs):
            return ((i, refs[0][i]) for i in range(blocks))

        coil_blocks = spoke_blocks
        spokes, coil_data, maps = gather(bundle[data_rows:]), gather(bundle[:data_rows]), gather(own_map)
        share = live_total // blocks
        first_of = lambda: (lax.axis_index("tile") * n_spk + lax.axis_index("spk")) * share

        def parts_of(part):
            return [lax.psum(part, ("tile", "coil", "spk"))]

    per_group = min(GROUP, share)
    groups, span, side_rows = share // per_group, per_group * ro // 2, n // 2 + 2 * MARGIN
    image = jax.ShapeDtypeStruct((2, n, n), F32)
    weighted = pltpu.VMEM((groups, 2, 2, span), F32)
    gridded = pltpu.VMEM((2, 2 * side_rows, n), F32)
    counts = (len(spokes), len(coil_data))
    row_tab, col_tab, data, back = pl.pallas_call(
        functools.partial(first_kernel, first_of, spoke_blocks, coil_blocks, live_total, counts, spk_dev, n),
        out_shape=[
            jax.ShapeDtypeStruct((groups, n, 2 * span), BF16),
            jax.ShapeDtypeStruct((groups, 2, side_rows, span), BF16),
            jax.ShapeDtypeStruct((groups, 2, 3, span), F32),
            jax.ShapeDtypeStruct((2 * n, n), F32),
        ],
        in_specs=[vmem] * (sum(counts) + 1),
        out_specs=[vmem] * 4,
        scratch_shapes=[
            pltpu.VMEM((blocks, fields * spk_dev, ro), F32),
            weighted,
            gridded,
            pltpu.SMEM((2, blocks * spk_dev + 1), jnp.int32),
        ],
        compiler_params=PARAMS,
    )(*spokes, *coil_data, const)
    map_t, part = pl.pallas_call(
        functools.partial(map_kernel, coil_blocks, len(maps)),
        out_shape=[image, image],
        in_specs=[vmem] * (len(maps) + 1),
        out_specs=[vmem, vmem],
        scratch_shapes=[pltpu.VMEM((2, n, n), F32)],
        compiler_params=PARAMS,
    )(*maps, back)
    estimate = []
    part, thresholds = lax.optimization_barrier((part, thresholds))
    limits, haar = pl.pallas_call(
        haar_kernel,
        out_shape=[jax.ShapeDtypeStruct((LEVELS, n), F32), jax.ShapeDtypeStruct((4, n, n), BF16)],
        in_specs=[smem],
        out_specs=[vmem] * 2,
        compiler_params=PARAMS,
    )(thresholds)
    parts = parts_of(part)
    for _ in range(1, ITERS):
        inputs = (*estimate, *parts, map_t, data, const, haar, row_tab, col_tab)
        *estimate, part = pl.pallas_call(
            functools.partial(step_kernel, len(estimate), len(parts)),
            out_shape=[image, image],
            in_specs=[vmem] * (len(inputs) + 1),
            out_specs=[vmem, vmem],
            scratch_shapes=[pltpu.VMEM((2, 2 * side_rows, n), BF16), weighted, gridded],
            compiler_params=PARAMS,
        )(limits, *inputs)
        parts = parts_of(part)
    mine_of = lambda: lax.axis_index("tile") * n_spk + lax.axis_index("spk")
    return pl.pallas_call(
        functools.partial(last_kernel, len(parts), rows, mine_of),
        out_shape=jax.ShapeDtypeStruct((rows, 2, n), F32),
        in_specs=[vmem] * (len(parts) + 3),
        out_specs=vmem,
        compiler_params=PARAMS,
    )(limits, *estimate, *parts, haar)


def solution(mesh):
    placed = (
        P("coil", ("grp", "tile", "spk"), None, None),
        P("coil", ("grp", "tile", "spk"), None, None),
        P(("grp", "tile", "spk"), None, None),
        P(("grp", "tile", "spk"), None),
        P(("grp", "tile", "spk")),
        P(),
    )

    return jax.shard_map(
        local,
        mesh=mesh,
        in_specs=placed,
        out_specs=P(("grp", "tile", "spk"), None, None),
        check_vma=False,
    )
```

```python
import functools
import math

import jax
import jax.numpy as jnp
import numpy as np
from jax import lax
from jax.experimental import pallas as pl
from jax.experimental.pallas import tpu as pltpu
from jax.sharding import PartitionSpec as P

LEVELS = 3
ITERS = 4
STEP_SIZE = 0.5
GROUP = 8
MARGIN = 8
PARAMS = pltpu.CompilerParams(vmem_limit_bytes=26 * 2**20)
STEP_PARAMS = pltpu.CompilerParams(vmem_limit_bytes=26 * 2**20)
F32 = jnp.float32
BF16 = jnp.bfloat16


STRIDE = 16


def dft_seeds(n):
    coarse, fine = STRIDE * np.arange(n // STRIDE), np.arange(STRIDE)
    rows = []
    for positions, scale in ((coarse, 1.0), (fine, 1.0 / math.sqrt(n)), (2 * fine, 1.0 / math.sqrt(n))):
        angles = 2.0 * math.pi / n * (np.outer(positions, np.arange(n)) % n)
        rows += [np.cos(angles) * scale, np.sin(angles) * scale]
    return np.concatenate(rows).astype(np.float32)


def dft_kernel(seed_ref, out_ref, left_ref):
    n = seed_ref.shape[1]
    half, coarse = n // 2, n // STRIDE
    at = [0, coarse, 2 * coarse, 2 * coarse + STRIDE, 2 * coarse + 2 * STRIDE, 2 * coarse + 3 * STRIDE]
    fine = [seed_ref[start : start + STRIDE, :] for start in at[2:]]

    def turned(i, cos, sin):
        big_cos, big_sin = (seed_ref[start + i : start + i + 1, :] for start in at[:2])
        return big_cos * cos - big_sin * sin, big_sin * cos + big_cos * sin

    for i in range(coarse):
        rows = slice(i * STRIDE, (i + 1) * STRIDE)
        (cos_h, cos_l), (sin_h, sin_l) = (split2(values) for values in turned(i, fine[0], fine[1]))
        for at_lane, cos, sin in ((0, cos_h, sin_h), (2 * n, cos_h, sin_h), (4 * n, cos_l, sin_l)):
            left_ref[rows, at_lane : at_lane + 2 * n] = joined([cos, sin], 1)
            left_ref[n + i * STRIDE : n + (i + 1) * STRIDE, at_lane : at_lane + 2 * n] = joined([-sin, cos], 1)
    for i in range(coarse // 2):
        cos, sin = (values[:, :half] for values in turned(2 * i, fine[2], fine[3]))
        for start, values in ((0, (cos, -sin)), (half, (sin, cos))):
            rows = slice(start + i * STRIDE, start + (i + 1) * STRIDE)
            out_ref[0, rows, :], out_ref[1, rows, :] = split2(joined(values, 1))
    parts = [part.astype(F32) for values in fine[:2] for part in split3(values[1:2] * math.sqrt(n))]
    parts.append(jnp.zeros((STRIDE - len(parts), n), F32))
    out_ref[2, 0:STRIDE, :] = joined(parts, 0).astype(BF16)


def haar_rows(positions, length):
    block, within = positions // length * length, positions % length
    hits = [(block + (within >> LEVELS), jnp.ones(positions.shape, F32))]
    for level in range(1, LEVELS + 1):
        sign = jnp.where((within >> (level - 1)) % 2 == 0, 1.0, -1.0)
        hits.append((block + (length >> level) + (within >> level), sign))
    return hits


def haar_signs(n, length, flipped):
    rows = lax.broadcasted_iota(jnp.int32, (1, n) if flipped else (n, 1), int(flipped))
    positions = lax.broadcasted_iota(jnp.int32, (n, 1) if flipped else (1, n), int(not flipped))
    out = jnp.zeros((n, n), F32)
    for row, sign in haar_rows(positions, length):
        out = jnp.where(rows == row, sign, out)
    return out.astype(BF16)


def split2(x):
    high = x.astype(BF16)
    return high, (x - high.astype(F32)).astype(BF16)


def split3(x):
    high, mid = split2(x)
    return high, mid, (x - high.astype(F32) - mid.astype(F32)).astype(BF16)


def mm(a, b):
    return jnp.dot(a, b, preferred_element_type=F32)


def mm_t(a, b):
    return lax.dot_general(a, b, (((1,), (1,)), ((), ())), preferred_element_type=F32)


def joined(parts, axis):
    return jnp.concatenate(parts, axis=axis)


def twiddles(const, half):
    rows = const[2, 0:8, 0:half].astype(F32)
    return rows[0:1] + rows[1:2] + rows[2:3], rows[3:4] + rows[4:5] + rows[5:6]


def half_dfts(first, second, const):
    high, low = split2(joined([first, second], 0))
    return mm(joined([high, low, high], 1), joined([const[0], const[0], const[1]], 0))


def right_dft(re, im, const):
    n = re.shape[0]
    half = n // 2
    cos, sin = twiddles(const, half)
    sum_re, sum_im = re[:, :half] + re[:, half:], im[:, :half] + im[:, half:]
    dif_re, dif_im = re[:, :half] - re[:, half:], im[:, :half] - im[:, half:]
    turned = joined([dif_re * cos + dif_im * sin, dif_im * cos - dif_re * sin], 1)
    out = half_dfts(joined([sum_re, sum_im], 1), turned, const)
    return joined([joined([out[:n, lo : lo + half], out[n:, lo : lo + half]], 1) for lo in (0, half)], 0)


def right_idft(re, im, const):
    n = re.shape[0]
    half = n // 2
    cos, sin = twiddles(const, half)
    even, odd = (joined([re[:, lo : lo + half], -im[:, lo : lo + half]], 1) for lo in (0, half))
    out = half_dfts(even, odd, const)
    even_re, even_im, odd_re, odd_im = out[:n, :half], -out[:n, half:], out[n:, :half], -out[n:, half:]
    turn_re, turn_im = odd_re * cos - odd_im * sin, odd_im * cos + odd_re * sin
    out_re = joined([even_re + turn_re, even_re - turn_re], 1)
    return joined([out_re, joined([even_im + turn_im, even_im - turn_im], 1)], 0)


def left_dft(re, im, left):
    high, low = split2(joined([re, im], 0))
    return mm(left[...], joined([high, low, high], 0))


def labels(positions, length):
    out = jnp.ones(positions.shape, F32)
    for level in range(1, LEVELS + 1):
        out = out + jnp.where(positions < length >> level, 1.0, 0.0)
    return out


def band_tables(col_pos, row_pos, n, thr_ref, thr_lanes):
    col_label, row_label = labels(col_pos, n), labels(row_pos % 2**LEVELS, 2**LEVELS)
    scale = jnp.exp2(-0.5 * jnp.minimum(col_label, LEVELS)) * jnp.exp2(-0.5 * jnp.minimum(row_label, LEVELS))
    band = jnp.minimum(col_label, row_label)
    limits = jnp.full(band.shape, 1.0, F32)
    for level in range(LEVELS):
        limits = jnp.where(band == level + 1, thr_ref[level : level + 1, :thr_lanes], limits)
    return limits, scale, band


def shrunk(re, im, limits, scale, band):
    re, im = re * scale, im * scale
    magnitude = jnp.sqrt(re * re + im * im)
    factor = jnp.maximum(magnitude - limits, 0.0) / jnp.maximum(magnitude, limits)
    factor = jnp.where(band <= LEVELS, factor, 1.0) * scale
    return re * factor, im * factor


def shrink(re, im, thr_ref, haar):
    n = re.shape[0]
    col_pos = lax.broadcasted_iota(jnp.int32, (n, 1), 0)
    row_pos = lax.broadcasted_iota(jnp.int32, (1, n), 1)
    tables = band_tables(col_pos, row_pos, n, thr_ref, n)
    half = mm(joined([haar[0]] * 2, 1), joined(split2(joined([re, im], 1)), 0))
    half = joined([half[:, :n], half[:, n:]], 0)
    full = mm(joined(split2(half), 1), joined([haar[2]] * 2, 0))
    kept = joined(shrunk(full[:n], full[n:], *tables), 1)
    half = mm(joined([haar[1]] * 2, 1), joined(split2(kept), 0))
    half = joined([half[:, :n], half[:, n:]], 0)
    full = mm(joined(split2(half), 1), joined([haar[3]] * 2, 0))
    return full[:n], full[n:]


def density_of(ro, n, live_total):
    lane = lax.broadcasted_iota(jnp.int32, (1, ro), 1)
    offset = jnp.abs(lane - ro // 2).astype(F32)
    return (offset + 0.5) * (n / (3.0 * ro * live_total))


def smear(col_table, weighted):
    col = col_table.astype(F32)
    return joined([(col * weighted[p : p + 1]).astype(BF16) for p in range(2)], 0)


def grid_group(group, rows_s, cols_s, weighted_s, grid_s):
    span = cols_s.shape[-1]
    for side in range(2):
        smeared = smear(cols_s[group, side], weighted_s[group, side])
        grid_s[side] += mm_t(smeared, rows_s[group, :, side * span : (side + 1) * span])


def to_sides(kspace):
    n = kspace.shape[0] // 2
    mid = n // 2
    low, high = [], []
    for part in (kspace[:n], kspace[n:]):
        low += [part[n - MARGIN :], part[: mid + MARGIN]]
        high += [part[mid - MARGIN :], part[:MARGIN]]
    return joined(low, 0), joined(high, 0)


def from_sides(grid_s):
    span = grid_s.shape[1] // 2
    mid, m = span - 2 * MARGIN, MARGIN
    out = []
    for p in range(2):
        low, high = grid_s[0, p * span : (p + 1) * span], grid_s[1, p * span : (p + 1) * span]
        out += [
            low[m : 2 * m] + high[mid + m :],
            low[2 * m : mid],
            low[mid:] + high[: 2 * m],
            high[2 * m : mid],
            high[mid : mid + m] + low[:m],
        ]
    return joined(out, 0)


def adjoint(gridded, const, left):
    n = gridded.shape[0] // 2
    half = left_dft(gridded[:n], -gridded[n:], left)
    return right_idft(half[:n], -half[n:], const)


def pack_kernel(data_ref, weight_ref, bins_ref, count_ref, out_ref):
    slots, ro = bins_ref.shape
    n = ro
    bins = bins_ref[...]
    fields = [data_ref[:, p, :].astype(F32) for p in range(2)]
    fields += [weight_ref[i].astype(F32) for i in range(weight_ref.shape[0])]
    fields += [(bins // n).astype(F32), (bins % n).astype(F32)]
    fields.append(jnp.full((slots, ro), count_ref[0].astype(F32)))
    out_ref[...] = joined(fields, 0).astype(BF16)


def join_kernel(data_rows, *refs):
    pieces, (data_out, spoke_out) = refs[:-2], refs[-2:]
    for i, piece in enumerate(pieces):
        data_out[i] = piece[:data_rows]
        spoke_out[i] = piece[data_rows:]


def stack_kernel(*refs):
    for i, piece in enumerate(refs[:-1]):
        refs[-1][i] = piece[...]


def haar_kernel(thr_ref, thr_out, haar_out):
    n = haar_out.shape[1]
    for level in range(LEVELS):
        thr_out[level : level + 1, :] = jnp.full((1, n), thr_ref[level])
    for i, (length, flipped) in enumerate(((n, False), (n, True), (2**LEVELS, True), (2**LEVELS, False))):
        haar_out[i] = haar_signs(n, length, flipped)


def first_kernel(first_of, spoke_blocks, coil_blocks, live_total, counts, spk_dev, n, *refs):
    spoke_refs, data_refs, refs = refs[: counts[0]], refs[counts[0] : sum(counts)], refs[sum(counts) :]
    const_ref, left_ref, rows_s, cols_s, data_out, back_out, slots, weighted_s, grid_s, list_s = refs
    spoke_rows = slots.shape[1] - 2 * spk_dev
    ro = slots.shape[-1]
    groups, _, _, span = weighted_s.shape
    per_group, half = 2 * span // ro, ro // 2
    for place, value in spoke_blocks(spoke_refs):
        slots[place, 0:spoke_rows] = value.astype(F32)
    for place, value in coil_blocks(data_refs):
        slots[place, spoke_rows:] = value.astype(F32)
    taken = jnp.int32(0)
    for block in range(slots.shape[0]):
        count = jnp.max(slots[block, spoke_rows - spk_dev : spoke_rows, :]).astype(jnp.int32)
        for depth in range(spk_dev):
            list_s[0, taken] = block
            list_s[1, taken] = depth
            taken = taken + (depth < count).astype(jnp.int32)
    start = first_of()
    density = density_of(ro, n, live_total)
    row_order = lax.broadcasted_iota(jnp.int32, (n, ro), 0)
    row_order = jnp.where(row_order < n // 2, 2 * row_order, 2 * row_order - n + 1)
    row_cells = row_order.astype(F32).astype(BF16)
    side_rows = n // 2 + 2 * MARGIN
    low_cells = lax.broadcasted_iota(jnp.int32, (side_rows, half), 0) + (n - MARGIN)
    side_cells = [((low_cells + side * (n // 2)) % n).astype(F32).astype(BF16) for side in range(2)]
    grid_s[...] = jnp.zeros_like(grid_s)

    def table(cells, at, weights):
        before = jnp.where(at == 0, n - 1.0, at - 1)
        after = jnp.where(at == n - 1, 0.0, at + 1)
        before, at, after = (t.astype(BF16) for t in (before, at, after))
        weights = [w.astype(BF16) for w in weights]
        out = jnp.where(cells == after, weights[2], jnp.zeros((), BF16))
        out = jnp.where(cells == at, weights[1], out)
        return jnp.where(cells == before, weights[0], out)

    def build(group):
        for j in range(per_group):
            which = start + group * per_group + j
            block, depth = list_s[0, which], list_s[1, which]
            slot = [slots[block, pl.ds(f * spk_dev + depth, 1), :] for f in (0, 1, 2, 3, 4, 5, 6, 7, 9, 10)]
            low_first = slot[7][:, 1:2] <= n // 2
            slot = [jnp.where(low_first, f, joined([f[:, half:], f[:, :half]], 1)) for f in slot + [density]]
            rows = table(row_cells, slot[6], slot[0:3])
            for side in range(2):
                lanes = slice(side * half, (side + 1) * half)
                to = slice(j * half, (j + 1) * half)
                rows_s[group, :, side * span + j * half : side * span + (j + 1) * half] = rows[:, lanes]
                cols_s[group, side, :, to] = table(side_cells[side], slot[7][:, lanes], [w[:, lanes] for w in slot[3:6]])
                data = joined([slot[8][:, lanes], slot[9][:, lanes]], 0)
                data_out[group, side, 0:2, to] = data
                data_out[group, side, 2:3, to] = slot[10][:, lanes]
                weighted_s[group, side, :, to] = -slot[10][:, lanes] * data

    build(0)

    def group_step(group, carry):
        grid_group(group - 1, rows_s, cols_s, weighted_s, grid_s)
        build(group)
        return carry

    lax.fori_loop(1, groups, group_step, 0, unroll=True)
    grid_group(groups - 1, rows_s, cols_s, weighted_s, grid_s)
    back_out[...] = adjoint(from_sides(grid_s), const_ref, left_ref)


def target_of(est_ref, part_refs):
    out = []
    for p in range(2):
        gradient = sum(part[p] for part in part_refs)
        out.append((0.0 if est_ref is None else est_ref[p]) - STEP_SIZE * gradient)
    return out


def step_kernel(n_est, n_parts, *refs):
    thr_ref, refs = refs[0], refs[1:]
    est_ref, refs = refs[0] if n_est else None, refs[n_est:]
    part_refs, refs = refs[:n_parts], refs[n_parts:]
    map_ref, data_ref, const_ref, left_ref, haar_ref, rows_s, cols_s, est_out, part_out, sides_s, weighted_s, grid_s = refs
    groups, _, _, span = weighted_s.shape
    n, rows = map_ref.shape[1], cols_s.shape[2]
    target = target_of(est_ref, part_refs)
    re, im = shrink(target[0], target[1], thr_ref, haar_ref)
    est_out[0] = re
    est_out[1] = im
    mre, mim = map_ref[0], map_ref[1]
    half = right_dft(mre * re - mim * im, mre * im + mim * re, const_ref)
    for side, values in enumerate(to_sides(left_dft(half[:n], half[n:], left_ref))):
        sides_s[side] = values.astype(BF16)
    grid_s[...] = jnp.zeros_like(grid_s)

    def sample_group(group):
        width = min(n, span)
        for side in range(2):
            for at in range(0, span, width):
                lanes = slice(at, at + width)
                inner = mm(sides_s[side], rows_s[group, :, side * span + at : side * span + at + width])
                col = cols_s[group, side, :, lanes].astype(F32)
                model = [jnp.sum(inner[p * rows : (p + 1) * rows] * col, axis=0, keepdims=True) for p in range(2)]
                data = data_ref[group, side, :, lanes]
                weighted_s[group, side, :, lanes] = data[2:3] * (joined(model, 0) - data[0:2])

    sample_group(0)

    def group_step(group, carry):
        grid_group(group - 1, rows_s, cols_s, weighted_s, grid_s)
        sample_group(group)
        return carry

    lax.fori_loop(1, groups, group_step, 0, unroll=True)
    grid_group(groups - 1, rows_s, cols_s, weighted_s, grid_s)
    back = adjoint(from_sides(grid_s), const_ref, left_ref)
    conj_map(map_ref[0], map_ref[1], back, part_out)


def conj_map(mre, mim, back, part_out):
    n = mre.shape[0]
    bre, bim = back[:n], back[n:]
    part_out[0] = mre * bre + mim * bim
    part_out[1] = mre * bim - mim * bre


def map_kernel(blocks_of, pieces, *refs):
    piece_refs, (back_ref, map_out, part_out, full) = refs[:pieces], refs[pieces:]
    rows = piece_refs[0].shape[1]
    for place, value in blocks_of(piece_refs):
        for p in range(2):
            full[p, pl.ds(place * rows, rows), :] = value[:, p, :]
    for p in range(2):
        map_out[p] = full[p].T
    conj_map(map_out[0], map_out[1], back_ref[...], part_out)


def last_kernel(n_parts, rows, mine_of, thr_ref, est_ref, *refs):
    part_refs, (haar_ref, out_ref) = refs[:n_parts], refs[n_parts:]
    n = est_ref.shape[1]
    target = target_of(est_ref, part_refs)
    pick = lax.broadcasted_iota(jnp.int32, (rows, n), 1) == (
        lax.broadcasted_iota(jnp.int32, (rows, n), 0) + mine_of() * rows
    )
    pick = jnp.where(pick, 1.0, 0.0).astype(BF16)
    own = mm_t(joined([pick] * 3, 1), joined(split3(joined(target, 0)), 1))
    row_pos = lax.broadcasted_iota(jnp.int32, (rows, 1), 0)
    col_pos = lax.broadcasted_iota(jnp.int32, (1, n), 1)
    tables = band_tables(col_pos, row_pos, n, thr_ref, n)
    row_haar, row_back = haar_ref[3][:rows, :rows], haar_ref[2][:rows, :rows]

    def by_rows(signs, wide):
        return mm(signs, split2(wide)[0]) + mm(signs, split2(wide)[1])

    half = by_rows(row_haar, own)
    half = joined([half[:, :n], half[:, n:]], 0)
    full = mm(joined(split2(half), 1), joined([haar_ref[1]] * 2, 0))
    kept = joined(shrunk(full[:rows], full[rows:], *tables), 0)
    half = mm(joined(split2(kept), 1), joined([haar_ref[0]] * 2, 0))
    full = by_rows(row_back, joined([half[:rows], half[rows:]], 1))
    out_ref[:, 0, :] = full[:, :n]
    out_ref[:, 1, :] = full[:, n:]


def local(coil_maps, kspace_data, interp_weights, sample_bins, spoke_count, thresholds):
    n_tile, n_coil, n_spk = (lax.axis_size(name) for name in ("tile", "coil", "spk"))
    blocks = n_tile * n_spk
    rows, _, n = coil_maps.shape[1:]
    spk_dev, ro = sample_bins.shape
    live_total = blocks * spk_dev // 2
    own_map = coil_maps[0]
    by_core = n_coil == n_spk == 2 and n_tile & (n_tile - 1) == 0
    vmem = pl.BlockSpec(memory_space=pltpu.VMEM)
    smem = pl.BlockSpec(memory_space=pltpu.SMEM)
    data_rows, fields = 2 * spk_dev, 11
    spoke_rows = fields * spk_dev - data_rows
    bundle = pl.pallas_call(
        pack_kernel,
        out_shape=jax.ShapeDtypeStruct((fields * spk_dev, ro), BF16),
        in_specs=[vmem, vmem, vmem, smem],
        out_specs=vmem,
        compiler_params=PARAMS,
    )(kspace_data[0], jnp.swapaxes(interp_weights, 0, 1), sample_bins, spoke_count)

    const, left = pl.pallas_call(
        dft_kernel,
        out_shape=[jax.ShapeDtypeStruct((3, n, n), BF16), jax.ShapeDtypeStruct((2 * n, 6 * n), BF16)],
        in_specs=[vmem],
        out_specs=[vmem] * 2,
        compiler_params=PARAMS,
    )(jnp.asarray(dft_seeds(n)))

    if by_core:
        onto = [(0, 2), (3, 1), (1, 0), (2, 3)]
        across = [(1, 2), (2, 1)]

        def spread(value):
            out = [value]
            for shift in range(1, n_tile):
                out.append(lax.ppermute(value, "tile", [(i, i ^ shift) for i in range(n_tile)]))
            return out

        def to_coil(value):
            return [value, lax.ppermute(value, ("coil", "spk"), across), lax.ppermute(value, ("coil", "spk"), onto)]

        def senders():
            tile = lax.axis_index("tile")
            return [tile ^ shift for shift in range(n_tile)]

        def spoke_blocks(refs):
            own, other = refs
            spk = lax.axis_index("spk")
            for i, at in enumerate(senders()):
                yield at * 2 + spk, own[i]
                yield at * 2 + 1 - spk, other[i]

        def coil_blocks(refs):
            own, far, near = refs
            coil = lax.axis_index("coil")
            is_own = coil == lax.axis_index("spk")
            for i, at in enumerate(senders()):
                yield at * 2 + coil, jnp.where(is_own, own[i], far[i])
                yield at * 2 + 1 - coil, near[i]

        swap = [(0, 1), (1, 0)]
        pieces = spread(bundle)
        own_map, bundle = lax.optimization_barrier((own_map, bundle))
        map_pieces = spread(own_map)
        pieces, const, left = lax.optimization_barrier((pieces, const, left))
        own_data, own_spokes = pl.pallas_call(
            functools.partial(join_kernel, data_rows),
            out_shape=[
                jax.ShapeDtypeStruct((n_tile, data_rows, ro), BF16),
                jax.ShapeDtypeStruct((n_tile, spoke_rows, ro), BF16),
            ],
            in_specs=[vmem] * n_tile,
            out_specs=[vmem] * 2,
            compiler_params=PARAMS,
        )(*pieces)
        other_spokes = lax.ppermute(own_spokes, "spk", swap)
        coil_data = to_coil(own_data)
        map_pieces, own_spokes, own_data = lax.optimization_barrier((map_pieces, own_spokes, own_data))
        own_maps = pl.pallas_call(
            stack_kernel,
            out_shape=jax.ShapeDtypeStruct((n_tile, *own_map.shape), F32),
            in_specs=[vmem] * n_tile,
            out_specs=vmem,
            compiler_params=PARAMS,
        )(*map_pieces)
        maps = to_coil(own_maps)
        spokes = [own_spokes, other_spokes]
        share, first_of = live_total, lambda: jnp.int32(0)

        def parts_of(part):
            return [part, lax.ppermute(part, "spk", swap)]
    else:
        def gather(value):
            return [lax.all_gather(value, ("tile", "spk"), axis=0, tiled=False)]

        def spoke_blocks(refs):
            return ((i, refs[0][i]) for i in range(blocks))

        coil_blocks = spoke_blocks
        spokes, coil_data, maps = gather(bundle[data_rows:]), gather(bundle[:data_rows]), gather(own_map)
        share = live_total // blocks
        first_of = lambda: (lax.axis_index("tile") * n_spk + lax.axis_index("spk")) * share

        def parts_of(part):
            return [lax.psum(part, ("tile", "coil", "spk"))]

    per_group = min(GROUP, share)
    groups, span, side_rows = share // per_group, per_group * ro // 2, n // 2 + 2 * MARGIN
    image = jax.ShapeDtypeStruct((2, n, n), F32)
    weighted = pltpu.VMEM((groups, 2, 2, span), F32)
    gridded = pltpu.VMEM((2, 2 * side_rows, n), F32)
    counts = (len(spokes), len(coil_data))
    row_tab, col_tab, data, back = pl.pallas_call(
        functools.partial(first_kernel, first_of, spoke_blocks, coil_blocks, live_total, counts, spk_dev, n),
        out_shape=[
            jax.ShapeDtypeStruct((groups, n, 2 * span), BF16),
            jax.ShapeDtypeStruct((groups, 2, side_rows, span), BF16),
            jax.ShapeDtypeStruct((groups, 2, 3, span), F32),
            jax.ShapeDtypeStruct((2 * n, n), F32),
        ],
        in_specs=[vmem] * (sum(counts) + 2),
        out_specs=[vmem] * 4,
        scratch_shapes=[
            pltpu.VMEM((blocks, fields * spk_dev, ro), F32),
            weighted,
            gridded,
            pltpu.SMEM((2, blocks * spk_dev + 1), jnp.int32),
        ],
        compiler_params=PARAMS,
    )(*spokes, *coil_data, const, left)
    map_t, part = pl.pallas_call(
        functools.partial(map_kernel, coil_blocks, len(maps)),
        out_shape=[image, image],
        in_specs=[vmem] * (len(maps) + 1),
        out_specs=[vmem, vmem],
        scratch_shapes=[pltpu.VMEM((2, n, n), F32)],
        compiler_params=PARAMS,
    )(*maps, back)
    estimate = []
    part, thresholds = lax.optimization_barrier((part, thresholds))
    limits, haar = pl.pallas_call(
        haar_kernel,
        out_shape=[jax.ShapeDtypeStruct((LEVELS, n), F32), jax.ShapeDtypeStruct((4, n, n), BF16)],
        in_specs=[smem],
        out_specs=[vmem] * 2,
        compiler_params=PARAMS,
    )(thresholds)
    parts = parts_of(part)
    for _ in range(1, ITERS):
        inputs = (*estimate, *parts, map_t, data, const, left, haar, row_tab, col_tab)
        *estimate, part = pl.pallas_call(
            functools.partial(step_kernel, len(estimate), len(parts)),
            out_shape=[image, image],
            in_specs=[vmem] * (len(inputs) + 1),
            out_specs=[vmem, vmem],
            scratch_shapes=[pltpu.VMEM((2, 2 * side_rows, n), BF16), weighted, gridded],
            compiler_params=STEP_PARAMS,
        )(limits, *inputs)
        parts = parts_of(part)
    mine_of = lambda: lax.axis_index("tile") * n_spk + lax.axis_index("spk")
    return pl.pallas_call(
        functools.partial(last_kernel, len(parts), rows, mine_of),
        out_shape=jax.ShapeDtypeStruct((rows, 2, n), F32),
        in_specs=[vmem] * (len(parts) + 3),
        out_specs=vmem,
        compiler_params=PARAMS,
    )(limits, *estimate, *parts, haar)


def solution(mesh):
    placed = (
        P("coil", ("grp", "tile", "spk"), None, None),
        P("coil", ("grp", "tile", "spk"), None, None),
        P(("grp", "tile", "spk"), None, None),
        P(("grp", "tile", "spk"), None),
        P(("grp", "tile", "spk")),
        P(),
    )

    return jax.shard_map(
        local,
        mesh=mesh,
        in_specs=placed,
        out_specs=P(("grp", "tile", "spk"), None, None),
        check_vma=False,
    )
```
